32 devices in a mesh: lat: 8 (over z, x), lon: 4 (over y, core).
Axes of the slice: x: 2, y: 2, z: 4, core: 2. Of those that a mesh axis runs over, the one named last changes fastest.
Arguments:
- courant: float32 [2, 16, 128, 512], P(None, None, 'lat', 'lon'), may hold values from -0.45 to 0.45
- obs_matrix: float32 [8, 32, 128, 128], P('lat', 'lon'), may hold values from -0.5 to 0.5
- obs_weight: float32 [8, 32, 128], P('lat', 'lon'), may hold values from 0.5 to 4
- innovation: float32 [8, 32, 128], P('lat', 'lon'), may hold values from -6 to 6
- block_owner: int32 [8, 32, 1], P('lat', 'lon'), may hold values from 0 to 3; in each aligned block of 8 rows (0 to 7, 8 to 15, ..., all dimensions but the last counted through in order) at most 2 rows name the same one
- block_row: int32 [8, 32], P('lat', 'lon'), may hold values from 0 to 255
- block_count: int32 [8, 4], P('lat', 'lon'), may hold values from 1 to 8, as said below
Outputs:
- increment: float32 [16, 128, 512], P(None, 'lat', 'lon')
- residual: float32 [16, 128, 512], P(None, 'lat', 'lon')
The draws below stay inside these ranges and needn't reach their ends.
Inputs may be any that keep to these rules, and one draw needn't show every extreme that they name: `block_owner`: among one device's 8 block slots no lon index is named more than 2 times, a bound that some block reaches. A device's first block_count slots are live, the rest are padding; some device has all 8 live.
All inputs are finite; a program needn't handle non-finite values.
Results may differ from the reference program's by a relative error of at most 0.0003.
Values sent between devices are 32-bit elements; how exact they have to be, the bound alone decides.
A program may use at most 64 MiB of HBM per device.

```python
import math
import jax
import jax.numpy as jnp
import numpy as np
from jax import lax

LEVELS = 16
CLAT = 16
CLON = 128
OBS = 128
CAP = 8
SLOT = 2
STEPS = 4
ITERS = 2
NLAT = 128
NLON = 512
BLOCKS = 32
N_LAT = 8
N_LON = 4


def draw_block_count(key, part):
    first_key, second_key = jax.random.split(jax.random.fold_in(key, 11))
    counted = jax.random.randint(first_key, (N_LAT * N_LON,), 1, CAP + 1)
    chosen = jax.random.randint(second_key, (), 0, N_LAT * N_LON)
    counted = jnp.where(jnp.arange(N_LAT * N_LON) == chosen, CAP, counted)
    return counted.reshape(N_LAT, N_LON).astype(jnp.int32)


def place_ends(drawn, key, smallest, high):
    dims = drawn.shape
    place = [jax.random.randint(jax.random.fold_in(key, axis), (), 0, dims[axis]) for axis in range(len(dims))]
    drawn = drawn.at[tuple(place)].set(smallest)
    longest = dims.index(max(dims))
    place[longest] = (place[longest] + 1) % dims[longest]
    return drawn.at[tuple(place)].set(high)


def block_scale(own_key, dims, cuts, smallest, high):
    def one(position, blocks):
        draws = jax.random.uniform(jax.random.fold_in(jax.random.fold_in(own_key, 6), position), (blocks,), jnp.float32, smallest / len(cuts), high / len(cuts))
        return jnp.repeat(jnp.exp(draws), dims[position] // blocks).reshape((-1,) + (1,) * (len(dims) - position - 1))

    level = one(*cuts[0])
    for cut in cuts[1:]:
        level = level * one(*cut)
    return level


def routed_block(rng, own, number, rows, number_of, top, reach, slope):
    sequence = jax.random.permutation(rng, number_of)
    heavy_load, usual = portions_of(number_of, rows * top, reach, slope, True), portions_of(number_of, rows * top, reach, slope, False)
    places = jnp.arange(number_of)

    def named(lengths, offset_by):
        used = int((lengths > 0).sum())
        fixed = max(1, used // 4)
        moved = fixed + (places - fixed + offset_by * (used - fixed)) % max(1, number_of - fixed)
        return jnp.zeros((number_of,), jnp.int32).at[sequence[jnp.where(places < fixed, places, moved)]].set(jnp.asarray(lengths, jnp.int32))

    lengths = jnp.where(number % 4 == 0, named(heavy_load, number // 4), named(usual, number - number // 4 - 1))
    mixed = jax.random.permutation(jax.random.fold_in(own, 3), number_of)
    donor, sink = mixed[0:number_of // 2 * 2:2], mixed[1:number_of // 2 * 2:2]
    room = jnp.minimum(lengths[donor] - 1, reach - lengths[sink]) // 2
    room = jnp.where((donor == sequence[0]) | (sink == sequence[0]) | (lengths[sink] == 0), 0, jnp.maximum(room, 0))
    moved = jax.random.randint(jax.random.fold_in(own, 4), (number_of // 2,), 0, 1 << 20) % (room + 1)
    lengths = lengths.at[donor].add(-moved).at[sink].add(moved)
    items = jnp.searchsorted(jnp.cumsum(lengths), jnp.arange(rows * top), side="right").astype(jnp.int32)
    listing = items.reshape(top, rows).T
    listing = listing[jax.random.permutation(jax.random.fold_in(own, 1), rows)]
    offset_by = jax.random.randint(jax.random.fold_in(own, 2), (rows, 1), 0, top)
    return jnp.take_along_axis(listing, (jnp.arange(top)[None, :] + offset_by) % top, axis=1)


def portions_of(number_of, total, limit, slope, full):
    weights = [(1 << 20) // math.isqrt(rank ** slope) + 1 for rank in range(1, number_of + 1)]
    largest = limit if full else min(limit, max(-(-total // number_of), total * weights[0] // sum(weights)))
    least = 1 if total - largest >= number_of - 1 else 0
    given, spare = [largest] + [least] * (number_of - 1), total - largest - least * (number_of - 1)
    while spare > 0:
        movable = [i for i in range(1, number_of) if given[i] < largest] or [i for i in range(1, number_of) if given[i] < limit]
        pool, remaining = sum([weights[i] for i in movable]), spare
        for i in movable:
            addition = min(limit - given[i], max(1, remaining * weights[i] // pool), spare)
            given[i] = given[i] + addition
            spare = spare - addition
    return np.array(given)


def scatter_about(rng, extent, scale, limit, cuts=(), kind=jnp.bfloat16):
    level = block_scale(rng, extent, cuts, -0.22, 0.18) if cuts else 1.0
    array = jax.random.normal(rng, extent, jnp.float32) * scale * level
    return jnp.minimum(jnp.maximum(array, -limit), limit).astype(kind)


def setup_inputs(seed: int = 0) -> dict:
    splits = jax.random.split(jax.random.key(seed), 8)
    courant = jnp.clip(jax.random.uniform(splits[0], (2, LEVELS, NLAT, NLON), jnp.float32, -0.45, 0.45) * block_scale(splits[0], (2, LEVELS, NLAT, NLON), ((2, 8), (3, 4)), -0.4, 0.0), -0.45, 0.45)
    obs_matrix = scatter_about(splits[1], (N_LAT, BLOCKS, OBS, CLON), CLON ** -0.5, 0.5, ((0, 8), (1, 4)), jnp.float32)
    obs_weight = jnp.clip(jnp.exp(math.log(4.0) - 2.0794415 * jax.random.uniform(splits[2], (N_LAT, BLOCKS, OBS), jnp.float32) ** block_scale(splits[2], (N_LAT, BLOCKS, OBS), ((0, 8), (1, 4)), -0.2, 0.2)), 0.5, 4.0)
    innovation = scatter_about(splits[3], (N_LAT, BLOCKS, OBS), 1.0, 6.0, ((0, 8), (1, 4)), jnp.float32)
    block_owner_keys = jax.random.split(jax.random.fold_in(splits[4], 1), N_LAT * BLOCKS // CAP)
    block_owner_turns = jax.random.permutation(jax.random.fold_in(splits[4], 3), N_LAT * BLOCKS // CAP)
    block_owner = jax.vmap(lambda own, number: routed_block(jax.random.fold_in(splits[4], 2), own, number, CAP, N_LON, 1, SLOT, 2))(block_owner_keys, block_owner_turns).reshape((N_LAT, BLOCKS, 1))
    block_row = place_ends(jax.random.randint(splits[5], (N_LAT, BLOCKS), 0, LEVELS * CLAT), jax.random.fold_in(splits[5], 1), 0, (LEVELS * CLAT) - 1).astype(jnp.int32)
    block_count = draw_block_count(jax.random.fold_in(splits[7], 71), 0)
    return dict(courant=courant, obs_matrix=obs_matrix, obs_weight=obs_weight, innovation=innovation, block_owner=block_owner, block_row=block_row, block_count=block_count)


def from_south(grid_field):
    return jnp.pad(grid_field[:, :-1, :], ((0, 0), (1, 0), (0, 0)))


def from_north(grid_field):
    return jnp.pad(grid_field[:, 1:, :], ((0, 0), (0, 1), (0, 0)))


def tangent_step(grid_field, rate_parts, keep_self):
    return (keep_self * grid_field + rate_parts[0] * from_south(grid_field) + rate_parts[1] * from_north(grid_field)
            + rate_parts[2] * jnp.roll(grid_field, 1, axis=2) + rate_parts[3] * jnp.roll(grid_field, -1, axis=2))


def adjoint_step(grid_field, rate_parts, keep_self):
    return (keep_self * grid_field + from_north(rate_parts[0] * grid_field) + from_south(rate_parts[1] * grid_field)
            + jnp.roll(rate_parts[2] * grid_field, -1, axis=2) + jnp.roll(rate_parts[3] * grid_field, 1, axis=2))


def reference(courant, obs_matrix, obs_weight, innovation, block_owner, block_row, block_count):
    rate_parts = (jnp.maximum(courant[0], 0.0), jnp.maximum(-courant[0], 0.0),
                  jnp.maximum(courant[1], 0.0), jnp.maximum(-courant[1], 0.0))
    keep_self = 1.0 - rate_parts[0] - rate_parts[1] - rate_parts[2] - rate_parts[3]
    owner_lon = block_owner[:, :, 0]
    level_idx = block_row // CLAT
    lat_idx = jnp.arange(N_LAT, dtype=jnp.int32)[:, None] * CLAT + block_row % CLAT
    lon_idx = owner_lon[:, :, None] * CLON + jnp.arange(CLON, dtype=jnp.int32)[None, None, :]
    cell_index = ((level_idx * NLAT + lat_idx) * NLON)[:, :, None] + lon_idx
    slot_index = jnp.arange(BLOCKS, dtype=jnp.int32) % CAP
    live_mask = slot_index[None, :] < jnp.repeat(block_count, CAP, axis=1)
    weighted = jnp.where(live_mask[:, :, None], obs_weight, 0.0)

    def observe(grid_field):
        seen_rows = grid_field.reshape(-1)[cell_index]
        return jnp.einsum("ibok,ibk->ibo", obs_matrix, seen_rows, precision=lax.Precision.HIGHEST)

    def observe_adjoint(block_terms):
        spread = jnp.einsum("ibok,ibo->ibk", obs_matrix, block_terms, precision=lax.Precision.HIGHEST)
        flat_out = jnp.zeros((LEVELS * NLAT * NLON,), jnp.float32).at[cell_index].add(spread)
        return flat_out.reshape(LEVELS, NLAT, NLON)

    def model_adjoint(grid_field):
        for sweep in range(STEPS):
            grid_field = adjoint_step(grid_field, rate_parts, keep_self)
        return grid_field

    def hessian(vector):
        moved = vector
        for sweep in range(STEPS):
            moved = tangent_step(moved, rate_parts, keep_self)
        return vector + model_adjoint(observe_adjoint(weighted * observe(moved)))

    right_side = model_adjoint(observe_adjoint(weighted * innovation))
    increment = jnp.zeros_like(right_side)
    residual = right_side
    direction = right_side
    norm_now = jnp.sum(residual * residual)
    for sweep in range(ITERS):
        image_vec = hessian(direction)
        step_size = norm_now / jnp.sum(direction * image_vec)
        increment = increment + step_size * direction
        residual = residual - step_size * image_vec
        if sweep + 1 < ITERS:
            norm_next = jnp.sum(residual * residual)
            direction = residual + (norm_next / norm_now) * direction
            norm_now = norm_next
    return increment, residual
```

```python
import functools

import jax
import jax.numpy as jnp
from jax import lax
from jax.experimental import pallas as pl
from jax.experimental.pallas import tpu as pltpu
from jax.sharding import PartitionSpec as P

STEPS = 4
HALO = 2 * STEPS
SLOT = 2
WIN = 2 * HALO + 1
PAD_WIN = WIN + 1
MESH = pl.DeviceIdType.MESH
F32 = jnp.float32
BF16 = jnp.bfloat16


def split3(x):
    hi = x.astype(BF16)
    rest = x - hi.astype(F32)
    mid = rest.astype(BF16)
    low = (rest - mid.astype(F32)).astype(BF16)
    return hi, mid, low


def dot3(onehot, x):
    total = None
    for part in split3(x):
        term = jnp.dot(onehot, part, preferred_element_type=F32)
        total = term if total is None else total + term
    return total


def split_rates(c0, c1):
    a, b = jnp.maximum(c0, 0.0), jnp.maximum(-c0, 0.0)
    e, f = jnp.maximum(c1, 0.0), jnp.maximum(-c1, 0.0)
    return a, b, e, f, 1.0 - a - b - e - f


def kernel(
    n_lat, n_lon,
    courant, obs, weight_in, innov_in, owner_in, row_in, count_in,
    inc_out, res_out,
    flow, obs_v, terms, codes, code_out, hot, dense_hot, field, dense_field,
    main_out, main_edge, strip_out, strip_edge, main_in, strip_in, side_in,
    win_rates, lat_out, lat_in, lon_out, lon_in, lat_halo, lon_halo, parts, red_lon, red_lat,
    ask_out, ask_in,
    obs_sem, flow_sem, wide_send, wide_recv, lat_send, lat_recv, lon_send, lon_recv,
    red_lon_send, red_lon_recv, red_lat_send, red_lat_recv,
    weight, innov, owner, row, count, input_sems,
):
    li = lax.axis_index("lat")
    lo = lax.axis_index("lon")
    _, levels, clat, clon = flow.shape
    cap = obs_v.shape[0]
    n_src = 3 * n_lon
    n_blocks = codes.shape[0] * cap
    span = 4 * clat
    half = levels // 2
    ring = clat + HALO
    width = clon // levels

    small = [
        pltpu.make_async_copy(src, dst, input_sems.at[n])
        for n, (src, dst) in enumerate((
            (owner_in, owner), (row_in, row), (count_in, count), (weight_in, weight), (innov_in, innov)))
    ]
    for copy in small:
        copy.start()
    flow_copy = pltpu.make_async_copy(courant, flow, flow_sem)
    flow_copy.start()
    obs_copy = pltpu.make_async_copy(obs.at[0], obs_v, obs_sem)
    obs_copy.start()

    def exists(d):
        return (li + d >= 0) & (li + d < n_lat)

    def guarded(d, run):
        if d == 0:
            run()
        else:
            pl.when(exists(d))(run)

    def lon_at(j):
        return lax.rem(lo + j + n_lon, n_lon)

    barrier = pltpu.get_barrier_semaphore()

    def greet(lat, lon):
        pl.semaphore_signal(barrier, inc=1, device_id={"lat": lat, "lon": lon}, device_id_type=MESH)

    @pl.loop(1, n_lat)
    def _(j):
        greet(lax.rem(li + j, n_lat), lo)

    for d in (-1, 1):
        def hello(d=d):
            for j in range(1, n_lon):
                greet(li + d, lon_at(j))
        guarded(d, hello)
    for j in range(1, n_lon):
        greet(li, lon_at(j))

    for copy in small:
        copy.wait()

    sub = lax.broadcasted_iota(jnp.int32, (cap, clon), 0)
    live = count[0, 0]
    owners = [owner[0, b] for b in range(cap)]
    levs = [lax.div(row[0, b], jnp.int32(clat)) for b in range(cap)]
    lats = [row[0, b] - levs[b] * clat for b in range(cap)]
    slots = []
    for b in range(cap):
        s = jnp.int32(0)
        for c in range(b):
            s = s + (owners[c] == owners[b]).astype(jnp.int32)
        slots.append(jnp.minimum(s, SLOT - 1))
    for o in range(n_lon):
        for s in range(SLOT):
            lev = jnp.int32(0)
            for b in range(cap):
                lev = jnp.where((owners[b] == o) & (slots[b] == s), levs[b], lev)
            ask_out[0, o * SLOT + s] = lev

    def column(values):
        tile = jnp.full((cap, clon), values[0], jnp.int32)
        for b in range(1, cap):
            tile = jnp.where(sub == b, values[b], tile)
        return tile

    level_tile, lat_tile, owner_tile = column(levs), column(lats), column(owners)

    def code_of(owner_now, lat_now):
        return (level_tile * n_lon + owner_now) * span + lat_now + clat

    for d in (-1, 0, 1):
        code_out[d + 1] = jnp.where(sub < live, code_of(owner_tile, lat_tile - clat * d), -1).astype(F32)

    sides = (li > 0).astype(jnp.int32) + (li < n_lat - 1).astype(jnp.int32)
    pl.semaphore_wait(barrier, (n_lon - 1) + (n_lat - 1) + sides * (n_lon - 1))

    def wide(kind, d, j, src, dst):
        return pltpu.make_async_remote_copy(
            src_ref=src, dst_ref=dst,
            send_sem=wide_send.at[kind, d + 1, j], recv_sem=wide_recv.at[kind, d + 1, j],
            device_id={"lat": li + d, "lon": lon_at(j)}, device_id_type=MESH,
        )

    def slot_of(d, j, out):
        return (1 - d) * n_lon + (lo if out else lon_at(-j))

    def start_wide(make):
        for d in (-1, 1, 0):
            def run(d=d):
                for j in range(n_lon):
                    if (d, j) != (0, 0):
                        make(d, j, True).start()
            guarded(d, run)

    def recv_wide(make):
        for d in (-1, 1, 0):
            def run(d=d):
                for j in range(n_lon):
                    if (d, j) != (0, 0):
                        make(d, j, False).wait_recv()
            guarded(-d, run)

    def done_wide(make):
        for d in (-1, 1, 0):
            def run(d=d):
                for j in range(n_lon):
                    if (d, j) != (0, 0):
                        make(d, j, True).wait_send()
            guarded(d, run)

    def code_make(d, j, out):
        return wide(0, d, j, code_out.at[d + 1], codes.at[slot_of(d, j, out)])

    def ask_make(d, j, out):
        return wide(1, d, j, ask_out, ask_in.at[slot_of(d, j, out)])

    def place(d):
        return (HALO, clat) if d == 0 else ((0, HALO) if d == 1 else (HALO + clat, HALO))

    def main_make(d, j, out):
        first, size = place(d)
        src = main_out.at[j] if d == 0 else main_edge.at[(d + 1) // 2, j]
        return wide(2, d, j, src, main_in.at[:, lo if out else lon_at(-j), :, pl.ds(first, size), :])

    def strip_make(d, j, out):
        first, size = place(d)
        src = strip_out.at[j] if d == 0 else strip_edge.at[(d + 1) // 2, j]
        return wide(3, d, j, src, strip_in.at[lo if out else lon_at(-j), pl.ds(first, size), :])

    def term_make(rnd):
        def make(d, j, out):
            return wide(4 + rnd, d, j, terms.at[rnd, n_lon + lo], terms.at[rnd, slot_of(d, j, out)])
        return make

    def lat_make(d):
        return pltpu.make_async_remote_copy(
            src_ref=lat_out.at[(d + 1) // 2], dst_ref=lat_in.at[(1 - d) // 2],
            send_sem=lat_send.at[(d + 1) // 2], recv_sem=lat_recv.at[(d + 1) // 2],
            device_id={"lat": li + d, "lon": lo}, device_id_type=MESH)

    def lon_make(role, d):
        if d == 0:
            first, size, dst = 0, clat, 0
        elif d == 1:
            first, size, dst = clat - HALO, HALO, clat + HALO
        else:
            first, size, dst = 0, HALO, clat
        return pltpu.make_async_remote_copy(
            src_ref=lon_out.at[role, :, pl.ds(first, size), :], dst_ref=lon_in.at[role, :, pl.ds(dst, size), :],
            send_sem=lon_send.at[role, d + 1], recv_sem=lon_recv.at[role, d + 1],
            device_id={"lat": li + d, "lon": lon_at(-1 if role == 0 else 1)}, device_id_type=MESH)

    start_wide(ask_make)
    start_wide(code_make)
    codes[n_lon + lo] = code_out[1]

    low = sub[:HALO] < STEPS
    flow_copy.wait()
    for f in range(2):
        for n in range(half):
            lat_out[1, f, n] = jnp.where(
                low, pltpu.roll(flow[f, n + half, clat - HALO:clat, :], STEPS, 0), flow[f, n, clat - HALO:clat, :])
            lat_out[0, f, n] = jnp.where(
                low, flow[f, n, 0:HALO, :], pltpu.roll(flow[f, n + half, 0:HALO, :], STEPS, 0))
    for d in (-1, 1):
        def send_lat(d=d):
            lat_make(d).start()
        guarded(d, send_lat)

    live_rows = sub < live
    w_rows = jnp.where(live_rows, weight[0], 0.0)
    wy_rows = w_rows * innov[0]
    stacked = jnp.concatenate([w_rows, wy_rows, jnp.zeros((clon - 2 * cap, clon), F32)], axis=0)
    columns = jnp.transpose(stacked)
    w_col = [columns[:, b:b + 1] for b in range(cap)]
    wy_col = [columns[:, cap + b:cap + b + 1] for b in range(cap)]

    def spread(rnd, u_cols):
        out = [jnp.sum(obs_v[b] * u_cols[b], axis=0, keepdims=True) for b in range(cap)]
        terms[rnd, n_lon + lo] = jnp.concatenate(out, axis=0)
        start_wide(term_make(rnd))

    obs_copy.wait()
    spread(0, wy_col)

    lane = lax.broadcasted_iota(jnp.int32, (1, clon), 1)
    group = lane // HALO

    def answer(d, j):
        if d == 0:
            first, size = 0, clat
        elif d == 1:
            first, size = clat - HALO, HALO
        else:
            first, size = 0, HALO
        slot = (d + 1) * n_lon + lon_at(j)

        def asked(o, s):
            if (d, j) == (0, 0):
                return ask_out[0, o * SLOT + s]
            return ask_in[slot, 0, o * SLOT + s]

        tile = jnp.zeros((size, clon), F32)
        for s in range(SLOT):
            lev = asked(lo, s)
            right, left = asked(lon_at(-1), s), asked(lon_at(1), s)
            for f in range(2):
                rows = flow[f, lev, first:first + size, :]
                if (d, j) == (0, 0):
                    main_in[f, lo, s, HALO:HALO + clat, :] = rows
                elif d == 0:
                    main_out[j, f, s] = rows
                else:
                    main_edge[(d + 1) // 2, j, f, s] = rows
                g = s * 2 + f
                moved = pltpu.roll(flow[f, right, first:first + size, :], g * HALO, 1)
                tile = jnp.where(group == g, moved, tile)
                g = (SLOT + s) * 2 + f
                moved = pltpu.roll(flow[f, left, first:first + size, :], (g + 1) * HALO, 1)
                tile = jnp.where(group == g, moved, tile)
        if (d, j) == (0, 0):
            strip_in[lo, HALO:HALO + clat, :] = tile
        else:
            if d == 0:
                strip_out[j] = tile
            else:
                strip_edge[(d + 1) // 2, j] = tile
            main_make(d, j, True).start()
            strip_make(d, j, True).start()

    recv_wide(ask_make)
    for d in (-1, 1, 0):
        def respond(d=d):
            for j in range(n_lon):
                if (d, j) != (0, 0):
                    answer(d, j)
        guarded(d, respond)
    answer(0, 0)

    lane_level = lane // width
    for f in range(2):
        right = jnp.zeros((clat, clon), F32)
        left = jnp.zeros((clat, clon), F32)
        for n in range(levels):
            rows = flow[f, n]
            right = jnp.where(lane_level == n, pltpu.roll(rows, n * width, 1), right)
            left = jnp.where(lane_level == n, pltpu.roll(rows, (n * width + width) % clon, 1), left)
        lon_out[0, f] = right
        lon_out[1, f] = left
    for d in (-1, 1, 0):
        def send_lon(d=d):
            for role in range(2):
                lon_make(role, d).start()
        guarded(d, send_lon)

    pad = codes.shape[0] - n_src
    none = jnp.full((n_lon, cap, clon), -1.0, F32)
    if pad:
        codes[n_src:] = jnp.full((pad, cap, clon), -1.0, F32)
        for rnd in range(3):
            terms[rnd, n_src:] = jnp.zeros((pad, cap, clon), F32)
    for d in (-1, 1):
        @pl.when(jnp.logical_not(exists(d)))
        def _(d=d):
            first = (d + 1) * n_lon
            codes[first:first + n_lon] = none
            for rnd in range(3):
                terms[rnd, first:first + n_lon] = jnp.zeros((n_lon, cap, clon), F32)
            lat0 = 0 if d == -1 else HALO + clat
            main_in[:, :, :, lat0:lat0 + HALO, :] = jnp.zeros((2, n_lon, SLOT, HALO, clon), F32)
            strip_in[:, lat0:lat0 + HALO, :] = jnp.zeros((n_lon, HALO, clon), F32)
            lat_in[(d + 1) // 2] = jnp.zeros((2, half, HALO, clon), F32)
            lon0 = clat + HALO if d == -1 else clat
            lon_in[:, :, lon0:lon0 + HALO, :] = jnp.zeros((2, 2, HALO, clon), F32)

    recv_wide(code_make)
    code_row = jnp.transpose(codes[...].reshape(n_blocks, clon))[0:1, :]

    def wide_tile(tile):
        return jnp.concatenate([tile] * (n_blocks // clon), axis=1) if n_blocks > clon else tile[:, :n_blocks]

    def matches(place_code):
        return jnp.where(place_code.astype(F32) == code_row, 1.0, 0.0).astype(BF16)

    window_rows = PAD_WIN * cap
    for part, shift in enumerate((0, n_lon - 1, 1)):
        tile = wide_tile(code_of(lax.rem(owner_tile + shift, n_lon), lat_tile))
        for d in range(0, PAD_WIN, 2):
            first = part * window_rows + d * cap
            hot[first:first + 2 * cap, :] = matches(jnp.concatenate([tile + (d - HALO), tile + (d + 1 - HALO)], axis=0))
    ring_row = lax.broadcasted_iota(jnp.int32, (ring, n_blocks), 0)
    ring_lat = jnp.where(ring_row < clat + STEPS, ring_row, ring_row - ring) + clat
    for part, shift in enumerate((0, n_lon - 1, 1)):
        lon_now = lon_at(shift)
        for n in range(0, levels, 2):
            pair = [ring_lat + ((n + k) * n_lon + lon_now) * span for k in range(2)]
            first = (part * levels + n) * ring
            dense_hot[first:first + 2 * ring, :] = matches(jnp.concatenate(pair, axis=0))

    middle = clon // 2
    last_lane = lane == clon - 1
    first_lane = lane == 0

    def lon_up(m, s):
        mr, sr = pltpu.roll(m, clon - 1, 1), pltpu.roll(s, clon - 1, 1)
        return jnp.where(last_lane, sr, mr), jnp.where(last_lane, mr, sr)

    def lon_down(m, s):
        mr, sr = pltpu.roll(m, 1, 1), pltpu.roll(s, 1, 1)
        return jnp.where(first_lane, sr, mr), jnp.where(first_lane, mr, sr)

    def load_window(rnd):
        field[...] = dot3(hot[...], terms[rnd].reshape(n_blocks, clon))

    recv_wide(term_make(0))
    load_window(0)

    recv_wide(strip_make)
    for o in range(n_lon):
        from_right, from_left = strip_in[(o + 1) % n_lon], strip_in[(o - 1) % n_lon]
        for s in range(SLOT):
            for f in range(2):
                g = s * 2 + f
                right = pltpu.roll(from_right, (clon - g * HALO) % clon, 1)
                g = (SLOT + s) * 2 + f
                left = pltpu.roll(from_left, (2 * clon - HALO - g * HALO) % clon, 1)
                side_in[f, o, s] = jnp.where(lane < middle, right, left)
    recv_wide(main_make)

    def gather(ref, f, d):
        tile = None
        for b in range(cap):
            line = ref[f, owners[b], slots[b], pl.ds(lats[b] + d, 1), :]
            tile = jnp.broadcast_to(line, (cap, clon)) if tile is None else jnp.where(sub == b, line, tile)
        return tile

    for d in range(WIN):
        for side, ref in enumerate((main_in, side_in)):
            if d in (0, WIN - 1):
                if side == 0:
                    c0 = gather(ref, 0, d)
                    win_rates[1 if d == 0 else 0, d, side] = jnp.maximum(-c0 if d == 0 else c0, 0.0)
                continue
            for k, value in enumerate(split_rates(gather(ref, 0, d), gather(ref, 1, d))):
                win_rates[k, d, side] = value

    def window_model():
        a, b, e, f, keep = range(5)

        def part(n, d):
            first = n * window_rows + d * cap
            return field[first:first + cap, :]

        main = {d: part(0, d) for d in range(WIN)}
        side = {d: jnp.where(lane < middle, part(2, d), part(1, d)) for d in range(1, WIN - 1)}
        for step in range(STEPS):
            a_main = {d: win_rates[a, d, 0] * main[d] for d in range(step + 2, WIN - step)}
            b_main = {d: win_rates[b, d, 0] * main[d] for d in range(step, WIN - step - 2)}
            a_side = {d: win_rates[a, d, 1] * side[d] for d in range(step + 3, WIN - step - 1)}
            b_side = {d: win_rates[b, d, 1] * side[d] for d in range(step + 1, WIN - step - 3)}
            new_main, new_side = {}, {}
            for d in range(step + 1, WIN - step - 1):
                up = lon_up(win_rates[e, d, 0] * main[d], win_rates[e, d, 1] * side[d])
                down = lon_down(win_rates[f, d, 0] * main[d], win_rates[f, d, 1] * side[d])
                new_main[d] = win_rates[keep, d, 0] * main[d] + a_main[d + 1] + b_main[d - 1] + up[0] + down[0]
                if step + 2 <= d < WIN - step - 2:
                    new_side[d] = win_rates[keep, d, 1] * side[d] + a_side[d + 1] + b_side[d - 1] + up[1] + down[1]
            main, side = new_main, new_side
        for d in list(main):
            lat_now = lat_tile + (li * clat + d - HALO)
            inside = (lat_now >= 0) & (lat_now < n_lat * clat)
            main[d] = jnp.where(inside, main[d], 0.0)
            if d in side:
                side[d] = jnp.where(inside, side[d], 0.0)
        for step in range(STEPS):
            reach = STEPS - 1 - step
            new_main, new_side = {}, {}
            for d in range(HALO - reach, HALO + reach + 1):
                down, up = lon_down(main[d], side[d]), lon_up(main[d], side[d])
                new_main[d] = (win_rates[keep, d, 0] * main[d] + win_rates[a, d, 0] * main[d - 1] + win_rates[b, d, 0] * main[d + 1]
                               + win_rates[e, d, 0] * down[0] + win_rates[f, d, 0] * up[0])
                if abs(d - HALO) < reach:
                    new_side[d] = (win_rates[keep, d, 1] * side[d] + win_rates[a, d, 1] * side[d - 1]
                                   + win_rates[b, d, 1] * side[d + 1] + win_rates[e, d, 1] * down[1] + win_rates[f, d, 1] * up[1])
            main, side = new_main, new_side
        seen = main[HALO]
        return [jnp.sum(obs_v[b] * seen[b:b + 1, :], axis=1, keepdims=True) for b in range(cap)]

    def recv_dense():
        for d in (-1, 1):
            def wait_lat(d=d):
                lat_make(d).wait_recv()
            guarded(-d, wait_lat)
        for d in (-1, 1, 0):
            def wait_lon(d=d):
                for role in range(2):
                    lon_make(role, d).wait_recv()
            guarded(-d, wait_lon)
        for f in range(2):
            for n in range(half):
                north, south = lat_in[1, f, n], lat_in[0, f, n]
                lat_halo[f, n] = jnp.where(low, north, south)
                lat_halo[f, n + half] = pltpu.roll(jnp.where(low, south, north), STEPS, 0)
            sides_in = []
            for role in range(2):
                edge = jnp.where(low, lon_in[role, f, clat:clat + HALO, :], lon_in[role, f, clat + HALO:, :])
                sides_in.append(jnp.concatenate([lon_in[role, f, 0:clat, :], edge], axis=0))
            for n in range(levels):
                right = pltpu.roll(sides_in[0], (clon - n * width) % clon, 1)
                left = pltpu.roll(sides_in[1], (2 * clon - width - n * width) % clon, 1)
                lon_halo[f, n] = jnp.where(lane < middle, right, left)

    def dense(rnd):
        flat = dot3(dense_hot[...], terms[rnd].reshape(n_blocks, clon))
        dense_field[...] = flat.reshape(3, levels, ring, clon)

        @pl.loop(0, levels, unroll=2)
        def _(n):
            rates = []
            for f in range(2):
                rates.append((jnp.concatenate([flow[f, n], lat_halo[f, n]], axis=0), lon_halo[f, n]))
            main_rates = split_rates(rates[0][0], rates[1][0])
            side_rates = split_rates(rates[0][1], rates[1][1])
            m = dense_field[0, n]
            s = jnp.where(lane < middle, dense_field[2, n], dense_field[1, n])
            for _ in range(STEPS):
                up = lon_up(main_rates[2] * m, side_rates[2] * s)
                down = lon_down(main_rates[3] * m, side_rates[3] * s)
                m, s = (
                    (r[4] * x + pltpu.roll(r[0] * x, ring - 1, 0) + pltpu.roll(r[1] * x, 1, 0) + up[k] + down[k])
                    for k, (r, x) in enumerate(((main_rates, m), (side_rates, s))))
            parts[rnd, n] = m[0:clat]

    def red_lon_make(j, out):
        return pltpu.make_async_remote_copy(
            src_ref=red_lon.at[lo], dst_ref=red_lon.at[lo if out else lon_at(-j)],
            send_sem=red_lon_send.at[j], recv_sem=red_lon_recv.at[j],
            device_id={"lat": li, "lon": lon_at(j)}, device_id_type=MESH)

    def red_lat_make(j, out):
        at = li if out else lax.rem(li - j + n_lat, n_lat)
        return pltpu.make_async_remote_copy(
            src_ref=red_lat.at[li], dst_ref=red_lat.at[at],
            send_sem=red_lat_send.at[j], recv_sem=red_lat_recv.at[j],
            device_id={"lat": lax.rem(li + j, n_lat), "lon": lo}, device_id_type=MESH)

    def column_total(xs, ys):
        return jnp.sum(sum(x * y for x, y in zip(xs, ys)), axis=0, keepdims=True)

    p1 = window_model()
    u1 = [w_col[b] * p1[b] for b in range(cap)]
    spread(1, u1)
    recv_dense()
    dense(0)
    recv_wide(term_make(1))
    load_window(1)
    g1 = window_model()
    u2 = [w_col[b] * g1[b] for b in range(cap)]
    tile = jnp.zeros((8, clon), F32)
    for n, value in enumerate((column_total(wy_col, p1), column_total(u1, p1), column_total(u1, g1), column_total(u2, g1))):
        tile = jnp.where(sub == n, value, tile)
    red_lon[lo] = tile
    for j in range(1, n_lon):
        red_lon_make(j, True).start()
    spread(2, u2)
    dense(1)
    for j in range(1, n_lon):
        red_lon_make(j, False).wait_recv()
    red_lat[li] = jnp.sum(red_lon[...], axis=0)

    @pl.loop(1, n_lat)
    def _(j):
        red_lat_make(j, True).start()

    recv_wide(term_make(2))
    dense(2)

    @pl.loop(1, n_lat)
    def _(j):
        red_lat_make(j, False).wait_recv()

    sums = jnp.sum(red_lat[...], axis=0)
    bb, s1, tt, s3 = (sums[n:n + 1, 0:1] for n in range(4))
    scale = bb + s1
    alpha1, left1 = bb / scale, s1 / scale
    rr = left1 * (left1 * bb - alpha1 * s1) - alpha1 * (left1 * s1 - alpha1 * tt)
    sr1 = left1 * s1 - alpha1 * tt
    srr = left1 * sr1 - alpha1 * (left1 * tt - alpha1 * s3)
    beta = rr / bb
    curve = rr + beta * beta * bb + (srr + 2.0 * beta * sr1 + beta * beta * s1)
    alpha2 = rr / curve
    mix = left1 + beta
    inc_b, inc_t = alpha1 + alpha2 * mix, -alpha2 * alpha1
    res_b, res_t, res_2 = left1 - alpha2 * mix, -alpha1 - alpha2 * (mix - alpha1), alpha2 * alpha1
    for n in range(levels):
        b0, t1, t2 = parts[0, n], parts[1, n], parts[2, n]
        inc_out[n] = inc_b * b0 + inc_t * t1
        res_out[n] = res_b * b0 + res_t * t1 + res_2 * t2

    for make in (code_make, ask_make, main_make, strip_make, term_make(0), term_make(1), term_make(2)):
        done_wide(make)
    for d in (-1, 1):
        def sent_lat(d=d):
            lat_make(d).wait_send()
        guarded(d, sent_lat)
    for d in (-1, 1, 0):
        def sent_lon(d=d):
            for role in range(2):
                lon_make(role, d).wait_send()
        guarded(d, sent_lon)
    for j in range(1, n_lon):
        red_lon_make(j, True).wait_send()

    @pl.loop(1, n_lat)
    def _(j):
        red_lat_make(j, True).wait_send()


def shards(n_lat, n_lon, courant, obs_matrix, obs_weight, innovation, block_owner, block_row, block_count):
    _, levels, clat, clon = courant.shape
    cap = block_row.shape[1]
    ring = clat + HALO
    rows = clat + 2 * HALO
    unit = clon // cap
    src_pad = -(-3 * n_lon // unit) * unit
    n_blocks = src_pad * cap
    vmem = pl.BlockSpec(memory_space=pltpu.VMEM)
    hbm = pl.BlockSpec(memory_space=pl.ANY)
    dma = pltpu.SemaphoreType.DMA

    def f32(*shape):
        return pltpu.VMEM(shape, F32)

    def i32(*shape):
        return pltpu.SMEM(shape, jnp.int32)

    field = jax.ShapeDtypeStruct((levels, clat, clon), F32)
    return pl.pallas_call(
        functools.partial(kernel, n_lat, n_lon),
        out_shape=(field, field),
        in_specs=[hbm] * 7,
        out_specs=(vmem, vmem),
        scratch_shapes=[
            f32(2, levels, clat, clon),
            f32(cap, clon, clon),
            f32(3, src_pad, cap, clon),
            f32(src_pad, cap, clon),
            f32(3, cap, clon),
            pltpu.VMEM((3 * PAD_WIN * cap, n_blocks), BF16),
            pltpu.VMEM((3 * levels * ring, n_blocks), BF16),
            f32(3 * PAD_WIN * cap, clon),
            f32(3, levels, ring, clon),
            f32(n_lon, 2, SLOT, clat, clon),
            f32(2, n_lon, 2, SLOT, HALO, clon),
            f32(n_lon, clat, clon),
            f32(2, n_lon, HALO, clon),
            f32(2, n_lon, SLOT, rows, clon),
            f32(n_lon, rows, clon),
            f32(2, n_lon, SLOT, rows, clon),
            f32(5, WIN, 2, cap, clon),
            f32(2, 2, levels // 2, HALO, clon),
            f32(2, 2, levels // 2, HALO, clon),
            f32(2, 2, clat, clon),
            f32(2, 2, rows, clon),
            f32(2, levels, HALO, clon),
            f32(2, levels, ring, clon),
            f32(3, levels, clat, clon),
            f32(n_lon, 8, clon),
            f32(n_lat, 8, clon),
            i32(1, n_lon * SLOT),
            i32(3 * n_lon, 1, n_lon * SLOT),
            dma, dma,
            dma((7, 3, n_lon)), dma((7, 3, n_lon)),
            dma((2,)), dma((2,)),
            dma((2, 3)), dma((2, 3)),
            dma((n_lon,)), dma((n_lon,)),
            dma((n_lat,)), dma((n_lat,)),
            f32(1, cap, clon), f32(1, cap, clon),
            i32(1, cap), i32(1, cap), i32(1, 1),
            dma((5,)),
        ],
        compiler_params=pltpu.CompilerParams(collective_id=0, has_side_effects=True),
    )(courant, obs_matrix, obs_weight, innovation, block_owner[:, :, 0], block_row, block_count)


def solution(mesh):
    placed = (
        P(None, None, "lat", "lon"),
        P("lat", "lon", None, None),
        P("lat", "lon", None),
        P("lat", "lon", None),
        P("lat", "lon", None),
        P("lat", "lon"),
        P("lat", "lon"),
    )
    return jax.shard_map(
        functools.partial(shards, mesh.shape["lat"], mesh.shape["lon"]),
        mesh=mesh,
        in_specs=placed,
        out_specs=(P(None, "lat", "lon"), P(None, "lat", "lon")),
        check_vma=False,
    )
```

```python
import functools

import jax
import jax.numpy as jnp
from jax import lax
from jax.experimental import pallas as pl
from jax.experimental.pallas import tpu as pltpu
from jax.sharding import PartitionSpec as P

STEPS = 4
HALO = 2 * STEPS
SLOT = 2
WIN = 2 * HALO + 1
PAD_WIN = WIN + 1
MESH = pl.DeviceIdType.MESH
F32 = jnp.float32
BF16 = jnp.bfloat16


def split3(x):
    hi = x.astype(BF16)
    rest = x - hi.astype(F32)
    mid = rest.astype(BF16)
    low = (rest - mid.astype(F32)).astype(BF16)
    return hi, mid, low


def dot3(onehot, parts):
    total = None
    for part in parts:
        term = jnp.dot(onehot, part, preferred_element_type=F32)
        total = term if total is None else total + term
    return total


def split_rates(c0, c1):
    a, b = jnp.maximum(c0, 0.0), jnp.maximum(-c0, 0.0)
    e, f = jnp.maximum(c1, 0.0), jnp.maximum(-c1, 0.0)
    return a, b, e, f, 1.0 - a - b - e - f


def kernel(
    n_lat, n_lon,
    courant, courant_flat, obs, weight_in, innov_in, owner_in, row_in, count_in,
    inc_out, res_out,
    flow, flow_flat, obs_v, terms, codes, code_out, hot_main, hot_side, dense_main, dense_side, field, dense_field,
    main_out, main_edge, strip_out, strip_edge, main_in, strip_in, side_in,
    win_rates, lat_out, lat_in, lon_out, lon_in, dense_rates, weight_wide, parts, red_lon, red_lat,
    ask_out, ask_in,
    obs_sem, flow_sem, flat_sem, wide_send, wide_recv, lat_send, lat_recv, lon_send, lon_recv, red_sems,
    weight, innov, owner, row, count, input_sems,
):
    li = lax.axis_index("lat")
    lo = lax.axis_index("lon")
    clon = flow_flat.shape[1]
    cap = obs_v.shape[0]
    tiles, clat = parts.shape[1:3]
    levels = tiles * 8
    n_src = 3 * n_lon
    n_blocks = terms.shape[1] * cap
    span = 4 * clat
    ring = clat + 2 * STEPS
    width = clon // clat

    small = [
        pltpu.make_async_copy(src, dst, input_sems.at[n])
        for n, (src, dst) in enumerate((
            (owner_in, owner), (row_in, row), (count_in, count), (weight_in, weight), (innov_in, innov)))
    ]
    for copy in small:
        copy.start()
    flow_copy = pltpu.make_async_copy(courant, flow, flow_sem)
    flow_copy.start()
    flat_copy = pltpu.make_async_copy(courant_flat, flow_flat, flat_sem)
    obs_copy = pltpu.make_async_copy(obs.at[0], obs_v, obs_sem)
    obs_copy.start()
    flat_copy.start()

    def exists(d):
        return (li + d >= 0) & (li + d < n_lat)

    def guarded(d, run):
        if d == 0:
            run()
        else:
            pl.when(exists(d))(run)

    def lon_at(j):
        return lax.rem(lo + j + n_lon, n_lon)

    barrier = pltpu.get_barrier_semaphore()

    def greet(lat, lon):
        pl.semaphore_signal(barrier, inc=1, device_id={"lat": lat, "lon": lon}, device_id_type=MESH)

    @pl.loop(1, n_lat)
    def _(j):
        greet(lax.rem(li + j, n_lat), lo)

    for d in (-1, 1):
        def hello(d=d):
            for j in range(1, n_lon):
                greet(li + d, lon_at(j))
        guarded(d, hello)
    for j in range(1, n_lon):
        greet(li, lon_at(j))

    for copy in small:
        copy.wait()

    sub = lax.broadcasted_iota(jnp.int32, (cap, clon), 0)
    live = count[0, 0]
    owners = [owner[0, b] for b in range(cap)]
    levs = [lax.div(row[0, b], jnp.int32(clat)) for b in range(cap)]
    lats = [row[0, b] - levs[b] * clat for b in range(cap)]
    slots = []
    for b in range(cap):
        s = jnp.int32(0)
        for c in range(b):
            s = s + (owners[c] == owners[b]).astype(jnp.int32)
        slots.append(jnp.minimum(s, SLOT - 1))
    for o in range(n_lon):
        for s in range(SLOT):
            lev = jnp.int32(0)
            for b in range(cap):
                lev = jnp.where((owners[b] == o) & (slots[b] == s), levs[b], lev)
            ask_out[0, o * SLOT + s] = lev

    def column(values):
        tile = jnp.full((cap, clon), values[0], jnp.int32)
        for b in range(1, cap):
            tile = jnp.where(sub == b, values[b], tile)
        return tile

    level_tile, lat_tile, owner_tile = column(levs), column(lats), column(owners)

    def code_of(owner_now, lat_now):
        return (level_tile * n_lon + owner_now) * span + lat_now + clat

    lane = lax.broadcasted_iota(jnp.int32, (1, clon), 1)
    middle = clon // 2
    code_line = jnp.full((1, clon), -1, jnp.int32)
    for b in range(cap):
        code = (levs[b] * n_lon + owners[b]) * span + lats[b] + clat
        code_line = jnp.where(lane == b, jnp.where(b < live, code, -4 * span), code_line)
    for d in (-1, 0, 1):
        code_out[d + 1] = (code_line - clat * d).astype(F32)

    sides = (li > 0).astype(jnp.int32) + (li < n_lat - 1).astype(jnp.int32)
    pl.semaphore_wait(barrier, (n_lon - 1) + (n_lat - 1) + sides * (n_lon - 1))

    def wide(kind, d, j, src, dst):
        return pltpu.make_async_remote_copy(
            src_ref=src, dst_ref=dst,
            send_sem=wide_send.at[kind, d + 1], recv_sem=wide_recv.at[kind, d + 1],
            device_id={"lat": li + d, "lon": lon_at(j)}, device_id_type=MESH,
        )

    def slot_of(d, j, out):
        return (1 - d) * n_lon + (lo if out else lon_at(-j))

    def several(d):
        return n_lon - 1 if d == 0 else n_lon

    def start_wide(make):
        for d in (-1, 1, 0):
            def run(d=d):
                for j in (2, 3, 1, 0) if n_lon == 4 else range(n_lon):
                    if (d, j) != (0, 0):
                        make(d, j).start()
            guarded(d, run)

    def recv_wide(whole):
        for d in (-1, 1, 0):
            def run(d=d):
                kind, _, into = whole(d)
                wide(kind, d, 1, into, into).wait_recv()
            guarded(-d, run)

    def done_wide(whole):
        for d in (-1, 1, 0):
            def run(d=d):
                kind, out, _ = whole(d)
                wide(kind, d, 1, out, out).wait_send()
            guarded(d, run)

    def code_make(d, j):
        return wide(0, d, j, code_out.at[d + 1], codes.at[slot_of(d, j, True)])

    def code_all(d):
        ref = codes.at[pl.ds((1 - d) * n_lon, several(d))]
        return 0, ref, ref

    def ask_make(d, j):
        return wide(1, d, j, ask_out, ask_in.at[slot_of(d, j, True)])

    def ask_all(d):
        ref = ask_in.at[pl.ds((1 - d) * n_lon, several(d))]
        return 1, ref, ref

    def place(d):
        return (HALO, clat) if d == 0 else ((0, HALO) if d == 1 else (HALO + clat, HALO))

    def main_make(d, j):
        first, size = place(d)
        src = main_out.at[j] if d == 0 else main_edge.at[(d + 1) // 2, j]
        return wide(2, d, j, src, main_in.at[:, lo, :, pl.ds(first, size), :])

    def main_all(d):
        first, size = place(d)
        src = main_out.at[pl.ds(1, n_lon - 1)] if d == 0 else main_edge.at[(d + 1) // 2]
        return 2, src, main_in.at[:, pl.ds(0, several(d)), :, pl.ds(first, size), :]

    def strip_make(d, j):
        first, size = place(d)
        src = strip_out.at[j] if d == 0 else strip_edge.at[(d + 1) // 2, j]
        return wide(3, d, j, src, strip_in.at[lo, pl.ds(first, size), :])

    def strip_all(d):
        first, size = place(d)
        src = strip_out.at[pl.ds(1, n_lon - 1)] if d == 0 else strip_edge.at[(d + 1) // 2]
        return 3, src, strip_in.at[pl.ds(0, several(d)), pl.ds(first, size), :]

    def term_make(rnd):
        def make(d, j):
            return wide(4 + rnd, d, j, terms.at[rnd, n_lon + lo], terms.at[rnd, slot_of(d, j, True)])
        return make

    def term_all(rnd):
        def whole(d):
            ref = terms.at[rnd, pl.ds((1 - d) * n_lon, several(d))]
            return 4 + rnd, ref, ref
        return whole

    def lat_make(d):
        return pltpu.make_async_remote_copy(
            src_ref=lat_out.at[(d + 1) // 2], dst_ref=lat_in.at[(1 - d) // 2],
            send_sem=lat_send.at[(d + 1) // 2], recv_sem=lat_recv.at[(d + 1) // 2],
            device_id={"lat": li + d, "lon": lo}, device_id_type=MESH)

    def lon_make(role, d):
        return pltpu.make_async_remote_copy(
            src_ref=lon_out.at[role], dst_ref=lon_in.at[role, 1 - d],
            send_sem=lon_send.at[role, d + 1], recv_sem=lon_recv.at[role, d + 1],
            device_id={"lat": li + d, "lon": lon_at(-1 if role == 0 else 1)}, device_id_type=MESH)

    start_wide(ask_make)
    start_wide(code_make)
    codes[n_lon + lo] = code_out[1]

    flow_copy.wait()

    def flow_rows(f, lev, first, size):
        return flow[f, lev, first:first + size, :]

    def flow_levels(f, tile, lat):
        return flow_flat[pl.ds((f * levels + tile * 8) * clat + lat, 8, stride=clat), :]

    live_rows = sub < live
    w_rows = jnp.where(live_rows, weight[0], 0.0)
    wy_rows = w_rows * innov[0]
    stacked = jnp.concatenate([w_rows, wy_rows, jnp.zeros((clon - 2 * cap, clon), F32)], axis=0)
    columns = jnp.transpose(stacked)
    for b in range(cap):
        weight_wide[b] = jnp.broadcast_to(columns[:, b:b + 1], (clon, clon))
    wy_col = [columns[:, cap + b:cap + b + 1] for b in range(cap)]

    def spread(rnd, u_cols):
        out = [jnp.sum(obs_v[b] * u_cols[b], axis=0, keepdims=True) for b in range(cap)]
        terms[rnd, n_lon + lo] = jnp.concatenate(out, axis=0)
        start_wide(term_make(rnd))

    obs_copy.wait()
    spread(0, wy_col)

    group = lane // HALO

    def answer(d, j):
        if d == 0:
            first, size = 0, clat
        elif d == 1:
            first, size = clat - HALO, HALO
        else:
            first, size = 0, HALO
        slot = (d + 1) * n_lon + lon_at(j)

        def asked(o, s):
            if (d, j) == (0, 0):
                return ask_out[0, o * SLOT + s]
            return ask_in[slot, 0, o * SLOT + s]

        tile = jnp.zeros((size, clon), F32)
        for s in range(SLOT):
            lev = asked(lo, s)
            right, left = asked(lon_at(-1), s), asked(lon_at(1), s)
            for f in range(2):
                rows = flow_rows(f, lev, first, size)
                if (d, j) == (0, 0):
                    main_in[f, lo, s, HALO:HALO + clat, :] = rows
                elif d == 0:
                    main_out[j, f, s] = rows
                else:
                    main_edge[(d + 1) // 2, j, f, s] = rows
                g = s * 2 + f
                moved = pltpu.roll(flow_rows(f, right, first, size), g * HALO, 1)
                tile = jnp.where(group == g, moved, tile)
                g = (SLOT + s) * 2 + f
                moved = pltpu.roll(flow_rows(f, left, first, size), (g + 1) * HALO, 1)
                tile = jnp.where(group == g, moved, tile)
        if (d, j) == (0, 0):
            strip_in[lo, HALO:HALO + clat, :] = tile
        else:
            if d == 0:
                strip_out[j] = tile
            else:
                strip_edge[(d + 1) // 2, j] = tile
            main_make(d, j).start()
            strip_make(d, j).start()

    recv_wide(ask_all)
    for d in (-1, 1, 0):
        def respond(d=d):
            for j in range(n_lon):
                if (d, j) != (0, 0):
                    answer(d, j)
        guarded(d, respond)
    answer(0, 0)

    def send_dense():
        flat_copy.wait()
        for f in range(2):
            for t in range(tiles):
                for k in range(STEPS):
                    lat_out[0, f, k, t] = flow_levels(f, t, k)
                    lat_out[1, f, k, t] = flow_levels(f, t, clat - STEPS + k)
        for d in (-1, 1):
            def send_lat(d=d):
                lat_make(d).start()
            guarded(d, send_lat)
        lane_lat = lane // width
        for f in range(2):
            for t in range(tiles):
                right = jnp.zeros((8, clon), F32)
                left = jnp.zeros((8, clon), F32)
                for n in range(clat):
                    rows = flow_levels(f, t, n)
                    right = jnp.where(lane_lat == n, pltpu.roll(rows, n * width, 1), right)
                    left = jnp.where(lane_lat == n, pltpu.roll(rows, (n * width + width) % clon, 1), left)
                lon_out[0, f, t] = right
                lon_out[1, f, t] = left
        for d in (-1, 1, 0):
            def send_lon(d=d):
                for role in range(2):
                    lon_make(role, d).start()
            guarded(d, send_lon)

    pad = terms.shape[1] - n_src
    if pad:
        for rnd in range(3):
            terms[rnd, n_src:] = jnp.zeros((pad, cap, clon), F32)
    for d in (-1, 1):
        @pl.when(jnp.logical_not(exists(d)))
        def _(d=d):
            first = (d + 1) * n_lon
            codes[first:first + n_lon] = jnp.full((n_lon, 1, clon), -4.0 * span, F32)
            for rnd in range(3):
                terms[rnd, first:first + n_lon] = jnp.zeros((n_lon, cap, clon), F32)
            lat0 = 0 if d == -1 else HALO + clat
            main_in[:, :, :, lat0:lat0 + HALO, :] = jnp.zeros((2, n_lon, SLOT, HALO, clon), F32)
            strip_in[:, lat0:lat0 + HALO, :] = jnp.zeros((n_lon, HALO, clon), F32)
            lat_in[(d + 1) // 2] = jnp.zeros((2, STEPS, tiles, 8, clon), F32)
            lon_in[:, d + 1] = jnp.zeros((2, 2, tiles, 8, clon), F32)

    recv_wide(code_all)
    code_parts = []
    for first in range(0, n_blocks, clon):
        line = jnp.full((1, clon), -4.0 * span, F32)
        for k in range(clon // cap):
            slot = first // cap + k
            if slot < n_src:
                line = jnp.where(lane // cap == k, pltpu.roll(codes[slot], k * cap, 1), line)
        code_parts.append(line)
    code_row = code_parts[0] if len(code_parts) == 1 else jnp.concatenate(code_parts, axis=1)

    def wide_tile(tile):
        return jnp.concatenate([tile] * (n_blocks // clon), axis=1) if n_blocks > clon else tile[:, :n_blocks]

    def matches(place_code):
        return jnp.where(place_code.astype(F32) == code_row, 1.0, 0.0).astype(BF16)

    for part, shift in enumerate((0, n_lon - 1, 1)):
        tile = wide_tile(code_of(lax.rem(owner_tile + shift, n_lon), lat_tile))
        for d in range(0, PAD_WIN, 2):
            rows = matches(jnp.concatenate([tile + (d - HALO), tile + (d + 1 - HALO)], axis=0))
            if part == 0:
                hot_main[d * cap:(d + 2) * cap, :] = rows
            else:
                hot_side[d * cap:(d + 2) * cap, (part - 1) * n_blocks:part * n_blocks] = rows

    def build_dense():
        lev_codes = lax.broadcasted_iota(jnp.int32, (levels, n_blocks), 0) * (n_lon * span)
        for part, shift in enumerate((0, n_lon - 1, 1)):
            for d in range(ring):
                rows = matches(lev_codes + (lon_at(shift) * span + (d - STEPS + clat)))
                if part == 0:
                    dense_main[d * levels:(d + 1) * levels, :] = rows
                else:
                    dense_side[d * levels:(d + 1) * levels, (part - 1) * n_blocks:part * n_blocks] = rows

    last_lane = lane == clon - 1
    first_lane = lane == 0

    def lon_up(m, s):
        mr, sr = pltpu.roll(m, clon - 1, 1), pltpu.roll(s, clon - 1, 1)
        return jnp.where(last_lane, sr, mr), jnp.where(last_lane, mr, sr)

    def lon_down(m, s):
        mr, sr = pltpu.roll(m, 1, 1), pltpu.roll(s, 1, 1)
        return jnp.where(first_lane, sr, mr), jnp.where(first_lane, mr, sr)

    def term_parts(rnd):
        flat = terms[rnd].reshape(n_blocks, clon)
        halves = [jnp.where(lane >= middle, flat, 0.0), jnp.where(lane < middle, flat, 0.0)]
        return split3(flat), split3(jnp.concatenate(halves, axis=0))

    def load_window(rnd):
        main_parts, side_parts = term_parts(rnd)
        field[0] = dot3(hot_main[...], main_parts).reshape(PAD_WIN, cap, clon)
        field[1] = dot3(hot_side[...], side_parts).reshape(PAD_WIN, cap, clon)

    def adjoint(rate, main, side, first, last):
        a, b, e, f, keep = range(5)
        for _ in range(STEPS):
            a_main = {d: rate(a, 0, d) * main[d] for d in range(first + 2, last + 1)}
            b_main = {d: rate(b, 0, d) * main[d] for d in range(first, last - 1)}
            a_side = {d: rate(a, 1, d) * side[d] for d in range(first + 3, last)}
            b_side = {d: rate(b, 1, d) * side[d] for d in range(first + 1, last - 2)}
            new_main, new_side = {}, {}
            for d in range(first + 1, last):
                up = lon_up(rate(e, 0, d) * main[d], rate(e, 1, d) * side[d])
                down = lon_down(rate(f, 0, d) * main[d], rate(f, 1, d) * side[d])
                new_main[d] = rate(keep, 0, d) * main[d] + a_main[d + 1] + b_main[d - 1] + up[0] + down[0]
                if first + 2 <= d < last - 1:
                    new_side[d] = rate(keep, 1, d) * side[d] + a_side[d + 1] + b_side[d - 1] + up[1] + down[1]
            main, side = new_main, new_side
            first, last = first + 1, last - 1
        return main, side

    recv_wide(term_all(0))
    load_window(0)

    recv_wide(strip_all)
    for o in range(n_lon):
        from_right, from_left = strip_in[(o + 1) % n_lon], strip_in[(o - 1) % n_lon]
        for s in range(SLOT):
            for f in range(2):
                g = s * 2 + f
                right = pltpu.roll(from_right, (clon - g * HALO) % clon, 1)
                g = (SLOT + s) * 2 + f
                left = pltpu.roll(from_left, (2 * clon - HALO - g * HALO) % clon, 1)
                side_in[f, o, s] = jnp.where(lane < middle, right, left)
    recv_wide(main_all)

    def gather(ref, f, d):
        tile = None
        for b in range(cap):
            line = ref[f, owners[b], slots[b], pl.ds(lats[b] + d, 1), :]
            tile = jnp.broadcast_to(line, (cap, clon)) if tile is None else jnp.where(sub == b, line, tile)
        return tile

    for d in range(WIN):
        for side, ref in enumerate((main_in, side_in)):
            if d in (0, WIN - 1):
                if side == 0:
                    c0 = gather(ref, 0, d)
                    win_rates[1 if d == 0 else 0, d, side] = jnp.maximum(-c0 if d == 0 else c0, 0.0)
                continue
            for k, value in enumerate(split_rates(gather(ref, 0, d), gather(ref, 1, d))):
                win_rates[k, d, side] = value

    def window_model():
        a, b, e, f, keep = range(5)
        main = {d: field[0, d] for d in range(WIN)}
        side = {d: field[1, d] for d in range(1, WIN - 1)}
        main, side = adjoint(lambda k, n, d: win_rates[k, d, n], main, side, 0, WIN - 1)
        for d in list(main):
            lat_now = lat_tile + (li * clat + d - HALO)
            inside = (lat_now >= 0) & (lat_now < n_lat * clat)
            main[d] = jnp.where(inside, main[d], 0.0)
            if d in side:
                side[d] = jnp.where(inside, side[d], 0.0)
        for step in range(STEPS):
            reach = STEPS - 1 - step
            new_main, new_side = {}, {}
            for d in range(HALO - reach, HALO + reach + 1):
                down, up = lon_down(main[d], side[d]), lon_up(main[d], side[d])
                new_main[d] = (win_rates[keep, d, 0] * main[d] + win_rates[a, d, 0] * main[d - 1] + win_rates[b, d, 0] * main[d + 1]
                               + win_rates[e, d, 0] * down[0] + win_rates[f, d, 0] * up[0])
                if abs(d - HALO) < reach:
                    new_side[d] = (win_rates[keep, d, 1] * side[d] + win_rates[a, d, 1] * side[d - 1]
                                   + win_rates[b, d, 1] * side[d + 1] + win_rates[e, d, 1] * down[1] + win_rates[f, d, 1] * up[1])
            main, side = new_main, new_side
        seen = main[HALO]
        return [jnp.sum(obs_v[b] * seen[b:b + 1, :], axis=1, keepdims=True) for b in range(cap)]

    def recv_dense():
        for d in (-1, 1):
            def wait_lat(d=d):
                lat_make(d).wait_recv()
            guarded(-d, wait_lat)
        for d in (-1, 1, 0):
            def wait_lon(d=d):
                for role in range(2):
                    lon_make(role, d).wait_recv()
            guarded(-d, wait_lon)
        for t in range(tiles):
            for d in range(ring):
                lat = d - STEPS
                if lat < 0:
                    main = [lat_in[0, f, d, t] for f in range(2)]
                    slot = 0
                elif lat >= clat:
                    main = [lat_in[1, f, lat - clat, t] for f in range(2)]
                    slot = 2
                else:
                    main = [flow_levels(f, t, lat) for f in range(2)]
                    slot = 1
                at = lat % clat * width
                side = [
                    jnp.where(lane < middle, pltpu.roll(lon_in[0, slot, f, t], (clon - at) % clon, 1),
                              pltpu.roll(lon_in[1, slot, f, t], (2 * clon - width - at) % clon, 1))
                    for f in range(2)
                ]
                for n, pair in enumerate((main, side)):
                    for k, value in enumerate(split_rates(*pair)):
                        dense_rates[k, n, t, d] = value

    def dense(rnd):
        main_parts, side_parts = term_parts(rnd)
        dense_field[0] = dot3(dense_main[...], main_parts).reshape(ring, tiles, 8, clon)
        dense_field[1] = dot3(dense_side[...], side_parts).reshape(ring, tiles, 8, clon)

        @pl.loop(0, tiles)
        def _(t):
            main = {d: dense_field[0, d, t] for d in range(ring)}
            side = {d: dense_field[1, d, t] for d in range(1, ring - 1)}
            main, _ = adjoint(lambda k, n, d: dense_rates[k, n, t, d], main, side, 0, ring - 1)
            for lat in range(clat):
                parts[rnd, t, lat] = main[lat + STEPS]

    def red_lon_make(j):
        return pltpu.make_async_remote_copy(
            src_ref=red_lon.at[lo], dst_ref=red_lon.at[lo],
            send_sem=red_sems.at[0], recv_sem=red_sems.at[1],
            device_id={"lat": li, "lon": lon_at(j)}, device_id_type=MESH)

    def red_lat_make(j):
        return pltpu.make_async_remote_copy(
            src_ref=red_lat.at[li], dst_ref=red_lat.at[li],
            send_sem=red_sems.at[2], recv_sem=red_sems.at[3],
            device_id={"lat": lax.rem(li + j, n_lat), "lon": lo}, device_id_type=MESH)

    def red_all(ref, size, n):
        whole = ref.at[pl.ds(0, size)]
        return pltpu.make_async_remote_copy(
            src_ref=whole, dst_ref=whole, send_sem=red_sems.at[n], recv_sem=red_sems.at[n + 1],
            device_id={"lat": li, "lon": lon_at(1)}, device_id_type=MESH)

    def packed(cols):
        tile = jnp.zeros((clon, clon), F32)
        for b in range(cap):
            tile = jnp.where(lane == b, cols[b], tile)
        return tile

    p1 = window_model()
    spread(1, [weight_wide[b] * p1[b] for b in range(cap)])
    send_dense()
    build_dense()
    recv_wide(term_all(1))
    load_window(1)
    g1 = window_model()
    spread(2, [weight_wide[b] * g1[b] for b in range(cap)])
    p_all, g_all = packed(p1), packed(g1)
    u_all = columns * p_all
    tile = jnp.zeros((8, clon), F32)
    for n, value in enumerate((pltpu.roll(columns, clon - cap, 1) * p_all, u_all * p_all, u_all * g_all, columns * g_all * g_all)):
        tile = jnp.where(sub == n, jnp.sum(value, axis=0, keepdims=True), tile)
    red_lon[lo] = tile
    for j in range(1, n_lon):
        red_lon_make(j).start()
    recv_dense()
    dense(0)
    red_all(red_lon, n_lon - 1, 0).wait_recv()
    red_lat[li] = jnp.sum(red_lon[...], axis=0)

    @pl.loop(1, n_lat)
    def _(j):
        red_lat_make(j).start()

    dense(1)
    recv_wide(term_all(2))
    dense(2)
    red_all(red_lat, n_lat - 1, 2).wait_recv()

    sums = jnp.sum(jnp.sum(red_lat[...], axis=0), axis=1, keepdims=True)
    bb, s1, tt, s3 = (sums[n:n + 1] for n in range(4))
    scale = bb + s1
    alpha1, left1 = bb / scale, s1 / scale
    rr = left1 * (left1 * bb - alpha1 * s1) - alpha1 * (left1 * s1 - alpha1 * tt)
    sr1 = left1 * s1 - alpha1 * tt
    srr = left1 * sr1 - alpha1 * (left1 * tt - alpha1 * s3)
    beta = rr / bb
    curve = rr + beta * beta * bb + (srr + 2.0 * beta * sr1 + beta * beta * s1)
    alpha2 = rr / curve
    mix = left1 + beta
    inc_b, inc_t = alpha1 + alpha2 * mix, -alpha2 * alpha1
    res_b, res_t, res_2 = left1 - alpha2 * mix, -alpha1 - alpha2 * (mix - alpha1), alpha2 * alpha1
    for t in range(tiles):
        for lat in range(clat):
            b0, t1, t2 = (parts[rnd, t, lat] for rnd in range(3))
            rows = pl.ds(t * 8 * clat + lat, 8, stride=clat)
            inc_out[rows, :] = inc_b * b0 + inc_t * t1
            res_out[rows, :] = res_b * b0 + res_t * t1 + res_2 * t2

    for whole in (code_all, ask_all, main_all, strip_all, term_all(0), term_all(1), term_all(2)):
        done_wide(whole)
    for d in (-1, 1):
        def sent_lat(d=d):
            lat_make(d).wait_send()
        guarded(d, sent_lat)
    for d in (-1, 1, 0):
        def sent_lon(d=d):
            for role in range(2):
                lon_make(role, d).wait_send()
        guarded(d, sent_lon)
    red_all(red_lon, n_lon - 1, 0).wait_send()
    red_all(red_lat, n_lat - 1, 2).wait_send()


def store_kernel(inc, res, inc_out, res_out, sems):
    pairs = ((inc, inc_out), (res, res_out))
    copies = [pltpu.make_async_copy(src, dst, sems.at[n]) for n, (src, dst) in enumerate(pairs)]
    for copy in copies:
        copy.start()
    for copy in copies:
        copy.wait()


def shards(n_lat, n_lon, courant, obs_matrix, obs_weight, innovation, block_owner, block_row, block_count):
    _, levels, clat, clon = courant.shape
    cap = block_row.shape[1]
    tiles = levels // 8
    ring = clat + 2 * STEPS
    rows = clat + 2 * HALO
    unit = clon // cap
    src_pad = -(-3 * n_lon // unit) * unit
    n_blocks = src_pad * cap
    anywhere = pl.BlockSpec(memory_space=pl.ANY)
    dma = pltpu.SemaphoreType.DMA

    def f32(*shape):
        return pltpu.VMEM(shape, F32)

    def bf16(*shape):
        return pltpu.VMEM(shape, BF16)

    def i32(*shape):
        return pltpu.SMEM(shape, jnp.int32)

    flat = (levels * clat, clon)
    fields = pl.pallas_call(
        functools.partial(kernel, n_lat, n_lon),
        out_shape=(f32(*flat), f32(*flat)),
        in_specs=[anywhere] * 8,
        out_specs=(pl.BlockSpec(memory_space=pltpu.VMEM),) * 2,
        scratch_shapes=[
            f32(2, levels, clat, clon),
            f32(2 * levels * clat, clon),
            f32(cap, clon, clon),
            f32(3, src_pad, cap, clon),
            f32(3 * n_lon, 1, clon),
            f32(3, 1, clon),
            bf16(PAD_WIN * cap, n_blocks),
            bf16(PAD_WIN * cap, 2 * n_blocks),
            bf16(ring * levels, n_blocks),
            bf16(ring * levels, 2 * n_blocks),
            f32(2, PAD_WIN, cap, clon),
            f32(2, ring, tiles, 8, clon),
            f32(n_lon, 2, SLOT, clat, clon),
            f32(2, n_lon, 2, SLOT, HALO, clon),
            f32(n_lon, clat, clon),
            f32(2, n_lon, HALO, clon),
            f32(2, n_lon, SLOT, rows, clon),
            f32(n_lon, rows, clon),
            f32(2, n_lon, SLOT, rows, clon),
            f32(5, WIN, 2, cap, clon),
            f32(2, 2, STEPS, tiles, 8, clon),
            f32(2, 2, STEPS, tiles, 8, clon),
            f32(2, 2, tiles, 8, clon),
            f32(2, 3, 2, tiles, 8, clon),
            f32(5, 2, tiles, ring, 8, clon),
            f32(cap, clon, clon),
            f32(3, tiles, clat, 8, clon),
            f32(n_lon, 8, clon),
            f32(n_lat, 8, clon),
            i32(1, n_lon * SLOT),
            i32(3 * n_lon, 1, n_lon * SLOT),
            dma, dma, dma,
            dma((7, 3)), dma((7, 3)),
            dma((2,)), dma((2,)),
            dma((2, 3)), dma((2, 3)),
            dma((4,)),
            f32(1, cap, clon), f32(1, cap, clon),
            i32(1, cap), i32(1, cap), i32(1, 1),
            dma((5,)),
        ],
        compiler_params=pltpu.CompilerParams(collective_id=0, has_side_effects=True),
    )(courant, courant.reshape(2 * levels * clat, clon), obs_matrix, obs_weight, innovation, block_owner[:, :, 0], block_row, block_count)
    out = jax.ShapeDtypeStruct(flat, F32)
    stored = pl.pallas_call(
        store_kernel,
        out_shape=(out, out),
        in_specs=[anywhere] * 2,
        out_specs=(anywhere,) * 2,
        scratch_shapes=[dma((2,))],
    )(*[pltpu.with_memory_space_constraint(field, pltpu.VMEM) for field in fields])
    return tuple(field.reshape(levels, clat, clon) for field in stored)


def solution(mesh):
    placed = (
        P(None, None, "lat", "lon"),
        P("lat", "lon", None, None),
        P("lat", "lon", None),
        P("lat", "lon", None),
        P("lat", "lon", None),
        P("lat", "lon"),
        P("lat", "lon"),
    )
    return jax.shard_map(
        functools.partial(shards, mesh.shape["lat"], mesh.shape["lon"]),
        mesh=mesh,
        in_specs=placed,
        out_specs=(P(None, "lat", "lon"), P(None, "lat", "lon")),
        check_vma=False,
    )
```

```python
import functools

import jax
import jax.numpy as jnp
from jax import lax
from jax.experimental import pallas as pl
from jax.experimental.pallas import tpu as pltpu
from jax.sharding import PartitionSpec as P

STEPS = 4
HALO = 2 * STEPS
SLOT = 2
DIRECT = 64
WIN = 2 * HALO + 1
PAD_WIN = WIN + 1
MESH = pl.DeviceIdType.MESH
F32 = jnp.float32
BF16 = jnp.bfloat16


def split2(x):
    hi = x.astype(BF16)
    return hi, (x - hi.astype(F32)).astype(BF16)


def dot2(onehot, parts):
    total = None
    for part in parts:
        term = jnp.dot(onehot, part, preferred_element_type=F32)
        total = term if total is None else total + term
    return total


def split_rates(c0, c1):
    a, b = jnp.maximum(c0, 0.0), jnp.maximum(-c0, 0.0)
    e, f = jnp.maximum(c1, 0.0), jnp.maximum(-c1, 0.0)
    return a, b, e, f, 1.0 - a - b - e - f


def kernel(
    n_lat, n_lon,
    courant, courant_flat, obs, weight_in, innov_in, owner_in, row_in, count_in,
    inc_out, res_out,
    flow, flow_flat, obs_v, terms, codes, code_out, hot_main, hot_side, dense_main, dense_side, field, dense_field,
    main_out, main_edge, strip_out, strip_edge, main_in, strip_in, side_in,
    win_rates, lat_out, lat_in, lon_out, lon_in, lon_edge_out, lon_edge_in, dense_rates, weight_wide, parts, red_lon, red_far,
    ask_out, ask_in,
    obs_sem, flow_sem, flat_sem, wide_send, wide_recv, ask_recv, lat_send, lat_recv, lon_send, lon_recv, red_sems,
    weight, innov, owner, row, count, input_sems,
):
    li = lax.axis_index("lat")
    lo = lax.axis_index("lon")
    clon = flow_flat.shape[1]
    cap = obs_v.shape[0]
    tiles, clat = parts.shape[1:3]
    levels = tiles * 8
    n_src = 3 * n_lon
    n_blocks = terms.shape[1] * cap
    span = 4 * clat
    ring = clat + 2 * STEPS
    width = clon // clat
    n_all = n_lat * n_lon
    direct = n_all <= DIRECT

    small = [
        pltpu.make_async_copy(src, dst, input_sems.at[n])
        for n, (src, dst) in enumerate((
            (owner_in, owner), (row_in, row), (count_in, count), (weight_in, weight), (innov_in, innov)))
    ]
    for copy in small:
        copy.start()
    flow_copy = pltpu.make_async_copy(courant, flow, flow_sem)
    flow_copy.start()
    flat_copy = pltpu.make_async_copy(courant_flat, flow_flat, flat_sem)
    obs_copy = pltpu.make_async_copy(obs.at[0], obs_v, obs_sem)
    obs_copy.start()
    flat_copy.start()

    def exists(d):
        return (li + d >= 0) & (li + d < n_lat)

    def guarded(d, run):
        if d == 0:
            run()
        else:
            pl.when(exists(d))(run)

    def lon_at(j):
        return lax.rem(lo + j + n_lon, n_lon)

    barrier = pltpu.get_barrier_semaphore()

    def greet(lat, lon):
        pl.semaphore_signal(barrier, inc=1, device_id={"lat": lat, "lon": lon}, device_id_type=MESH)

    if direct:
        for j in range(1, n_all):
            other = lax.rem(li * n_lon + lo + j, n_all)
            greet(lax.div(other, n_lon), lax.rem(other, n_lon))
    else:
        @pl.loop(1, n_lat)
        def _(j):
            greet(lax.rem(li + j, n_lat), lo)

        for d in (-1, 1):
            def hello(d=d):
                for j in range(1, n_lon):
                    greet(li + d, lon_at(j))
            guarded(d, hello)
        for j in range(1, n_lon):
            greet(li, lon_at(j))

    for copy in small:
        copy.wait()

    sub = lax.broadcasted_iota(jnp.int32, (cap, clon), 0)
    live = count[0, 0]
    owners = [owner[0, b] for b in range(cap)]
    levs = [lax.div(row[0, b], jnp.int32(clat)) for b in range(cap)]
    lats = [row[0, b] - levs[b] * clat for b in range(cap)]
    slots = []
    for b in range(cap):
        s = jnp.int32(0)
        for c in range(b):
            s = s + (owners[c] == owners[b]).astype(jnp.int32)
        slots.append(jnp.minimum(s, SLOT - 1))
    for o in range(n_lon):
        for s in range(SLOT):
            lev = jnp.int32(0)
            for b in range(cap):
                lev = jnp.where((owners[b] == o) & (slots[b] == s), levs[b], lev)
            ask_out[0, o * SLOT + s] = lev

    def column(values):
        tile = jnp.full((cap, clon), values[0], jnp.int32)
        for b in range(1, cap):
            tile = jnp.where(sub == b, values[b], tile)
        return tile

    level_tile, lat_tile, owner_tile = column(levs), column(lats), column(owners)

    def code_of(owner_now, lat_now):
        return (level_tile * n_lon + owner_now) * span + lat_now + clat

    lane = lax.broadcasted_iota(jnp.int32, (1, clon), 1)
    middle = clon // 2
    code_line = jnp.full((1, clon), -1, jnp.int32)
    for b in range(cap):
        code = (levs[b] * n_lon + owners[b]) * span + lats[b] + clat
        code_line = jnp.where(lane == b, jnp.where(b < live, code, -4 * span), code_line)
    for d in (-1, 0, 1):
        code_out[d + 1] = (code_line - clat * d).astype(F32)

    if direct:
        pl.semaphore_wait(barrier, n_all - 1)
    else:
        sides = (li > 0).astype(jnp.int32) + (li < n_lat - 1).astype(jnp.int32)
        pl.semaphore_wait(barrier, (n_lon - 1) + (n_lat - 1) + sides * (n_lon - 1))

    def wide(kind, d, j, src, dst):
        return pltpu.make_async_remote_copy(
            src_ref=src, dst_ref=dst,
            send_sem=wide_send.at[kind, d + 1], recv_sem=wide_recv.at[kind, d + 1],
            device_id={"lat": li + d, "lon": lon_at(j)}, device_id_type=MESH,
        )

    def slot_of(d, j, out):
        return (1 - d) * n_lon + (lo if out else lon_at(-j))

    def several(d):
        return n_lon - 1 if d == 0 else n_lon

    def start_wide(make):
        for d in (-1, 1, 0):
            def run(d=d):
                for j in (2, 3, 1, 0) if n_lon == 4 else range(n_lon):
                    if (d, j) != (0, 0):
                        make(d, j).start()
            guarded(d, run)

    def recv_wide(whole):
        for d in (-1, 1, 0):
            def run(d=d):
                kind, _, into = whole(d)
                wide(kind, d, 1, into, into).wait_recv()
            guarded(-d, run)

    def done_wide(whole):
        for d in (-1, 1, 0):
            def run(d=d):
                kind, out, _ = whole(d)
                wide(kind, d, 1, out, out).wait_send()
            guarded(d, run)

    def code_make(d, j):
        return wide(0, d, j, code_out.at[d + 1], codes.at[slot_of(d, j, True)])

    def code_all(d):
        ref = codes.at[pl.ds((1 - d) * n_lon, several(d))]
        return 0, ref, ref

    def ask_make(d, j, out=True):
        return pltpu.make_async_remote_copy(
            src_ref=ask_out, dst_ref=ask_in.at[slot_of(d, j, out)],
            send_sem=wide_send.at[1, d + 1], recv_sem=ask_recv.at[d + 1, j],
            device_id={"lat": li + d, "lon": lon_at(j)}, device_id_type=MESH)

    def ask_all(d):
        ref = ask_in.at[pl.ds((1 - d) * n_lon, several(d))]
        return 1, ref, ref

    def place(d):
        return (HALO, clat) if d == 0 else ((0, HALO) if d == 1 else (HALO + clat, HALO))

    def main_make(d, j):
        first, size = place(d)
        src = main_out.at[j] if d == 0 else main_edge.at[(d + 1) // 2, j]
        return wide(2, d, j, src, main_in.at[:, lo, :, pl.ds(first, size), :])

    def main_all(d):
        first, size = place(d)
        src = main_out.at[pl.ds(1, n_lon - 1)] if d == 0 else main_edge.at[(d + 1) // 2]
        return 2, src, main_in.at[:, pl.ds(0, several(d)), :, pl.ds(first, size), :]

    def strip_make(d, j):
        first, size = place(d)
        src = strip_out.at[j] if d == 0 else strip_edge.at[(d + 1) // 2, j]
        return wide(3, d, j, src, strip_in.at[lo, pl.ds(first, size), :])

    def strip_all(d):
        first, size = place(d)
        src = strip_out.at[pl.ds(1, n_lon - 1)] if d == 0 else strip_edge.at[(d + 1) // 2]
        return 3, src, strip_in.at[pl.ds(0, several(d)), pl.ds(first, size), :]

    def term_make(rnd):
        def make(d, j):
            return wide(4 + rnd, d, j, terms.at[rnd, n_lon + lo], terms.at[rnd, slot_of(d, j, True)])
        return make

    def term_all(rnd):
        def whole(d):
            ref = terms.at[rnd, pl.ds((1 - d) * n_lon, several(d))]
            return 4 + rnd, ref, ref
        return whole

    def lat_make(f, d):
        return pltpu.make_async_remote_copy(
            src_ref=lat_out.at[f, (d + 1) // 2], dst_ref=lat_in.at[f, (1 - d) // 2],
            send_sem=lat_send.at[f, (d + 1) // 2], recv_sem=lat_recv.at[f, (d + 1) // 2],
            device_id={"lat": li + d, "lon": lo}, device_id_type=MESH)

    def lon_make(role, d):
        if d == 0:
            src, dst = lon_out.at[role], lon_in.at[role]
        else:
            src, dst = lon_edge_out.at[role, (d + 1) // 2], lon_edge_in.at[role, (1 - d) // 2]
        return pltpu.make_async_remote_copy(
            src_ref=src, dst_ref=dst,
            send_sem=lon_send.at[role, d + 1], recv_sem=lon_recv.at[role, d + 1],
            device_id={"lat": li + d, "lon": lon_at(-1 if role == 0 else 1)}, device_id_type=MESH)

    start_wide(ask_make)
    start_wide(code_make)
    codes[n_lon + lo] = code_out[1]

    flow_copy.wait()

    def flow_rows(f, lev, first, size):
        return flow[f, lev, first:first + size, :]

    def flow_levels(f, tile, lat):
        return flow_flat[pl.ds((f * levels + tile * 8) * clat + lat, 8, stride=clat), :]

    live_rows = sub < live
    w_rows = jnp.where(live_rows, weight[0], 0.0)
    wy_rows = w_rows * innov[0]
    stacked = jnp.concatenate([w_rows, wy_rows, jnp.zeros((clon - 2 * cap, clon), F32)], axis=0)
    columns = jnp.transpose(stacked)
    for b in range(cap):
        weight_wide[b] = jnp.broadcast_to(columns[:, b:b + 1], (clon, clon))
    wy_col = [columns[:, cap + b:cap + b + 1] for b in range(cap)]

    def spread(rnd, u_cols):
        out = [jnp.sum(obs_v[b] * u_cols[b], axis=0, keepdims=True) for b in range(cap)]
        terms[rnd, n_lon + lo] = jnp.concatenate(out, axis=0)
        start_wide(term_make(rnd))

    obs_copy.wait()
    spread(0, wy_col)

    flat_copy.wait()
    for f in range(2):
        for t in range(tiles):
            for k in range(STEPS):
                lat_out[f, 0, k, t] = flow_levels(f, t, k)
                lat_out[f, 1, k, t] = flow_levels(f, t, clat - STEPS + k)
    lane_lat = lane // width
    bunch = STEPS * width
    lane_bunch = lane // bunch
    for role in range(2):
        edges = [jnp.zeros((8, clon), F32)] * 2
        for f in range(2):
            for t in range(tiles):
                tile = jnp.zeros((8, clon), F32)
                for n in range(clat):
                    at = (n * width + role * width) % clon
                    tile = jnp.where(lane_lat == n, pltpu.roll(flow_levels(f, t, n), at, 1), tile)
                lon_out[role, f, t] = tile
                i = f * tiles + t
                for k, at in enumerate((i * bunch, (clon + i * bunch - (clat - STEPS) * width) % clon)):
                    edges[k] = jnp.where(lane_bunch == i, pltpu.roll(tile, at, 1), edges[k])
        for k in range(2):
            lon_edge_out[role, k] = edges[k]

    def send_dense(f):
        for d in (-1, 1):
            def send(d=d):
                lat_make(f, d).start()
                lon_make(f, d).start()
            guarded(d, send)
        lon_make(f, 0).start()

    send_dense(1)

    group = lane // HALO

    def answer(d, j):
        if d == 0:
            first, size = 0, clat
        elif d == 1:
            first, size = clat - HALO, HALO
        else:
            first, size = 0, HALO
        slot = (d + 1) * n_lon + lon_at(j)

        def asked(o, s):
            if (d, j) == (0, 0):
                return ask_out[0, o * SLOT + s]
            return ask_in[slot, 0, o * SLOT + s]

        tile = jnp.zeros((size, clon), F32)
        for s in range(SLOT):
            lev = asked(lo, s)
            right, left = asked(lon_at(-1), s), asked(lon_at(1), s)
            for f in range(2):
                rows = flow_rows(f, lev, first, size)
                if (d, j) == (0, 0):
                    main_in[f, lo, s, HALO:HALO + clat, :] = rows
                elif d == 0:
                    main_out[j, f, s] = rows
                else:
                    main_edge[(d + 1) // 2, j, f, s] = rows
                g = s * 2 + f
                moved = pltpu.roll(flow_rows(f, right, first, size), g * HALO, 1)
                tile = jnp.where(group == g, moved, tile)
                g = (SLOT + s) * 2 + f
                moved = pltpu.roll(flow_rows(f, left, first, size), (g + 1) * HALO, 1)
                tile = jnp.where(group == g, moved, tile)
        if (d, j) == (0, 0):
            strip_in[lo, HALO:HALO + clat, :] = tile
        else:
            if d == 0:
                strip_out[j] = tile
            else:
                strip_edge[(d + 1) // 2, j] = tile
            main_make(d, j).start()
            strip_make(d, j).start()

    def respond(d, j):
        def run():
            ask_make(-d, (n_lon - j) % n_lon, False).wait_recv()
            answer(d, j)
        guarded(d, run)

    answer(0, 0)
    near = [j for j in range(1, n_lon) if 2 * j != n_lon]
    far = [j for j in range(1, n_lon) if 2 * j == n_lon]
    for d, js in ((0, near), (1, [0]), (-1, [0]), (0, far), (1, near), (-1, near), (1, far), (-1, far)):
        for j in js:
            respond(d, j)

    pad = terms.shape[1] - n_src
    if pad:
        for rnd in range(3):
            terms[rnd, n_src:] = jnp.zeros((pad, cap, clon), F32)
    for d in (-1, 1):
        @pl.when(jnp.logical_not(exists(d)))
        def _(d=d):
            first = (d + 1) * n_lon
            codes[first:first + n_lon] = jnp.full((n_lon, 1, clon), -4.0 * span, F32)
            for rnd in range(3):
                terms[rnd, first:first + n_lon] = jnp.zeros((n_lon, cap, clon), F32)
            lat0 = 0 if d == -1 else HALO + clat
            main_in[:, :, :, lat0:lat0 + HALO, :] = jnp.zeros((2, n_lon, SLOT, HALO, clon), F32)
            strip_in[:, lat0:lat0 + HALO, :] = jnp.zeros((n_lon, HALO, clon), F32)
            lat_in[:, (d + 1) // 2] = jnp.zeros((2, STEPS, tiles, 8, clon), F32)
            lon_edge_in[:, (d + 1) // 2] = jnp.zeros((2, 8, clon), F32)

    recv_wide(code_all)
    code_parts = []
    for first in range(0, n_blocks, clon):
        line = jnp.full((1, clon), -4.0 * span, F32)
        for k in range(clon // cap):
            slot = first // cap + k
            if slot < n_src:
                line = jnp.where(lane // cap == k, pltpu.roll(codes[slot], k * cap, 1), line)
        code_parts.append(line)
    code_row = code_parts[0] if len(code_parts) == 1 else jnp.concatenate(code_parts, axis=1)

    def wide_tile(tile):
        return jnp.concatenate([tile] * (n_blocks // clon), axis=1) if n_blocks > clon else tile[:, :n_blocks]

    def matches(place_code):
        return jnp.where(place_code.astype(F32) == code_row, 1.0, 0.0).astype(BF16)

    for part, shift in enumerate((0, n_lon - 1, 1)):
        tile = wide_tile(code_of(lax.rem(owner_tile + shift, n_lon), lat_tile))
        for d in range(0, PAD_WIN, 2):
            rows = matches(jnp.concatenate([tile + (d - HALO), tile + (d + 1 - HALO)], axis=0))
            if part == 0:
                hot_main[d * cap:(d + 2) * cap, :] = rows
            else:
                hot_side[d * cap:(d + 2) * cap, (part - 1) * n_blocks:part * n_blocks] = rows

    def build_dense():
        lev_codes = lax.broadcasted_iota(jnp.int32, (levels, n_blocks), 0) * (n_lon * span)
        for part, shift in enumerate((0, n_lon - 1, 1)):
            for d in range(ring):
                rows = matches(lev_codes + (lon_at(shift) * span + (d - STEPS + clat)))
                if part == 0:
                    dense_main[d * levels:(d + 1) * levels, :] = rows
                else:
                    dense_side[d * levels:(d + 1) * levels, (part - 1) * n_blocks:part * n_blocks] = rows

    last_lane = lane == clon - 1
    first_lane = lane == 0

    def lon_up(m, s):
        mr, sr = pltpu.roll(m, clon - 1, 1), pltpu.roll(s, clon - 1, 1)
        return jnp.where(last_lane, sr, mr), jnp.where(last_lane, mr, sr)

    def lon_down(m, s):
        mr, sr = pltpu.roll(m, 1, 1), pltpu.roll(s, 1, 1)
        return jnp.where(first_lane, sr, mr), jnp.where(first_lane, mr, sr)

    def term_parts(rnd):
        flat = terms[rnd].reshape(n_blocks, clon)
        halves = [jnp.where(lane >= middle, flat, 0.0), jnp.where(lane < middle, flat, 0.0)]
        return split2(flat), split2(jnp.concatenate(halves, axis=0))

    def load_window(rnd):
        main_parts, side_parts = term_parts(rnd)
        field[0] = dot2(hot_main[...], main_parts).reshape(PAD_WIN, cap, clon)
        field[1] = dot2(hot_side[...], side_parts).reshape(PAD_WIN, cap, clon)

    def adjoint(rate, main, side, first, last):
        a, b, e, f, keep = range(5)
        for _ in range(STEPS):
            a_main = {d: rate(a, 0, d) * main[d] for d in range(first + 2, last + 1)}
            b_main = {d: rate(b, 0, d) * main[d] for d in range(first, last - 1)}
            a_side = {d: rate(a, 1, d) * side[d] for d in range(first + 3, last)}
            b_side = {d: rate(b, 1, d) * side[d] for d in range(first + 1, last - 2)}
            new_main, new_side = {}, {}
            for d in range(first + 1, last):
                up = lon_up(rate(e, 0, d) * main[d], rate(e, 1, d) * side[d])
                down = lon_down(rate(f, 0, d) * main[d], rate(f, 1, d) * side[d])
                new_main[d] = rate(keep, 0, d) * main[d] + a_main[d + 1] + b_main[d - 1] + up[0] + down[0]
                if first + 2 <= d < last - 1:
                    new_side[d] = rate(keep, 1, d) * side[d] + a_side[d + 1] + b_side[d - 1] + up[1] + down[1]
            main, side = new_main, new_side
            first, last = first + 1, last - 1
        return main, side

    recv_wide(term_all(0))
    load_window(0)

    recv_wide(strip_all)
    for o in range(n_lon):
        from_right, from_left = strip_in[(o + 1) % n_lon], strip_in[(o - 1) % n_lon]
        for s in range(SLOT):
            for f in range(2):
                g = s * 2 + f
                right = pltpu.roll(from_right, (clon - g * HALO) % clon, 1)
                g = (SLOT + s) * 2 + f
                left = pltpu.roll(from_left, (2 * clon - HALO - g * HALO) % clon, 1)
                side_in[f, o, s] = jnp.where(lane < middle, right, left)
    recv_wide(main_all)
    send_dense(0)

    def gather(ref, f, d):
        tile = None
        for b in range(cap):
            line = ref[f, owners[b], slots[b], pl.ds(lats[b] + d, 1), :]
            tile = jnp.broadcast_to(line, (cap, clon)) if tile is None else jnp.where(sub == b, line, tile)
        return tile

    for d in range(WIN):
        for side, ref in enumerate((main_in, side_in)):
            if d in (0, WIN - 1):
                if side == 0:
                    c0 = gather(ref, 0, d)
                    win_rates[1 if d == 0 else 0, d, side] = jnp.maximum(-c0 if d == 0 else c0, 0.0)
                continue
            for k, value in enumerate(split_rates(gather(ref, 0, d), gather(ref, 1, d))):
                win_rates[k, d, side] = value

    def window_model():
        a, b, e, f, keep = range(5)
        main = {d: field[0, d] for d in range(WIN)}
        side = {d: field[1, d] for d in range(1, WIN - 1)}
        main, side = adjoint(lambda k, n, d: win_rates[k, d, n], main, side, 0, WIN - 1)
        for d in list(main):
            lat_now = lat_tile + (li * clat + d - HALO)
            inside = (lat_now >= 0) & (lat_now < n_lat * clat)
            main[d] = jnp.where(inside, main[d], 0.0)
            if d in side:
                side[d] = jnp.where(inside, side[d], 0.0)
        for step in range(STEPS):
            reach = STEPS - 1 - step
            new_main, new_side = {}, {}
            for d in range(HALO - reach, HALO + reach + 1):
                down, up = lon_down(main[d], side[d]), lon_up(main[d], side[d])
                new_main[d] = (win_rates[keep, d, 0] * main[d] + win_rates[a, d, 0] * main[d - 1] + win_rates[b, d, 0] * main[d + 1]
                               + win_rates[e, d, 0] * down[0] + win_rates[f, d, 0] * up[0])
                if abs(d - HALO) < reach:
                    new_side[d] = (win_rates[keep, d, 1] * side[d] + win_rates[a, d, 1] * side[d - 1]
                                   + win_rates[b, d, 1] * side[d + 1] + win_rates[e, d, 1] * down[1] + win_rates[f, d, 1] * up[1])
            main, side = new_main, new_side
        seen = main[HALO]
        return [jnp.sum(obs_v[b] * seen[b:b + 1, :], axis=1, keepdims=True) for b in range(cap)]

    def each_dense(run):
        for f in range(2):
            for d in (-1, 1, 0):
                def go(f=f, d=d):
                    if d:
                        run(lat_make(f, d))
                    run(lon_make(f, d))
                yield d, go

    def recv_dense():
        for d, go in each_dense(lambda copy: copy.wait_recv()):
            guarded(-d, go)
        for t in range(tiles):
            for d in range(ring):
                lat = d - STEPS
                if lat < 0:
                    main, edge, at = [lat_in[f, 0, d, t] for f in range(2)], 0, d
                elif lat >= clat:
                    main, edge, at = [lat_in[f, 1, lat - clat, t] for f in range(2)], 1, lat - clat
                else:
                    main, edge, at = [flow_levels(f, t, lat) for f in range(2)], None, lat
                side = []
                for f in range(2):
                    if edge is None:
                        first, pair = at * width, [lon_in[role, f, t] for role in range(2)]
                    else:
                        first, pair = (f * tiles + t) * bunch + at * width, [lon_edge_in[role, edge] for role in range(2)]
                    side.append(jnp.where(lane < middle, pltpu.roll(pair[0], (clon - first) % clon, 1),
                                          pltpu.roll(pair[1], (2 * clon - width - first) % clon, 1)))
                for n, pair in enumerate((main, side)):
                    for k, value in enumerate(split_rates(*pair)):
                        dense_rates[k, n, t, d] = value

    def dense(rnd):
        main_parts, side_parts = term_parts(rnd)
        dense_field[0] = dot2(dense_main[...], main_parts).reshape(ring, tiles, 8, clon)
        dense_field[1] = dot2(dense_side[...], side_parts).reshape(ring, tiles, 8, clon)

        @pl.loop(0, tiles)
        def _(t):
            main = {d: dense_field[0, d, t] for d in range(ring)}
            side = {d: dense_field[1, d, t] for d in range(1, ring - 1)}
            main, _ = adjoint(lambda k, n, d: dense_rates[k, n, t, d], main, side, 0, ring - 1)
            for lat in range(clat):
                parts[rnd, t, lat] = main[lat + STEPS]

    def red_make(n, ref, own, lat, lon):
        return pltpu.make_async_remote_copy(
            src_ref=ref.at[own], dst_ref=ref.at[own], send_sem=red_sems.at[n], recv_sem=red_sems.at[n + 1],
            device_id={"lat": lat, "lon": lon}, device_id_type=MESH)

    def red_all(n, ref, size):
        whole = ref.at[pl.ds(0, size)]
        return pltpu.make_async_remote_copy(
            src_ref=whole, dst_ref=whole, send_sem=red_sems.at[n], recv_sem=red_sems.at[n + 1],
            device_id={"lat": li, "lon": lon_at(1)}, device_id_type=MESH)

    def reduce_start(line):
        if direct:
            me = li * n_lon + lo
            red_far[me] = line
            for j in range(1, n_all):
                other = lax.rem(me + j, n_all)
                red_make(2, red_far, me, lax.div(other, n_lon), lax.rem(other, n_lon)).start()
        else:
            red_lon[lo] = line
            for j in range(1, n_lon):
                red_make(0, red_lon, lo, li, lon_at(j)).start()

    def reduce_turn():
        if not direct:
            red_all(0, red_lon, n_lon - 1).wait_recv()
            red_far[li] = jnp.sum(red_lon[...], axis=0)

            @pl.loop(1, n_lat)
            def _(j):
                red_make(2, red_far, li, lax.rem(li + j, n_lat), lo).start()

    far_size = n_all if direct else n_lat

    def packed(cols):
        tile = jnp.zeros((clon, clon), F32)
        for b in range(cap):
            tile = jnp.where(lane == b, cols[b], tile)
        return tile

    p1 = window_model()
    spread(1, [weight_wide[b] * p1[b] for b in range(cap)])
    build_dense()
    recv_wide(term_all(1))
    load_window(1)
    g1 = window_model()
    spread(2, [weight_wide[b] * g1[b] for b in range(cap)])
    p_all, g_all = packed(p1), packed(g1)
    u_all = columns * p_all
    line = jnp.zeros((1, clon), F32)
    for n, value in enumerate((pltpu.roll(columns, clon - cap, 1) * p_all, u_all * p_all, u_all * g_all, columns * g_all * g_all)):
        line = line + pltpu.roll(jnp.sum(value, axis=0, keepdims=True), n * cap, 1)
    reduce_start(line)
    recv_dense()
    dense(0)
    reduce_turn()
    dense(1)
    recv_wide(term_all(2))
    dense(2)
    red_all(2, red_far, far_size - 1).wait_recv()

    line = jnp.sum(red_far[...], axis=0)
    sums = [jnp.sum(jnp.where(lane // cap == n, line, 0.0), axis=1, keepdims=True) for n in range(4)]
    bb, s1, tt, s3 = sums
    scale = bb + s1
    alpha1, left1 = bb / scale, s1 / scale
    rr = left1 * (left1 * bb - alpha1 * s1) - alpha1 * (left1 * s1 - alpha1 * tt)
    sr1 = left1 * s1 - alpha1 * tt
    srr = left1 * sr1 - alpha1 * (left1 * tt - alpha1 * s3)
    beta = rr / bb
    curve = rr + beta * beta * bb + (srr + 2.0 * beta * sr1 + beta * beta * s1)
    alpha2 = rr / curve
    mix = left1 + beta
    inc_b, inc_t = alpha1 + alpha2 * mix, -alpha2 * alpha1
    res_b, res_t, res_2 = left1 - alpha2 * mix, -alpha1 - alpha2 * (mix - alpha1), alpha2 * alpha1
    for t in range(tiles):
        for lat in range(clat):
            b0, t1, t2 = (parts[rnd, t, lat] for rnd in range(3))
            rows = pl.ds(t * 8 * clat + lat, 8, stride=clat)
            inc_out[rows, :] = inc_b * b0 + inc_t * t1
            res_out[rows, :] = res_b * b0 + res_t * t1 + res_2 * t2

    for whole in (code_all, ask_all, main_all, strip_all, term_all(0), term_all(1), term_all(2)):
        done_wide(whole)
    for d, go in each_dense(lambda copy: copy.wait_send()):
        guarded(d, go)
    if not direct:
        red_all(0, red_lon, n_lon - 1).wait_send()
    red_all(2, red_far, far_size - 1).wait_send()


def store_kernel(inc, res, inc_out, res_out, sems):
    pairs = ((inc, inc_out), (res, res_out))
    copies = [pltpu.make_async_copy(src, dst, sems.at[n]) for n, (src, dst) in enumerate(pairs)]
    for copy in copies:
        copy.start()
    for copy in copies:
        copy.wait()


def shards(n_lat, n_lon, courant, obs_matrix, obs_weight, innovation, block_owner, block_row, block_count):
    _, levels, clat, clon = courant.shape
    cap = block_row.shape[1]
    tiles = levels // 8
    ring = clat + 2 * STEPS
    rows = clat + 2 * HALO
    unit = clon // cap
    src_pad = -(-3 * n_lon // unit) * unit
    n_blocks = src_pad * cap
    anywhere = pl.BlockSpec(memory_space=pl.ANY)
    dma = pltpu.SemaphoreType.DMA

    def f32(*shape):
        return pltpu.VMEM(shape, F32)

    def bf16(*shape):
        return pltpu.VMEM(shape, BF16)

    def i32(*shape):
        return pltpu.SMEM(shape, jnp.int32)

    flat = (levels * clat, clon)
    fields = pl.pallas_call(
        functools.partial(kernel, n_lat, n_lon),
        out_shape=(f32(*flat), f32(*flat)),
        in_specs=[anywhere] * 8,
        out_specs=(pl.BlockSpec(memory_space=pltpu.VMEM),) * 2,
        scratch_shapes=[
            f32(2, levels, clat, clon),
            f32(2 * levels * clat, clon),
            f32(cap, clon, clon),
            f32(3, src_pad, cap, clon),
            f32(3 * n_lon, 1, clon),
            f32(3, 1, clon),
            bf16(PAD_WIN * cap, n_blocks),
            bf16(PAD_WIN * cap, 2 * n_blocks),
            bf16(ring * levels, n_blocks),
            bf16(ring * levels, 2 * n_blocks),
            f32(2, PAD_WIN, cap, clon),
            f32(2, ring, tiles, 8, clon),
            f32(n_lon, 2, SLOT, clat, clon),
            f32(2, n_lon, 2, SLOT, HALO, clon),
            f32(n_lon, clat, clon),
            f32(2, n_lon, HALO, clon),
            f32(2, n_lon, SLOT, rows, clon),
            f32(n_lon, rows, clon),
            f32(2, n_lon, SLOT, rows, clon),
            f32(5, WIN, 2, cap, clon),
            f32(2, 2, STEPS, tiles, 8, clon),
            f32(2, 2, STEPS, tiles, 8, clon),
            f32(2, 2, tiles, 8, clon),
            f32(2, 2, tiles, 8, clon),
            f32(2, 2, 8, clon),
            f32(2, 2, 8, clon),
            f32(5, 2, tiles, ring, 8, clon),
            f32(cap, clon, clon),
            f32(3, tiles, clat, 8, clon),
            f32(n_lon, 1, clon),
            f32(n_lat * n_lon if n_lat * n_lon <= DIRECT else n_lat, 1, clon),
            i32(1, n_lon * SLOT),
            i32(3 * n_lon, 1, n_lon * SLOT),
            dma, dma, dma,
            dma((7, 3)), dma((7, 3)),
            dma((3, n_lon)),
            dma((2, 2)), dma((2, 2)),
            dma((2, 3)), dma((2, 3)),
            dma((4,)),
            f32(1, cap, clon), f32(1, cap, clon),
            i32(1, cap), i32(1, cap), i32(1, 1),
            dma((5,)),
        ],
        compiler_params=pltpu.CompilerParams(collective_id=0, has_side_effects=True),
    )(courant, courant.reshape(2 * levels * clat, clon), obs_matrix, obs_weight, innovation, block_owner[:, :, 0], block_row, block_count)
    out = jax.ShapeDtypeStruct(flat, F32)
    stored = pl.pallas_call(
        store_kernel,
        out_shape=(out, out),
        in_specs=[anywhere] * 2,
        out_specs=(anywhere,) * 2,
        scratch_shapes=[dma((2,))],
    )(*[pltpu.with_memory_space_constraint(field, pltpu.VMEM) for field in fields])
    return tuple(field.reshape(levels, clat, clon) for field in stored)


def solution(mesh):
    placed = (
        P(None, None, "lat", "lon"),
        P("lat", "lon", None, None),
        P("lat", "lon", None),
        P("lat", "lon", None),
        P("lat", "lon", None),
        P("lat", "lon"),
        P("lat", "lon"),
    )
    return jax.shard_map(
        functools.partial(shards, mesh.shape["lat"], mesh.shape["lon"]),
        mesh=mesh,
        in_specs=placed,
        out_specs=(P(None, "lat", "lon"), P(None, "lat", "lon")),
        check_vma=False,
    )
```

```python
import functools

import jax
import jax.numpy as jnp
from jax import lax
from jax.experimental import pallas as pl
from jax.experimental.pallas import tpu as pltpu
from jax.sharding import PartitionSpec as P

STEPS = 4
HALO = 2 * STEPS
SLOT = 2
DIRECT = 64
WIN = 2 * HALO + 1
PAD_WIN = WIN + 1
MESH = pl.DeviceIdType.MESH
F32 = jnp.float32
BF16 = jnp.bfloat16


def split2(x):
    hi = x.astype(BF16)
    return hi, (x - hi.astype(F32)).astype(BF16)


def dot2(onehot, parts):
    total = None
    for part in parts:
        term = jnp.dot(onehot, part, preferred_element_type=F32)
        total = term if total is None else total + term
    return total


def split_rates(c0, c1):
    a, b = jnp.maximum(c0, 0.0), jnp.maximum(-c0, 0.0)
    e, f = jnp.maximum(c1, 0.0), jnp.maximum(-c1, 0.0)
    return a, b, e, f, 1.0 - a - b - e - f


def kernel(
    n_lat, n_lon,
    courant, courant_flat, obs, weight_in, innov_in, owner_in, row_in, count_in,
    inc_out, res_out,
    flow, flow_flat, obs_v, terms, codes, code_out, hot_main, hot_side, dense_main, dense_side, field, dense_field,
    main_out, main_edge, strip_out, strip_edge, main_in, strip_in, strip_edge_in, side_in,
    win_rates, lat_out, lat_in, lon_out, lon_in, lon_edge_out, lon_edge_in, dense_rates, weight_wide, parts, red_lon, red_far,
    proxy, ask_out, ask_in,
    obs_sem, flow_sem, flat_sem, wide_send, wide_recv, ask_send, ask_recv, red_sems,
    weight, innov, owner, row, count, input_sems,
):
    li = lax.axis_index("lat")
    lo = lax.axis_index("lon")
    clon = flow_flat.shape[1]
    cap = obs_v.shape[0]
    tiles, clat = parts.shape[1:3]
    levels = tiles * 8
    n_src = 3 * n_lon
    n_blocks = terms.shape[1] * cap
    span = 4 * clat
    ring = clat + 2 * STEPS
    width = clon // clat
    n_all = n_lat * n_lon
    direct = n_all <= DIRECT

    small = [
        pltpu.make_async_copy(src, dst, input_sems.at[n])
        for n, (src, dst) in enumerate((
            (owner_in, owner), (row_in, row), (count_in, count), (weight_in, weight), (innov_in, innov)))
    ]
    for copy in small:
        copy.start()
    flow_copy = pltpu.make_async_copy(courant, flow, flow_sem)
    flow_copy.start()
    flat_copy = pltpu.make_async_copy(courant_flat, flow_flat, flat_sem)
    obs_copy = pltpu.make_async_copy(obs.at[0], obs_v, obs_sem)
    obs_copy.start()
    flat_copy.start()

    def exists(d):
        return (li + d >= 0) & (li + d < n_lat)

    def guarded(d, run):
        if d == 0:
            run()
        else:
            pl.when(exists(d))(run)

    def lon_at(j):
        return lax.rem(lo + j + n_lon, n_lon)

    barrier = pltpu.get_barrier_semaphore()

    def greet(lat, lon):
        pl.semaphore_signal(barrier, inc=1, device_id={"lat": lat, "lon": lon}, device_id_type=MESH)

    if direct:
        for j in range(1, n_all):
            other = lax.rem(li * n_lon + lo + j, n_all)
            greet(lax.div(other, n_lon), lax.rem(other, n_lon))
    else:
        @pl.loop(1, n_lat)
        def _(j):
            greet(lax.rem(li + j, n_lat), lo)

        for d in (-1, 1):
            def hello(d=d):
                for j in range(1, n_lon):
                    greet(li + d, lon_at(j))
            guarded(d, hello)
        for j in range(1, n_lon):
            greet(li, lon_at(j))

    for copy in small:
        copy.wait()

    sub = lax.broadcasted_iota(jnp.int32, (cap, clon), 0)
    live = count[0, 0]
    owners = [owner[0, b] for b in range(cap)]
    levs = [lax.div(row[0, b], jnp.int32(clat)) for b in range(cap)]
    lats = [row[0, b] - levs[b] * clat for b in range(cap)]
    slots = []
    for b in range(cap):
        s = jnp.int32(0)
        for c in range(b):
            s = s + (owners[c] == owners[b]).astype(jnp.int32)
        slots.append(jnp.minimum(s, SLOT - 1))
    for o in range(n_lon):
        for s in range(SLOT):
            lev = jnp.int32(0)
            for b in range(cap):
                lev = jnp.where((owners[b] == o) & (slots[b] == s), levs[b], lev)
            ask_out[0, o * SLOT + s] = lev

    def column(values):
        tile = jnp.full((cap, clon), values[0], jnp.int32)
        for b in range(1, cap):
            tile = jnp.where(sub == b, values[b], tile)
        return tile

    level_tile, lat_tile, owner_tile = column(levs), column(lats), column(owners)

    def code_of(owner_now, lat_now):
        return (level_tile * n_lon + owner_now) * span + lat_now + clat

    lane = lax.broadcasted_iota(jnp.int32, (1, clon), 1)
    middle = clon // 2
    code_line = jnp.full((1, clon), -1, jnp.int32)
    for b in range(cap):
        code = (levs[b] * n_lon + owners[b]) * span + lats[b] + clat
        code_line = jnp.where(lane == b, jnp.where(b < live, code, -4 * span), code_line)
    for d in (-1, 0, 1):
        code_out[d + 1] = (code_line - clat * d).astype(F32)

    if direct:
        pl.semaphore_wait(barrier, n_all - 1)
    else:
        sides = (li > 0).astype(jnp.int32) + (li < n_lat - 1).astype(jnp.int32)
        pl.semaphore_wait(barrier, (n_lon - 1) + (n_lat - 1) + sides * (n_lon - 1))

    def wide(kind, d, j, src, dst):
        return pltpu.make_async_remote_copy(
            src_ref=src, dst_ref=dst, send_sem=wide_send.at[d + 1], recv_sem=wide_recv.at[kind],
            device_id={"lat": li + d, "lon": lon_at(j)}, device_id_type=MESH,
        )

    def rows_of(sem, ref, rows):
        whole = ref.at[pl.ds(0, rows)]
        return pltpu.make_async_remote_copy(
            src_ref=whole, dst_ref=whole, send_sem=sem, recv_sem=sem,
            device_id={"lat": li, "lon": lon_at(1)}, device_id_type=MESH)

    def with_sides(run):
        both = exists(-1) & exists(1)
        pl.when(both)(lambda: run(2))
        pl.when(jnp.logical_not(both))(lambda: run(1))

    def recv_rows(kind, own, side):
        with_sides(lambda sides: rows_of(wide_recv.at[kind], proxy, own + sides * side).wait_recv())

    def recv_wide(kind, rows):
        recv_rows(kind, (n_lon - 1) * rows, n_lon * rows)

    def slot_of(d, j, out):
        return (1 - d) * n_lon + (lo if out else lon_at(-j))

    def start_wide(make):
        for d in (-1, 1, 0):
            def run(d=d):
                for j in (2, 3, 1, 0) if n_lon == 4 else range(n_lon):
                    if (d, j) != (0, 0):
                        make(d, j).start()
            guarded(d, run)

    def code_make(d, j):
        return wide(0, d, j, code_out.at[d + 1], codes.at[slot_of(d, j, True)])

    def ask_make(d, j, out=True):
        return pltpu.make_async_remote_copy(
            src_ref=ask_out, dst_ref=ask_in.at[slot_of(d, j, out)],
            send_sem=ask_send, recv_sem=ask_recv.at[d + 1, j],
            device_id={"lat": li + d, "lon": lon_at(j)}, device_id_type=MESH)

    def place(d):
        return (HALO, clat) if d == 0 else ((0, HALO) if d == 1 else (HALO + clat, HALO))

    def main_make(d, j):
        first, size = place(d)
        src = main_out.at[j] if d == 0 else main_edge.at[(d + 1) // 2, j]
        return wide(1, d, j, src, main_in.at[:, lo, :, pl.ds(first, size), :])

    def strip_make(d, j):
        if d == 0:
            return wide(2, d, j, strip_out.at[j], strip_in.at[lo])
        return wide(3, d, j, strip_edge.at[(d + 1) // 2, j], strip_edge_in.at[(1 - d) // 2, lo])

    def term_make(rnd):
        def make(d, j):
            return wide(4 + rnd, d, j, terms.at[rnd, n_lon + lo], terms.at[rnd, slot_of(d, j, True)])
        return make

    def lat_make(f, d):
        return wide(7, d, 0, lat_out.at[f, (d + 1) // 2], lat_in.at[f, (1 - d) // 2])

    def lon_make(role, d):
        if d == 0:
            src, dst = lon_out.at[role], lon_in.at[role]
        else:
            src, dst = lon_edge_out.at[role, (d + 1) // 2], lon_edge_in.at[role, (1 - d) // 2]
        return wide(7, d, -1 if role == 0 else 1, src, dst)

    start_wide(ask_make)
    start_wide(code_make)
    codes[n_lon + lo] = code_out[1]

    flow_copy.wait()

    def flow_rows(f, lev, first, size):
        return flow[f, lev, first:first + size, :]

    def flow_levels(f, tile, lat):
        return flow_flat[pl.ds((f * levels + tile * 8) * clat + lat, 8, stride=clat), :]

    live_rows = sub < live
    w_rows = jnp.where(live_rows, weight[0], 0.0)
    wy_rows = w_rows * innov[0]
    stacked = jnp.concatenate([w_rows, wy_rows, jnp.zeros((clon - 2 * cap, clon), F32)], axis=0)
    columns = jnp.transpose(stacked)
    for b in range(cap):
        weight_wide[b] = jnp.broadcast_to(columns[:, b:b + 1], (clon, clon))
    wy_col = [columns[:, cap + b:cap + b + 1] for b in range(cap)]

    def spread(rnd, u_cols):
        out = [jnp.sum(obs_v[b] * u_cols[b], axis=0, keepdims=True) for b in range(cap)]
        terms[rnd, n_lon + lo] = jnp.concatenate(out, axis=0)
        start_wide(term_make(rnd))

    obs_copy.wait()
    spread(0, wy_col)

    flat_copy.wait()
    for f in range(2):
        for t in range(tiles):
            for k in range(STEPS):
                lat_out[f, 0, k, t] = flow_levels(f, t, k)
                lat_out[f, 1, k, t] = flow_levels(f, t, clat - STEPS + k)
    lane_lat = lane // width
    bunch = STEPS * width
    lane_bunch = lane // bunch
    for role in range(2):
        edges = [jnp.zeros((8, clon), F32)] * 2
        for f in range(2):
            for t in range(tiles):
                tile = jnp.zeros((8, clon), F32)
                for n in range(clat):
                    at = (n * width + role * width) % clon
                    tile = jnp.where(lane_lat == n, pltpu.roll(flow_levels(f, t, n), at, 1), tile)
                lon_out[role, f, t] = tile
                i = f * tiles + t
                for k, at in enumerate((i * bunch, (clon + i * bunch - (clat - STEPS) * width) % clon)):
                    edges[k] = jnp.where(lane_bunch == i, pltpu.roll(tile, at, 1), edges[k])
        for k in range(2):
            lon_edge_out[role, k] = edges[k]

    def send_dense(f):
        for d in (-1, 1):
            def send(d=d):
                lat_make(f, d).start()
                lon_make(f, d).start()
            guarded(d, send)
        lon_make(f, 0).start()

    send_dense(1)

    group = lane // HALO

    def answer(d, j):
        if d == 0:
            first, size = 0, clat
        elif d == 1:
            first, size = clat - HALO, HALO
        else:
            first, size = 0, HALO
        slot = (d + 1) * n_lon + lon_at(j)

        def asked(o, s):
            if (d, j) == (0, 0):
                return ask_out[0, o * SLOT + s]
            return ask_in[slot, 0, o * SLOT + s]

        tile = jnp.zeros((HALO, clon), F32)
        for s in range(SLOT):
            lev = asked(lo, s)
            right, left = asked(lon_at(-1), s), asked(lon_at(1), s)
            for f in range(2):
                rows = flow_rows(f, lev, first, size)
                if (d, j) == (0, 0):
                    main_in[f, lo, s, HALO:HALO + clat, :] = rows
                elif d == 0:
                    main_out[j, f, s] = rows
                else:
                    main_edge[(d + 1) // 2, j, f, s] = rows
                for k in range(size // HALO):
                    for g, lev_now, extra in ((s * 2 + f, right, 0), ((SLOT + s) * 2 + f, left, HALO)):
                        at = (k * middle + g * HALO + extra) % clon
                        moved = pltpu.roll(flow_rows(f, lev_now, first + k * HALO, HALO), at, 1)
                        tile = jnp.where(group == k * (middle // HALO) + g, moved, tile)
        if (d, j) == (0, 0):
            strip_in[lo] = tile
            return
        if d == 0:
            strip_out[j] = tile
        else:
            folded = pltpu.roll(pltpu.roll(tile, HALO // 2, 0), middle, 1)
            strip_edge[(d + 1) // 2, j] = jnp.where(lane < middle, tile, folded)[:HALO // 2]
        main_make(d, j).start()
        strip_make(d, j).start()

    def respond(d, j):
        def run():
            ask_make(-d, (n_lon - j) % n_lon, False).wait_recv()
            answer(d, j)
        guarded(d, run)

    answer(0, 0)
    near = [j for j in range(1, n_lon) if 2 * j != n_lon]
    far = [j for j in range(1, n_lon) if 2 * j == n_lon]
    for d, js in ((1, [0]), (-1, [0]), (1, near), (-1, near), (0, near), (1, far), (-1, far), (0, far)):
        for j in js:
            respond(d, j)

    pad = terms.shape[1] - n_src
    if pad:
        for rnd in range(3):
            terms[rnd, n_src:] = jnp.zeros((pad, cap, clon), F32)
    for d in (-1, 1):
        @pl.when(jnp.logical_not(exists(d)))
        def _(d=d):
            first = (d + 1) * n_lon
            codes[first:first + n_lon] = jnp.full((n_lon, 1, clon), -4.0 * span, F32)
            for rnd in range(3):
                terms[rnd, first:first + n_lon] = jnp.zeros((n_lon, cap, clon), F32)
            lat0 = 0 if d == -1 else HALO + clat
            main_in[:, :, :, lat0:lat0 + HALO, :] = jnp.zeros((2, n_lon, SLOT, HALO, clon), F32)
            strip_edge_in[(d + 1) // 2] = jnp.zeros((n_lon, HALO // 2, clon), F32)
            lat_in[:, (d + 1) // 2] = jnp.zeros((2, STEPS, tiles, 8, clon), F32)
            lon_edge_in[:, (d + 1) // 2] = jnp.zeros((2, 8, clon), F32)

    recv_wide(0, 1)
    code_parts = []
    for first in range(0, n_blocks, clon):
        line = jnp.full((1, clon), -4.0 * span, F32)
        for k in range(clon // cap):
            slot = first // cap + k
            if slot < n_src:
                line = jnp.where(lane // cap == k, pltpu.roll(codes[slot], k * cap, 1), line)
        code_parts.append(line)
    code_row = code_parts[0] if len(code_parts) == 1 else jnp.concatenate(code_parts, axis=1)

    def wide_tile(tile):
        return jnp.concatenate([tile] * (n_blocks // clon), axis=1) if n_blocks > clon else tile[:, :n_blocks]

    def matches(place_code):
        return jnp.where(place_code.astype(F32) == code_row, 1.0, 0.0).astype(BF16)

    for part, shift in enumerate((0, n_lon - 1, 1)):
        tile = wide_tile(code_of(lax.rem(owner_tile + shift, n_lon), lat_tile))
        for d in range(0, PAD_WIN, 2):
            rows = matches(jnp.concatenate([tile + (d - HALO), tile + (d + 1 - HALO)], axis=0))
            if part == 0:
                hot_main[d * cap:(d + 2) * cap, :] = rows
            else:
                hot_side[d * cap:(d + 2) * cap, (part - 1) * n_blocks:part * n_blocks] = rows

    def build_dense():
        lev_codes = lax.broadcasted_iota(jnp.int32, (levels, n_blocks), 0) * (n_lon * span)
        for part, shift in enumerate((0, n_lon - 1, 1)):
            for d in range(ring):
                rows = matches(lev_codes + (lon_at(shift) * span + (d - STEPS + clat)))
                if part == 0:
                    dense_main[d * levels:(d + 1) * levels, :] = rows
                else:
                    dense_side[d * levels:(d + 1) * levels, (part - 1) * n_blocks:part * n_blocks] = rows

    last_lane = lane == clon - 1
    first_lane = lane == 0

    def lon_up(m, s):
        mr, sr = pltpu.roll(m, clon - 1, 1), pltpu.roll(s, clon - 1, 1)
        return jnp.where(last_lane, sr, mr), jnp.where(last_lane, mr, sr)

    def lon_down(m, s):
        mr, sr = pltpu.roll(m, 1, 1), pltpu.roll(s, 1, 1)
        return jnp.where(first_lane, sr, mr), jnp.where(first_lane, mr, sr)

    def term_parts(rnd):
        flat = terms[rnd].reshape(n_blocks, clon)
        halves = [jnp.where(lane >= middle, flat, 0.0), jnp.where(lane < middle, flat, 0.0)]
        return split2(flat), split2(jnp.concatenate(halves, axis=0))

    def load_window(rnd):
        main_parts, side_parts = term_parts(rnd)
        field[0] = dot2(hot_main[...], main_parts).reshape(PAD_WIN, cap, clon)
        field[1] = dot2(hot_side[...], side_parts).reshape(PAD_WIN, cap, clon)

    def adjoint(rate, main, side, first, last):
        a, b, e, f, keep = range(5)
        for _ in range(STEPS):
            a_main = {d: rate(a, 0, d) * main[d] for d in range(first + 2, last + 1)}
            b_main = {d: rate(b, 0, d) * main[d] for d in range(first, last - 1)}
            a_side = {d: rate(a, 1, d) * side[d] for d in range(first + 3, last)}
            b_side = {d: rate(b, 1, d) * side[d] for d in range(first + 1, last - 2)}
            new_main, new_side = {}, {}
            for d in range(first + 1, last):
                up = lon_up(rate(e, 0, d) * main[d], rate(e, 1, d) * side[d])
                down = lon_down(rate(f, 0, d) * main[d], rate(f, 1, d) * side[d])
                new_main[d] = rate(keep, 0, d) * main[d] + a_main[d + 1] + b_main[d - 1] + up[0] + down[0]
                if first + 2 <= d < last - 1:
                    new_side[d] = rate(keep, 1, d) * side[d] + a_side[d + 1] + b_side[d - 1] + up[1] + down[1]
            main, side = new_main, new_side
            first, last = first + 1, last - 1
        return main, side

    recv_wide(4, cap)
    load_window(0)

    def unpack(sources, offset, first):
        for o in range(n_lon):
            from_right, from_left = sources[(o + 1) % n_lon], sources[(o - 1) % n_lon]
            for s in range(SLOT):
                for f in range(2):
                    at = offset + (s * 2 + f) * HALO
                    right = pltpu.roll(from_right, (clon - at) % clon, 1)
                    at = offset + ((SLOT + s) * 2 + f + 1) * HALO
                    left = pltpu.roll(from_left, (2 * clon - at) % clon, 1)
                    side_in[f, o, s, first:first + HALO, :] = jnp.where(lane < middle, right, left)

    rows_of(wide_recv.at[2], proxy, (n_lon - 1) * HALO).wait_recv()
    own_strips = [strip_in[o] for o in range(n_lon)]
    for k in range(clat // HALO):
        unpack(own_strips, k * middle, (k + 1) * HALO)
    recv_rows(3, 0, n_lon * HALO // 2)
    for k in range(2):
        edges = []
        for o in range(n_lon):
            edge = strip_edge_in[k, o]
            edges.append(jnp.concatenate([edge, pltpu.roll(edge, middle, 1)], axis=0))
        unpack(edges, 0, k * (HALO + clat))
    recv_rows(1, (n_lon - 1) * 2 * SLOT * clat, n_lon * 2 * SLOT * HALO)
    send_dense(0)

    def gather(ref, f, d):
        tile = None
        for b in range(cap):
            line = ref[f, owners[b], slots[b], pl.ds(lats[b] + d, 1), :]
            tile = jnp.broadcast_to(line, (cap, clon)) if tile is None else jnp.where(sub == b, line, tile)
        return tile

    for d in range(WIN):
        for side, ref in enumerate((main_in, side_in)):
            if d in (0, WIN - 1):
                if side == 0:
                    c0 = gather(ref, 0, d)
                    win_rates[1 if d == 0 else 0, d, side] = jnp.maximum(-c0 if d == 0 else c0, 0.0)
                continue
            for k, value in enumerate(split_rates(gather(ref, 0, d), gather(ref, 1, d))):
                win_rates[k, d, side] = value

    def window_model():
        a, b, e, f, keep = range(5)
        main = {d: field[0, d] for d in range(WIN)}
        side = {d: field[1, d] for d in range(1, WIN - 1)}
        main, side = adjoint(lambda k, n, d: win_rates[k, d, n], main, side, 0, WIN - 1)
        for d in list(main):
            lat_now = lat_tile + (li * clat + d - HALO)
            inside = (lat_now >= 0) & (lat_now < n_lat * clat)
            main[d] = jnp.where(inside, main[d], 0.0)
            if d in side:
                side[d] = jnp.where(inside, side[d], 0.0)
        for step in range(STEPS):
            reach = STEPS - 1 - step
            new_main, new_side = {}, {}
            for d in range(HALO - reach, HALO + reach + 1):
                down, up = lon_down(main[d], side[d]), lon_up(main[d], side[d])
                new_main[d] = (win_rates[keep, d, 0] * main[d] + win_rates[a, d, 0] * main[d - 1] + win_rates[b, d, 0] * main[d + 1]
                               + win_rates[e, d, 0] * down[0] + win_rates[f, d, 0] * up[0])
                if abs(d - HALO) < reach:
                    new_side[d] = (win_rates[keep, d, 1] * side[d] + win_rates[a, d, 1] * side[d - 1]
                                   + win_rates[b, d, 1] * side[d + 1] + win_rates[e, d, 1] * down[1] + win_rates[f, d, 1] * up[1])
            main, side = new_main, new_side
        seen = main[HALO]
        return [jnp.sum(obs_v[b] * seen[b:b + 1, :], axis=1, keepdims=True) for b in range(cap)]

    dense_own, dense_side_rows = 4 * tiles * 8, 2 * STEPS * tiles * 8 + 2 * 8

    def recv_dense():
        recv_rows(7, dense_own, dense_side_rows)
        for t in range(tiles):
            for d in range(ring):
                lat = d - STEPS
                if lat < 0:
                    main, edge, at = [lat_in[f, 0, d, t] for f in range(2)], 0, d
                elif lat >= clat:
                    main, edge, at = [lat_in[f, 1, lat - clat, t] for f in range(2)], 1, lat - clat
                else:
                    main, edge, at = [flow_levels(f, t, lat) for f in range(2)], None, lat
                side = []
                for f in range(2):
                    if edge is None:
                        first, pair = at * width, [lon_in[role, f, t] for role in range(2)]
                    else:
                        first, pair = (f * tiles + t) * bunch + at * width, [lon_edge_in[role, edge] for role in range(2)]
                    side.append(jnp.where(lane < middle, pltpu.roll(pair[0], (clon - first) % clon, 1),
                                          pltpu.roll(pair[1], (2 * clon - width - first) % clon, 1)))
                for n, pair in enumerate((main, side)):
                    for k, value in enumerate(split_rates(*pair)):
                        dense_rates[k, n, t, d] = value

    def dense(rnd):
        main_parts, side_parts = term_parts(rnd)
        dense_field[0] = dot2(dense_main[...], main_parts).reshape(ring, tiles, 8, clon)
        dense_field[1] = dot2(dense_side[...], side_parts).reshape(ring, tiles, 8, clon)

        @pl.loop(0, tiles, unroll=tiles)
        def _(t):
            main = {d: dense_field[0, d, t] for d in range(ring)}
            side = {d: dense_field[1, d, t] for d in range(1, ring - 1)}
            main, _ = adjoint(lambda k, n, d: dense_rates[k, n, t, d], main, side, 0, ring - 1)
            for lat in range(clat):
                parts[rnd, t, lat] = main[lat + STEPS]

    def red_make(n, ref, own, lat, lon):
        return pltpu.make_async_remote_copy(
            src_ref=ref.at[own], dst_ref=ref.at[own], send_sem=red_sems.at[n], recv_sem=red_sems.at[n + 1],
            device_id={"lat": lat, "lon": lon}, device_id_type=MESH)

    def red_all(n, ref, size):
        whole = ref.at[pl.ds(0, size)]
        return pltpu.make_async_remote_copy(
            src_ref=whole, dst_ref=whole, send_sem=red_sems.at[n], recv_sem=red_sems.at[n + 1],
            device_id={"lat": li, "lon": lon_at(1)}, device_id_type=MESH)

    def reduce_start(line):
        if direct:
            me = li * n_lon + lo
            red_far[me] = line
            for j in range(1, n_all):
                other = lax.rem(me + j, n_all)
                red_make(2, red_far, me, lax.div(other, n_lon), lax.rem(other, n_lon)).start()
        else:
            red_lon[lo] = line
            for j in range(1, n_lon):
                red_make(0, red_lon, lo, li, lon_at(j)).start()

    def reduce_turn():
        if not direct:
            red_all(0, red_lon, n_lon - 1).wait_recv()
            red_far[li] = jnp.sum(red_lon[...], axis=0)

            @pl.loop(1, n_lat)
            def _(j):
                red_make(2, red_far, li, lax.rem(li + j, n_lat), lo).start()

    far_size = n_all if direct else n_lat

    def packed(cols):
        tile = jnp.zeros((clon, clon), F32)
        for b in range(cap):
            tile = jnp.where(lane == b, cols[b], tile)
        return tile

    p1 = window_model()
    spread(1, [weight_wide[b] * p1[b] for b in range(cap)])
    build_dense()
    recv_wide(5, cap)
    load_window(1)
    g1 = window_model()
    spread(2, [weight_wide[b] * g1[b] for b in range(cap)])
    p_all, g_all = packed(p1), packed(g1)
    u_all = columns * p_all
    line = jnp.zeros((1, clon), F32)
    for n, value in enumerate((pltpu.roll(columns, clon - cap, 1) * p_all, u_all * p_all, u_all * g_all, columns * g_all * g_all)):
        line = line + pltpu.roll(jnp.sum(value, axis=0, keepdims=True), n * cap, 1)
    reduce_start(line)
    recv_dense()
    dense(0)
    reduce_turn()
    dense(1)
    recv_wide(6, cap)
    dense(2)
    red_all(2, red_far, far_size - 1).wait_recv()

    line = jnp.sum(red_far[...], axis=0)
    sums = [jnp.sum(jnp.where(lane // cap == n, line, 0.0), axis=1, keepdims=True) for n in range(4)]
    bb, s1, tt, s3 = sums
    scale = bb + s1
    alpha1, left1 = bb / scale, s1 / scale
    rr = left1 * (left1 * bb - alpha1 * s1) - alpha1 * (left1 * s1 - alpha1 * tt)
    sr1 = left1 * s1 - alpha1 * tt
    srr = left1 * sr1 - alpha1 * (left1 * tt - alpha1 * s3)
    beta = rr / bb
    curve = rr + beta * beta * bb + (srr + 2.0 * beta * sr1 + beta * beta * s1)
    alpha2 = rr / curve
    mix = left1 + beta
    inc_b, inc_t = alpha1 + alpha2 * mix, -alpha2 * alpha1
    res_b, res_t, res_2 = left1 - alpha2 * mix, -alpha1 - alpha2 * (mix - alpha1), alpha2 * alpha1
    for t in range(tiles):
        for lat in range(clat):
            b0, t1, t2 = (parts[rnd, t, lat] for rnd in range(3))
            rows = pl.ds(t * 8 * clat + lat, 8, stride=clat)
            inc_out[rows, :] = inc_b * b0 + inc_t * t1
            res_out[rows, :] = res_b * b0 + res_t * t1 + res_2 * t2

    for d in (-1, 1, 0):
        def sent(d=d):
            edge = HALO if d else clat
            strip = HALO // 2 if d else HALO
            rows = (n_lon if d else n_lon - 1) * (1 + 2 * SLOT * edge + strip + 3 * cap)
            rows_of(wide_send.at[d + 1], proxy, rows + (dense_side_rows if d else dense_own)).wait_send()
        guarded(d, sent)
    with_sides(lambda sides: rows_of(ask_send, ask_in, n_lon - 1 + sides * n_lon).wait_send())
    if not direct:
        red_all(0, red_lon, n_lon - 1).wait_send()
    red_all(2, red_far, far_size - 1).wait_send()


def store_kernel(inc, res, inc_out, res_out, sems):
    pairs = ((inc, inc_out), (res, res_out))
    copies = [pltpu.make_async_copy(src, dst, sems.at[n]) for n, (src, dst) in enumerate(pairs)]
    for copy in copies:
        copy.start()
    for copy in copies:
        copy.wait()


def shards(n_lat, n_lon, courant, obs_matrix, obs_weight, innovation, block_owner, block_row, block_count):
    _, levels, clat, clon = courant.shape
    cap = block_row.shape[1]
    tiles = levels // 8
    ring = clat + 2 * STEPS
    rows = clat + 2 * HALO
    unit = clon // cap
    src_pad = -(-3 * n_lon // unit) * unit
    n_blocks = src_pad * cap
    anywhere = pl.BlockSpec(memory_space=pl.ANY)
    dma = pltpu.SemaphoreType.DMA

    def f32(*shape):
        return pltpu.VMEM(shape, F32)

    def bf16(*shape):
        return pltpu.VMEM(shape, BF16)

    def i32(*shape):
        return pltpu.SMEM(shape, jnp.int32)

    flat = (levels * clat, clon)
    fields = pl.pallas_call(
        functools.partial(kernel, n_lat, n_lon),
        out_shape=(f32(*flat), f32(*flat)),
        in_specs=[anywhere] * 8,
        out_specs=(pl.BlockSpec(memory_space=pltpu.VMEM),) * 2,
        scratch_shapes=[
            f32(2, levels, clat, clon),
            f32(2 * levels * clat, clon),
            f32(cap, clon, clon),
            f32(3, src_pad, cap, clon),
            f32(3 * n_lon, 1, clon),
            f32(3, 1, clon),
            bf16(PAD_WIN * cap, n_blocks),
            bf16(PAD_WIN * cap, 2 * n_blocks),
            bf16(ring * levels, n_blocks),
            bf16(ring * levels, 2 * n_blocks),
            f32(2, PAD_WIN, cap, clon),
            f32(2, ring, tiles, 8, clon),
            f32(n_lon, 2, SLOT, clat, clon),
            f32(2, n_lon, 2, SLOT, HALO, clon),
            f32(n_lon, HALO, clon),
            f32(2, n_lon, HALO // 2, clon),
            f32(2, n_lon, SLOT, rows, clon),
            f32(n_lon, HALO, clon),
            f32(2, n_lon, HALO // 2, clon),
            f32(2, n_lon, SLOT, rows, clon),
            f32(5, WIN, 2, cap, clon),
            f32(2, 2, STEPS, tiles, 8, clon),
            f32(2, 2, STEPS, tiles, 8, clon),
            f32(2, 2, tiles, 8, clon),
            f32(2, 2, tiles, 8, clon),
            f32(2, 2, 8, clon),
            f32(2, 2, 8, clon),
            f32(5, 2, tiles, ring, 8, clon),
            f32(cap, clon, clon),
            f32(3, tiles, clat, 8, clon),
            f32(n_lon, 1, clon),
            f32(n_lat * n_lon if n_lat * n_lon <= DIRECT else n_lat, 1, clon),
            f32(n_lon * 256, clon),
            i32(1, n_lon * SLOT),
            i32(3 * n_lon, 1, n_lon * SLOT),
            dma, dma, dma,
            dma((3,)), dma((8,)), dma, dma((3, n_lon)),
            dma((4,)),
            f32(1, cap, clon), f32(1, cap, clon),
            i32(1, cap), i32(1, cap), i32(1, 1),
            dma((5,)),
        ],
        compiler_params=pltpu.CompilerParams(collective_id=0, has_side_effects=True),
    )(courant, courant.reshape(2 * levels * clat, clon), obs_matrix, obs_weight, innovation, block_owner[:, :, 0], block_row, block_count)
    out = jax.ShapeDtypeStruct(flat, F32)
    stored = pl.pallas_call(
        store_kernel,
        out_shape=(out, out),
        in_specs=[anywhere] * 2,
        out_specs=(anywhere,) * 2,
        scratch_shapes=[dma((2,))],
    )(*[pltpu.with_memory_space_constraint(field, pltpu.VMEM) for field in fields])
    return tuple(field.reshape(levels, clat, clon) for field in stored)


def solution(mesh):
    placed = (
        P(None, None, "lat", "lon"),
        P("lat", "lon", None, None),
        P("lat", "lon", None),
        P("lat", "lon", None),
        P("lat", "lon", None),
        P("lat", "lon"),
        P("lat", "lon"),
    )
    return jax.shard_map(
        functools.partial(shards, mesh.shape["lat"], mesh.shape["lon"]),
        mesh=mesh,
        in_specs=placed,
        out_specs=(P(None, "lat", "lon"), P(None, "lat", "lon")),
        check_vma=False,
    )
```

```python
import functools

import jax
import jax.numpy as jnp
from jax import lax
from jax.experimental import pallas as pl
from jax.experimental.pallas import tpu as pltpu
from jax.sharding import PartitionSpec as P

STEPS = 4
HALO = 2 * STEPS
SLOT = 2
DIRECT = 64
WIN = 2 * HALO + 1
PAD_WIN = WIN + 1
MESH = pl.DeviceIdType.MESH
F32 = jnp.float32
BF16 = jnp.bfloat16


def split2(x):
    hi = x.astype(BF16)
    return hi, (x - hi.astype(F32)).astype(BF16)


def dot2(onehot, parts):
    total = None
    for part in parts:
        term = jnp.dot(onehot, part, preferred_element_type=F32)
        total = term if total is None else total + term
    return total


def split_rates(c0, c1):
    a, b = jnp.maximum(c0, 0.0), jnp.maximum(-c0, 0.0)
    e, f = jnp.maximum(c1, 0.0), jnp.maximum(-c1, 0.0)
    return a, b, e, f, 1.0 - a - b - e - f


def kernel(
    n_lat, n_lon,
    courant, courant_flat, obs, weight_in, innov_in, owner_in, row_in, count_in,
    inc_out, res_out,
    flow, flow_flat, obs_v, terms, codes, code_out, hot_main, hot_side, dense_main, dense_side, field, dense_field,
    main_out, main_edge, strip_out, strip_edge, main_in, strip_in, strip_edge_in, side_in,
    win_rates, lat_out, lat_in, lon_out, lon_in, lon_edge_out, lon_edge_in, dense_rates, weight_wide, parts, red_lon, red_far,
    proxy, ask_out, ask_in,
    obs_sem, flow_sem, flat_sem, wide_send, wide_recv, ask_send, ask_recv, red_sems, token,
    weight, innov, owner, row, count, input_sems,
):
    li = lax.axis_index("lat")
    lo = lax.axis_index("lon")
    clon = flow_flat.shape[1]
    cap = obs_v.shape[0]
    tiles, clat = parts.shape[1:3]
    levels = tiles * 8
    n_src = 3 * n_lon
    n_blocks = terms.shape[1] * cap
    span = 4 * clat
    ring = clat + 2 * STEPS
    width = clon // clat
    n_all = n_lat * n_lon
    direct = n_all <= DIRECT

    small = [
        pltpu.make_async_copy(src, dst, input_sems.at[n])
        for n, (src, dst) in enumerate((
            (owner_in, owner), (row_in, row), (count_in, count), (weight_in, weight), (innov_in, innov)))
    ]
    for copy in small:
        copy.start()
    flow_copy = pltpu.make_async_copy(courant, flow, flow_sem)
    flow_copy.start()
    flat_copy = pltpu.make_async_copy(courant_flat, flow_flat, flat_sem)
    obs_copy = pltpu.make_async_copy(obs.at[0], obs_v, obs_sem)
    obs_copy.start()
    flat_copy.start()

    def exists(d):
        return (li + d >= 0) & (li + d < n_lat)

    def guarded(d, run):
        if d == 0:
            run()
        else:
            pl.when(exists(d))(run)

    def lon_at(j):
        return lax.rem(lo + j + n_lon, n_lon)

    barrier = pltpu.get_barrier_semaphore()

    def greet(lat, lon):
        pl.semaphore_signal(barrier, inc=1, device_id={"lat": lat, "lon": lon}, device_id_type=MESH)

    for d in (-1, 1):
        def hello(d=d):
            for j in range(n_lon):
                greet(li + d, lon_at(j))
        guarded(d, hello)
    for j in range(1, n_lon):
        greet(li, lon_at(j))
    sides = (li > 0).astype(jnp.int32) + (li < n_lat - 1).astype(jnp.int32)
    greeted = n_lon - 1 + sides * n_lon
    if not direct:
        @pl.loop(2, n_lat - 1)
        def _(j):
            greet(lax.rem(li + j, n_lat), lo)

        @pl.when(sides == 1)
        def _():
            greet(jnp.where(li == 0, n_lat - 1, 0), lo)
        greeted = greeted + n_lat - 3 + (sides == 1).astype(jnp.int32)

    for copy in small:
        copy.wait()

    sub = lax.broadcasted_iota(jnp.int32, (cap, clon), 0)
    live = count[0, 0]
    owners = [owner[0, b] for b in range(cap)]
    levs = [lax.div(row[0, b], jnp.int32(clat)) for b in range(cap)]
    lats = [row[0, b] - levs[b] * clat for b in range(cap)]
    slots = []
    for b in range(cap):
        s = jnp.int32(0)
        for c in range(b):
            s = s + (owners[c] == owners[b]).astype(jnp.int32)
        slots.append(jnp.minimum(s, SLOT - 1))
    for o in range(n_lon):
        for s in range(SLOT):
            lev = jnp.int32(0)
            for b in range(cap):
                lev = jnp.where((owners[b] == o) & (slots[b] == s), levs[b], lev)
            ask_out[0, o * SLOT + s] = lev

    def column(values):
        tile = jnp.full((cap, clon), values[0], jnp.int32)
        for b in range(1, cap):
            tile = jnp.where(sub == b, values[b], tile)
        return tile

    level_tile, lat_tile, owner_tile = column(levs), column(lats), column(owners)

    def code_of(owner_now, lat_now):
        return (level_tile * n_lon + owner_now) * span + lat_now + clat

    lane = lax.broadcasted_iota(jnp.int32, (1, clon), 1)
    middle = clon // 2
    code_line = jnp.full((1, clon), -1, jnp.int32)
    for b in range(cap):
        code = (levs[b] * n_lon + owners[b]) * span + lats[b] + clat
        code_line = jnp.where(lane == b, jnp.where(b < live, code, -4 * span), code_line)
    for d in (-1, 0, 1):
        code_out[d + 1] = (code_line - clat * d).astype(F32)

    pl.semaphore_wait(barrier, greeted)

    rounds = n_lat - 2 if direct else 0

    def news(k):
        if 0 < k <= rounds:
            for d in (-1, 1):
                guarded(-d, lambda d=d: pl.semaphore_wait(token.at[(1 - d) // 2], 1))
        if k < rounds:
            for d in (-1, 1):
                guarded(d, lambda d=d: pl.semaphore_signal(
                    token.at[(1 - d) // 2], inc=1, device_id={"lat": li + d, "lon": lo}, device_id_type=MESH))

    def wide(kind, d, j, src, dst):
        return pltpu.make_async_remote_copy(
            src_ref=src, dst_ref=dst, send_sem=wide_send.at[d + 1], recv_sem=wide_recv.at[kind],
            device_id={"lat": li + d, "lon": lon_at(j)}, device_id_type=MESH,
        )

    def rows_of(sem, ref, rows):
        whole = ref.at[pl.ds(0, rows)]
        return pltpu.make_async_remote_copy(
            src_ref=whole, dst_ref=whole, send_sem=sem, recv_sem=sem,
            device_id={"lat": li, "lon": lon_at(1)}, device_id_type=MESH)

    def with_sides(run):
        both = exists(-1) & exists(1)
        pl.when(both)(lambda: run(2))
        pl.when(jnp.logical_not(both))(lambda: run(1))

    def recv_rows(kind, own, side):
        with_sides(lambda sides: rows_of(wide_recv.at[kind], proxy, own + sides * side).wait_recv())

    def recv_wide(kind, rows):
        recv_rows(kind, (n_lon - 1) * rows, n_lon * rows)

    def slot_of(d, j, out):
        return (1 - d) * n_lon + (lo if out else lon_at(-j))

    def start_wide(make):
        for d in (-1, 1, 0):
            def run(d=d):
                for j in (2, 3, 1, 0) if n_lon == 4 else range(n_lon):
                    if (d, j) != (0, 0):
                        make(d, j).start()
            guarded(d, run)

    def code_make(d, j):
        return wide(0, d, j, code_out.at[d + 1], codes.at[slot_of(d, j, True)])

    def ask_make(d, j, out=True):
        return pltpu.make_async_remote_copy(
            src_ref=ask_out, dst_ref=ask_in.at[slot_of(d, j, out)],
            send_sem=ask_send, recv_sem=ask_recv.at[d + 1, j],
            device_id={"lat": li + d, "lon": lon_at(j)}, device_id_type=MESH)

    def place(d):
        return (HALO, clat) if d == 0 else ((0, HALO) if d == 1 else (HALO + clat, HALO))

    def main_make(d, j):
        first, size = place(d)
        src = main_out.at[j] if d == 0 else main_edge.at[(d + 1) // 2, j]
        return wide(1, d, j, src, main_in.at[:, lo, :, pl.ds(first, size), :])

    def strip_make(d, j):
        if d == 0:
            return wide(2, d, j, strip_out.at[j], strip_in.at[lo])
        return wide(3, d, j, strip_edge.at[(d + 1) // 2, j], strip_edge_in.at[(1 - d) // 2, lo])

    def term_make(rnd):
        def make(d, j):
            return wide(4 + rnd, d, j, terms.at[rnd, n_lon + lo], terms.at[rnd, slot_of(d, j, True)])
        return make

    def lat_make(f, d):
        return wide(7, d, 0, lat_out.at[f, (d + 1) // 2], lat_in.at[f, (1 - d) // 2])

    def lon_make(role, d):
        if d == 0:
            src, dst = lon_out.at[role], lon_in.at[role]
        else:
            src, dst = lon_edge_out.at[role, (d + 1) // 2], lon_edge_in.at[role, (1 - d) // 2]
        return wide(7, d, -1 if role == 0 else 1, src, dst)

    start_wide(ask_make)
    start_wide(code_make)
    news(0)
    codes[n_lon + lo] = code_out[1]

    flow_copy.wait()

    def flow_rows(f, lev, first, size):
        return flow[f, lev, first:first + size, :]

    def flow_levels(f, tile, lat):
        return flow_flat[pl.ds((f * levels + tile * 8) * clat + lat, 8, stride=clat), :]

    live_rows = sub < live
    w_rows = jnp.where(live_rows, weight[0], 0.0)
    wy_rows = w_rows * innov[0]
    stacked = jnp.concatenate([w_rows, wy_rows, jnp.zeros((clon - 2 * cap, clon), F32)], axis=0)
    columns = jnp.transpose(stacked)
    for b in range(cap):
        weight_wide[b] = jnp.broadcast_to(columns[:, b:b + 1], (clon, clon))
    wy_col = [columns[:, cap + b:cap + b + 1] for b in range(cap)]

    def spread(rnd, u_cols):
        out = [jnp.sum(obs_v[b] * u_cols[b], axis=0, keepdims=True) for b in range(cap)]
        terms[rnd, n_lon + lo] = jnp.concatenate(out, axis=0)
        start_wide(term_make(rnd))

    obs_copy.wait()
    spread(0, wy_col)

    flat_copy.wait()
    for f in range(2):
        for t in range(tiles):
            for k in range(STEPS):
                lat_out[f, 0, k, t] = flow_levels(f, t, k)
                lat_out[f, 1, k, t] = flow_levels(f, t, clat - STEPS + k)
    lane_lat = lane // width
    bunch = STEPS * width
    lane_bunch = lane // bunch
    for role in range(2):
        edges = [jnp.zeros((8, clon), F32)] * 2
        for f in range(2):
            for t in range(tiles):
                tile = jnp.zeros((8, clon), F32)
                for n in range(clat):
                    at = (n * width + role * width) % clon
                    tile = jnp.where(lane_lat == n, pltpu.roll(flow_levels(f, t, n), at, 1), tile)
                lon_out[role, f, t] = tile
                i = f * tiles + t
                for k, at in enumerate((i * bunch, (clon + i * bunch - (clat - STEPS) * width) % clon)):
                    edges[k] = jnp.where(lane_bunch == i, pltpu.roll(tile, at, 1), edges[k])
        for k in range(2):
            lon_edge_out[role, k] = edges[k]

    def send_dense(f):
        for d in (-1, 1):
            def send(d=d):
                lat_make(f, d).start()
                lon_make(f, d).start()
            guarded(d, send)
        lon_make(f, 0).start()

    send_dense(1)

    group = lane // HALO

    def answer(d, j):
        if d == 0:
            first, size = 0, clat
        elif d == 1:
            first, size = clat - HALO, HALO
        else:
            first, size = 0, HALO
        slot = (d + 1) * n_lon + lon_at(j)

        def asked(o, s):
            if (d, j) == (0, 0):
                return ask_out[0, o * SLOT + s]
            return ask_in[slot, 0, o * SLOT + s]

        tile = jnp.zeros((HALO, clon), F32)
        for s in range(SLOT):
            lev = asked(lo, s)
            right, left = asked(lon_at(-1), s), asked(lon_at(1), s)
            for f in range(2):
                rows = flow_rows(f, lev, first, size)
                if (d, j) == (0, 0):
                    main_in[f, lo, s, HALO:HALO + clat, :] = rows
                elif d == 0:
                    main_out[j, f, s] = rows
                else:
                    main_edge[(d + 1) // 2, j, f, s] = rows
                for k in range(size // HALO):
                    for g, lev_now, extra in ((s * 2 + f, right, 0), ((SLOT + s) * 2 + f, left, HALO)):
                        at = (k * middle + g * HALO + extra) % clon
                        moved = pltpu.roll(flow_rows(f, lev_now, first + k * HALO, HALO), at, 1)
                        tile = jnp.where(group == k * (middle // HALO) + g, moved, tile)
        if (d, j) == (0, 0):
            strip_in[lo] = tile
            return
        if d == 0:
            strip_out[j] = tile
        else:
            folded = pltpu.roll(pltpu.roll(tile, HALO // 2, 0), middle, 1)
            strip_edge[(d + 1) // 2, j] = jnp.where(lane < middle, tile, folded)[:HALO // 2]
        main_make(d, j).start()
        strip_make(d, j).start()

    def respond(d, j):
        def run():
            ask_make(-d, (n_lon - j) % n_lon, False).wait_recv()
            answer(d, j)
        guarded(d, run)

    answer(0, 0)
    near = [j for j in range(1, n_lon) if 2 * j != n_lon]
    far = [j for j in range(1, n_lon) if 2 * j == n_lon]
    for d, js in ((1, [0]), (-1, [0]), (1, near), (-1, near), (0, near), (1, far), (-1, far), (0, far)):
        for j in js:
            respond(d, j)

    news(1)
    pad = terms.shape[1] - n_src
    if pad:
        for rnd in range(3):
            terms[rnd, n_src:] = jnp.zeros((pad, cap, clon), F32)
    for d in (-1, 1):
        @pl.when(jnp.logical_not(exists(d)))
        def _(d=d):
            first = (d + 1) * n_lon
            codes[first:first + n_lon] = jnp.full((n_lon, 1, clon), -4.0 * span, F32)
            for rnd in range(3):
                terms[rnd, first:first + n_lon] = jnp.zeros((n_lon, cap, clon), F32)
            lat0 = 0 if d == -1 else HALO + clat
            main_in[:, :, :, lat0:lat0 + HALO, :] = jnp.zeros((2, n_lon, SLOT, HALO, clon), F32)
            strip_edge_in[(d + 1) // 2] = jnp.zeros((n_lon, HALO // 2, clon), F32)
            lat_in[:, (d + 1) // 2] = jnp.zeros((2, STEPS, tiles, 8, clon), F32)
            lon_edge_in[:, (d + 1) // 2] = jnp.zeros((2, 8, clon), F32)

    recv_wide(0, 1)
    code_parts = []
    for first in range(0, n_blocks, clon):
        line = jnp.full((1, clon), -4.0 * span, F32)
        for k in range(clon // cap):
            slot = first // cap + k
            if slot < n_src:
                line = jnp.where(lane // cap == k, pltpu.roll(codes[slot], k * cap, 1), line)
        code_parts.append(line)
    code_row = code_parts[0] if len(code_parts) == 1 else jnp.concatenate(code_parts, axis=1)

    def wide_tile(tile):
        return jnp.concatenate([tile] * (n_blocks // clon), axis=1) if n_blocks > clon else tile[:, :n_blocks]

    def matches(place_code):
        return jnp.where(place_code.astype(F32) == code_row, 1.0, 0.0).astype(BF16)

    for part, shift in enumerate((0, n_lon - 1, 1)):
        tile = wide_tile(code_of(lax.rem(owner_tile + shift, n_lon), lat_tile))
        for d in range(0, PAD_WIN, 2):
            rows = matches(jnp.concatenate([tile + (d - HALO), tile + (d + 1 - HALO)], axis=0))
            if part == 0:
                hot_main[d * cap:(d + 2) * cap, :] = rows
            else:
                hot_side[d * cap:(d + 2) * cap, (part - 1) * n_blocks:part * n_blocks] = rows

    def build_dense():
        lev_codes = lax.broadcasted_iota(jnp.int32, (levels, n_blocks), 0) * (n_lon * span)
        for part, shift in enumerate((0, n_lon - 1, 1)):
            for d in range(ring):
                rows = matches(lev_codes + (lon_at(shift) * span + (d - STEPS + clat)))
                if part == 0:
                    dense_main[d * levels:(d + 1) * levels, :] = rows
                else:
                    dense_side[d * levels:(d + 1) * levels, (part - 1) * n_blocks:part * n_blocks] = rows

    last_lane = lane == clon - 1
    first_lane = lane == 0

    def lon_up(m, s):
        mr, sr = pltpu.roll(m, clon - 1, 1), pltpu.roll(s, clon - 1, 1)
        return jnp.where(last_lane, sr, mr), jnp.where(last_lane, mr, sr)

    def lon_down(m, s):
        mr, sr = pltpu.roll(m, 1, 1), pltpu.roll(s, 1, 1)
        return jnp.where(first_lane, sr, mr), jnp.where(first_lane, mr, sr)

    def term_parts(rnd):
        flat = terms[rnd].reshape(n_blocks, clon)
        halves = [jnp.where(lane >= middle, flat, 0.0), jnp.where(lane < middle, flat, 0.0)]
        return split2(flat), split2(jnp.concatenate(halves, axis=0))

    def load_window(rnd):
        main_parts, side_parts = term_parts(rnd)
        field[0] = dot2(hot_main[...], main_parts).reshape(PAD_WIN, cap, clon)
        field[1] = dot2(hot_side[...], side_parts).reshape(PAD_WIN, cap, clon)

    def adjoint(rate, main, side, first, last):
        a, b, e, f, keep = range(5)
        for _ in range(STEPS):
            a_main = {d: rate(a, 0, d) * main[d] for d in range(first + 2, last + 1)}
            b_main = {d: rate(b, 0, d) * main[d] for d in range(first, last - 1)}
            a_side = {d: rate(a, 1, d) * side[d] for d in range(first + 3, last)}
            b_side = {d: rate(b, 1, d) * side[d] for d in range(first + 1, last - 2)}
            new_main, new_side = {}, {}
            for d in range(first + 1, last):
                up = lon_up(rate(e, 0, d) * main[d], rate(e, 1, d) * side[d])
                down = lon_down(rate(f, 0, d) * main[d], rate(f, 1, d) * side[d])
                new_main[d] = rate(keep, 0, d) * main[d] + a_main[d + 1] + b_main[d - 1] + up[0] + down[0]
                if first + 2 <= d < last - 1:
                    new_side[d] = rate(keep, 1, d) * side[d] + a_side[d + 1] + b_side[d - 1] + up[1] + down[1]
            main, side = new_main, new_side
            first, last = first + 1, last - 1
        return main, side

    recv_wide(4, cap)
    load_window(0)
    news(2)

    def unpack(sources, offset, first):
        for o in range(n_lon):
            from_right, from_left = sources[(o + 1) % n_lon], sources[(o - 1) % n_lon]
            for s in range(SLOT):
                for f in range(2):
                    at = offset + (s * 2 + f) * HALO
                    right = pltpu.roll(from_right, (clon - at) % clon, 1)
                    at = offset + ((SLOT + s) * 2 + f + 1) * HALO
                    left = pltpu.roll(from_left, (2 * clon - at) % clon, 1)
                    side_in[f, o, s, first:first + HALO, :] = jnp.where(lane < middle, right, left)

    rows_of(wide_recv.at[2], proxy, (n_lon - 1) * HALO).wait_recv()
    own_strips = [strip_in[o] for o in range(n_lon)]
    for k in range(clat // HALO):
        unpack(own_strips, k * middle, (k + 1) * HALO)
    news(3)
    recv_rows(3, 0, n_lon * HALO // 2)
    for k in range(2):
        edges = []
        for o in range(n_lon):
            edge = strip_edge_in[k, o]
            edges.append(jnp.concatenate([edge, pltpu.roll(edge, middle, 1)], axis=0))
        unpack(edges, 0, k * (HALO + clat))
    recv_rows(1, (n_lon - 1) * 2 * SLOT * clat, n_lon * 2 * SLOT * HALO)
    send_dense(0)

    def gather(ref, f, d):
        tile = None
        for b in range(cap):
            line = ref[f, owners[b], slots[b], pl.ds(lats[b] + d, 1), :]
            tile = jnp.broadcast_to(line, (cap, clon)) if tile is None else jnp.where(sub == b, line, tile)
        return tile

    for d in range(WIN):
        for side, ref in enumerate((main_in, side_in)):
            if d in (0, WIN - 1):
                if side == 0:
                    c0 = gather(ref, 0, d)
                    win_rates[1 if d == 0 else 0, d, side] = jnp.maximum(-c0 if d == 0 else c0, 0.0)
                continue
            for k, value in enumerate(split_rates(gather(ref, 0, d), gather(ref, 1, d))):
                win_rates[k, d, side] = value

    def window_model():
        a, b, e, f, keep = range(5)
        main = {d: field[0, d] for d in range(WIN)}
        side = {d: field[1, d] for d in range(1, WIN - 1)}
        main, side = adjoint(lambda k, n, d: win_rates[k, d, n], main, side, 0, WIN - 1)
        for d in list(main):
            lat_now = lat_tile + (li * clat + d - HALO)
            inside = (lat_now >= 0) & (lat_now < n_lat * clat)
            main[d] = jnp.where(inside, main[d], 0.0)
            if d in side:
                side[d] = jnp.where(inside, side[d], 0.0)
        for step in range(STEPS):
            reach = STEPS - 1 - step
            new_main, new_side = {}, {}
            for d in range(HALO - reach, HALO + reach + 1):
                down, up = lon_down(main[d], side[d]), lon_up(main[d], side[d])
                new_main[d] = (win_rates[keep, d, 0] * main[d] + win_rates[a, d, 0] * main[d - 1] + win_rates[b, d, 0] * main[d + 1]
                               + win_rates[e, d, 0] * down[0] + win_rates[f, d, 0] * up[0])
                if abs(d - HALO) < reach:
                    new_side[d] = (win_rates[keep, d, 1] * side[d] + win_rates[a, d, 1] * side[d - 1]
                                   + win_rates[b, d, 1] * side[d + 1] + win_rates[e, d, 1] * down[1] + win_rates[f, d, 1] * up[1])
            main, side = new_main, new_side
        seen = main[HALO]
        return [jnp.sum(obs_v[b] * seen[b:b + 1, :], axis=1, keepdims=True) for b in range(cap)]

    dense_own, dense_side_rows = 4 * tiles * 8, 2 * STEPS * tiles * 8 + 2 * 8

    def recv_dense():
        recv_rows(7, dense_own, dense_side_rows)
        for t in range(tiles):
            for d in range(ring):
                lat = d - STEPS
                if lat < 0:
                    main, edge, at = [lat_in[f, 0, d, t] for f in range(2)], 0, d
                elif lat >= clat:
                    main, edge, at = [lat_in[f, 1, lat - clat, t] for f in range(2)], 1, lat - clat
                else:
                    main, edge, at = [flow_levels(f, t, lat) for f in range(2)], None, lat
                side = []
                for f in range(2):
                    if edge is None:
                        first, pair = at * width, [lon_in[role, f, t] for role in range(2)]
                    else:
                        first, pair = (f * tiles + t) * bunch + at * width, [lon_edge_in[role, edge] for role in range(2)]
                    side.append(jnp.where(lane < middle, pltpu.roll(pair[0], (clon - first) % clon, 1),
                                          pltpu.roll(pair[1], (2 * clon - width - first) % clon, 1)))
                for n, pair in enumerate((main, side)):
                    for k, value in enumerate(split_rates(*pair)):
                        dense_rates[k, n, t, d] = value

    def dense(rnd):
        main_parts, side_parts = term_parts(rnd)
        dense_field[0] = dot2(dense_main[...], main_parts).reshape(ring, tiles, 8, clon)
        dense_field[1] = dot2(dense_side[...], side_parts).reshape(ring, tiles, 8, clon)

        @pl.loop(0, tiles, unroll=tiles)
        def _(t):
            main = {d: dense_field[0, d, t] for d in range(ring)}
            side = {d: dense_field[1, d, t] for d in range(1, ring - 1)}
            main, _ = adjoint(lambda k, n, d: dense_rates[k, n, t, d], main, side, 0, ring - 1)
            for lat in range(clat):
                parts[rnd, t, lat] = main[lat + STEPS]

    def red_make(n, ref, own, lat, lon):
        return pltpu.make_async_remote_copy(
            src_ref=ref.at[own], dst_ref=ref.at[own], send_sem=red_sems.at[n], recv_sem=red_sems.at[n + 1],
            device_id={"lat": lat, "lon": lon}, device_id_type=MESH)

    def red_all(n, ref, size):
        whole = ref.at[pl.ds(0, size)]
        return pltpu.make_async_remote_copy(
            src_ref=whole, dst_ref=whole, send_sem=red_sems.at[n], recv_sem=red_sems.at[n + 1],
            device_id={"lat": li, "lon": lon_at(1)}, device_id_type=MESH)

    def reduce_start(line):
        if direct:
            me = li * n_lon + lo
            red_far[me] = line
            for j in range(1, n_all):
                other = lax.rem(me + j, n_all)
                red_make(2, red_far, me, lax.div(other, n_lon), lax.rem(other, n_lon)).start()
        else:
            red_lon[lo] = line
            for j in range(1, n_lon):
                red_make(0, red_lon, lo, li, lon_at(j)).start()

    def reduce_turn():
        if not direct:
            red_all(0, red_lon, n_lon - 1).wait_recv()
            red_far[li] = jnp.sum(red_lon[...], axis=0)

            @pl.loop(1, n_lat)
            def _(j):
                red_make(2, red_far, li, lax.rem(li + j, n_lat), lo).start()

    far_size = n_all if direct else n_lat

    def packed(cols):
        tile = jnp.zeros((clon, clon), F32)
        for b in range(cap):
            tile = jnp.where(lane == b, cols[b], tile)
        return tile

    p1 = window_model()
    spread(1, [weight_wide[b] * p1[b] for b in range(cap)])
    news(4)
    build_dense()
    news(5)
    recv_wide(5, cap)
    load_window(1)
    g1 = window_model()
    spread(2, [weight_wide[b] * g1[b] for b in range(cap)])
    p_all, g_all = packed(p1), packed(g1)
    u_all = columns * p_all
    line = jnp.zeros((1, clon), F32)
    for n, value in enumerate((pltpu.roll(columns, clon - cap, 1) * p_all, u_all * p_all, u_all * g_all, columns * g_all * g_all)):
        line = line + pltpu.roll(jnp.sum(value, axis=0, keepdims=True), n * cap, 1)
    for k in range(6, max(rounds, 6) + 1):
        news(k)
    reduce_start(line)
    recv_dense()
    dense(0)
    reduce_turn()
    dense(1)
    recv_wide(6, cap)
    dense(2)
    red_all(2, red_far, far_size - 1).wait_recv()

    line = jnp.sum(red_far[...], axis=0)
    sums = [jnp.sum(jnp.where(lane // cap == n, line, 0.0), axis=1, keepdims=True) for n in range(4)]
    bb, s1, tt, s3 = sums
    scale = bb + s1
    alpha1, left1 = bb / scale, s1 / scale
    rr = left1 * (left1 * bb - alpha1 * s1) - alpha1 * (left1 * s1 - alpha1 * tt)
    sr1 = left1 * s1 - alpha1 * tt
    srr = left1 * sr1 - alpha1 * (left1 * tt - alpha1 * s3)
    beta = rr / bb
    curve = rr + beta * beta * bb + (srr + 2.0 * beta * sr1 + beta * beta * s1)
    alpha2 = rr / curve
    mix = left1 + beta
    inc_b, inc_t = alpha1 + alpha2 * mix, -alpha2 * alpha1
    res_b, res_t, res_2 = left1 - alpha2 * mix, -alpha1 - alpha2 * (mix - alpha1), alpha2 * alpha1
    for t in range(tiles):
        for lat in range(clat):
            b0, t1, t2 = (parts[rnd, t, lat] for rnd in range(3))
            rows = pl.ds(t * 8 * clat + lat, 8, stride=clat)
            inc_out[rows, :] = inc_b * b0 + inc_t * t1
            res_out[rows, :] = res_b * b0 + res_t * t1 + res_2 * t2

    for d in (-1, 1, 0):
        def sent(d=d):
            edge = HALO if d else clat
            strip = HALO // 2 if d else HALO
            rows = (n_lon if d else n_lon - 1) * (1 + 2 * SLOT * edge + strip + 3 * cap)
            rows_of(wide_send.at[d + 1], proxy, rows + (dense_side_rows if d else dense_own)).wait_send()
        guarded(d, sent)
    with_sides(lambda sides: rows_of(ask_send, ask_in, n_lon - 1 + sides * n_lon).wait_send())
    if not direct:
        red_all(0, red_lon, n_lon - 1).wait_send()
    red_all(2, red_far, far_size - 1).wait_send()


def store_kernel(inc, res, inc_out, res_out, sems):
    pairs = ((inc, inc_out), (res, res_out))
    copies = [pltpu.make_async_copy(src, dst, sems.at[n]) for n, (src, dst) in enumerate(pairs)]
    for copy in copies:
        copy.start()
    for copy in copies:
        copy.wait()


def shards(n_lat, n_lon, courant, obs_matrix, obs_weight, innovation, block_owner, block_row, block_count):
    _, levels, clat, clon = courant.shape
    cap = block_row.shape[1]
    tiles = levels // 8
    ring = clat + 2 * STEPS
    rows = clat + 2 * HALO
    unit = clon // cap
    src_pad = -(-3 * n_lon // unit) * unit
    n_blocks = src_pad * cap
    anywhere = pl.BlockSpec(memory_space=pl.ANY)
    dma = pltpu.SemaphoreType.DMA

    def f32(*shape):
        return pltpu.VMEM(shape, F32)

    def bf16(*shape):
        return pltpu.VMEM(shape, BF16)

    def i32(*shape):
        return pltpu.SMEM(shape, jnp.int32)

    flat = (levels * clat, clon)
    fields = pl.pallas_call(
        functools.partial(kernel, n_lat, n_lon),
        out_shape=(f32(*flat), f32(*flat)),
        in_specs=[anywhere] * 8,
        out_specs=(pl.BlockSpec(memory_space=pltpu.VMEM),) * 2,
        scratch_shapes=[
            f32(2, levels, clat, clon),
            f32(2 * levels * clat, clon),
            f32(cap, clon, clon),
            f32(3, src_pad, cap, clon),
            f32(3 * n_lon, 1, clon),
            f32(3, 1, clon),
            bf16(PAD_WIN * cap, n_blocks),
            bf16(PAD_WIN * cap, 2 * n_blocks),
            bf16(ring * levels, n_blocks),
            bf16(ring * levels, 2 * n_blocks),
            f32(2, PAD_WIN, cap, clon),
            f32(2, ring, tiles, 8, clon),
            f32(n_lon, 2, SLOT, clat, clon),
            f32(2, n_lon, 2, SLOT, HALO, clon),
            f32(n_lon, HALO, clon),
            f32(2, n_lon, HALO // 2, clon),
            f32(2, n_lon, SLOT, rows, clon),
            f32(n_lon, HALO, clon),
            f32(2, n_lon, HALO // 2, clon),
            f32(2, n_lon, SLOT, rows, clon),
            f32(5, WIN, 2, cap, clon),
            f32(2, 2, STEPS, tiles, 8, clon),
            f32(2, 2, STEPS, tiles, 8, clon),
            f32(2, 2, tiles, 8, clon),
            f32(2, 2, tiles, 8, clon),
            f32(2, 2, 8, clon),
            f32(2, 2, 8, clon),
            f32(5, 2, tiles, ring, 8, clon),
            f32(cap, clon, clon),
            f32(3, tiles, clat, 8, clon),
            f32(n_lon, 1, clon),
            f32(n_lat * n_lon if n_lat * n_lon <= DIRECT else n_lat, 1, clon),
            f32(n_lon * 256, clon),
            i32(1, n_lon * SLOT),
            i32(3 * n_lon, 1, n_lon * SLOT),
            dma, dma, dma,
            dma((3,)), dma((8,)), dma, dma((3, n_lon)),
            dma((4,)),
            pltpu.SemaphoreType.REGULAR((2,)),
            f32(1, cap, clon), f32(1, cap, clon),
            i32(1, cap), i32(1, cap), i32(1, 1),
            dma((5,)),
        ],
        compiler_params=pltpu.CompilerParams(collective_id=0, has_side_effects=True),
    )(courant, courant.reshape(2 * levels * clat, clon), obs_matrix, obs_weight, innovation, block_owner[:, :, 0], block_row, block_count)
    out = jax.ShapeDtypeStruct(flat, F32)
    stored = pl.pallas_call(
        store_kernel,
        out_shape=(out, out),
        in_specs=[anywhere] * 2,
        out_specs=(anywhere,) * 2,
        scratch_shapes=[dma((2,))],
    )(*[pltpu.with_memory_space_constraint(field, pltpu.VMEM) for field in fields])
    return tuple(field.reshape(levels, clat, clon) for field in stored)


def solution(mesh):
    placed = (
        P(None, None, "lat", "lon"),
        P("lat", "lon", None, None),
        P("lat", "lon", None),
        P("lat", "lon", None),
        P("lat", "lon", None),
        P("lat", "lon"),
        P("lat", "lon"),
    )
    return jax.shard_map(
        functools.partial(shards, mesh.shape["lat"], mesh.shape["lon"]),
        mesh=mesh,
        in_specs=placed,
        out_specs=(P(None, "lat", "lon"), P(None, "lat", "lon")),
        check_vma=False,
    )
```

```python
import functools

import jax
import jax.numpy as jnp
from jax import lax
from jax.experimental import pallas as pl
from jax.experimental.pallas import tpu as pltpu
from jax.sharding import PartitionSpec as P

STEPS = 4
HALO = 2 * STEPS
SLOT = 2
DIRECT = 64
WIN = 2 * HALO + 1
PAD_WIN = WIN + 1
MESH = pl.DeviceIdType.MESH
F32 = jnp.float32
BF16 = jnp.bfloat16


def split2(x):
    hi = x.astype(BF16)
    return hi, (x - hi.astype(F32)).astype(BF16)


def dot2(onehot, parts):
    total = None
    for part in parts:
        term = jnp.dot(onehot, part, preferred_element_type=F32)
        total = term if total is None else total + term
    return total


def split_rates(c0, c1):
    a, b = jnp.maximum(c0, 0.0), jnp.maximum(-c0, 0.0)
    e, f = jnp.maximum(c1, 0.0), jnp.maximum(-c1, 0.0)
    return a, b, e, f, 1.0 - a - b - e - f


def kernel(
    n_lat, n_lon,
    courant, courant_flat, obs, weight_in, innov_in, owner_in, row_in, count_in,
    inc_out, res_out,
    flow, flow_flat, obs_v, terms, codes, code_out, hot_main, hot_side, dense_main, dense_side, field, dense_field,
    main_out, main_edge, strip_out, strip_edge, main_in, strip_in, strip_edge_in, side_in,
    win_rates, lat_out, lat_in, lon_out, lon_in, lon_edge_out, lon_edge_in, dense_rates, weight_wide, parts, red_lon, red_far,
    proxy, ask_out, ask_in,
    obs_sem, flow_sem, flat_sem, wide_send, wide_recv, ask_send, ask_recv, red_sems, token,
    weight, innov, owner, row, count, input_sems,
):
    li = lax.axis_index("lat")
    lo = lax.axis_index("lon")
    clon = flow_flat.shape[1]
    cap = obs_v.shape[0]
    tiles, clat = parts.shape[1:3]
    levels = tiles * 8
    n_src = 3 * n_lon
    n_blocks = terms.shape[1] * cap
    span = 4 * clat
    ring = clat + 2 * STEPS
    width = clon // clat
    n_all = n_lat * n_lon
    direct = n_all <= DIRECT

    small = [
        pltpu.make_async_copy(src, dst, input_sems.at[n])
        for n, (src, dst) in enumerate((
            (owner_in, owner), (row_in, row), (count_in, count), (weight_in, weight), (innov_in, innov)))
    ]
    for copy in small:
        copy.start()
    flow_copy = pltpu.make_async_copy(courant, flow, flow_sem)
    flow_copy.start()
    flat_copy = pltpu.make_async_copy(courant_flat, flow_flat, flat_sem)
    obs_copy = pltpu.make_async_copy(obs.at[0], obs_v, obs_sem)
    obs_copy.start()
    flat_copy.start()

    def exists(d):
        return (li + d >= 0) & (li + d < n_lat)

    def guarded(d, run):
        if d == 0:
            run()
        else:
            pl.when(exists(d))(run)

    def lon_at(j):
        return lax.rem(lo + j + n_lon, n_lon)

    barrier = pltpu.get_barrier_semaphore()

    def greet(lat, lon):
        pl.semaphore_signal(barrier, inc=1, device_id={"lat": lat, "lon": lon}, device_id_type=MESH)

    for d in (-1, 1):
        def hello(d=d):
            for j in range(n_lon):
                greet(li + d, lon_at(j))
        guarded(d, hello)
    for j in range(1, n_lon):
        greet(li, lon_at(j))
    sides = (li > 0).astype(jnp.int32) + (li < n_lat - 1).astype(jnp.int32)
    greeted = n_lon - 1 + sides * n_lon
    if not direct:
        @pl.loop(2, n_lat - 1)
        def _(j):
            greet(lax.rem(li + j, n_lat), lo)

        @pl.when(sides == 1)
        def _():
            greet(jnp.where(li == 0, n_lat - 1, 0), lo)
        greeted = greeted + n_lat - 3 + (sides == 1).astype(jnp.int32)

    for copy in small:
        copy.wait()

    sub = lax.broadcasted_iota(jnp.int32, (cap, clon), 0)
    live = count[0, 0]
    owners = [owner[0, b] for b in range(cap)]
    levs = [lax.div(row[0, b], jnp.int32(clat)) for b in range(cap)]
    lats = [row[0, b] - levs[b] * clat for b in range(cap)]
    slots = []
    for b in range(cap):
        s = jnp.int32(0)
        for c in range(b):
            s = s + (owners[c] == owners[b]).astype(jnp.int32)
        slots.append(jnp.minimum(s, SLOT - 1))
    for o in range(n_lon):
        for s in range(SLOT):
            lev = jnp.int32(0)
            for b in range(cap):
                lev = jnp.where((owners[b] == o) & (slots[b] == s), levs[b], lev)
            ask_out[0, o * SLOT + s] = lev

    def column(values):
        tile = jnp.full((cap, clon), values[0], jnp.int32)
        for b in range(1, cap):
            tile = jnp.where(sub == b, values[b], tile)
        return tile

    level_tile, lat_tile, owner_tile = column(levs), column(lats), column(owners)

    def code_of(owner_now, lat_now):
        return (level_tile * n_lon + owner_now) * span + lat_now + clat

    lane = lax.broadcasted_iota(jnp.int32, (1, clon), 1)
    middle = clon // 2
    code_line = jnp.full((1, clon), -1, jnp.int32)
    for b in range(cap):
        code = (levs[b] * n_lon + owners[b]) * span + lats[b] + clat
        code_line = jnp.where(lane == b, jnp.where(b < live, code, -4 * span), code_line)
    for d in (-1, 0, 1):
        code_out[d + 1] = (code_line - clat * d).astype(F32)

    pl.semaphore_wait(barrier, greeted)

    rounds = n_lat - 2 if direct else 0

    def news(k):
        if 0 < k <= rounds:
            for d in (-1, 1):
                guarded(-d, lambda d=d: pl.semaphore_wait(token.at[(1 - d) // 2], 1))
        if k < rounds:
            for d in (-1, 1):
                guarded(d, lambda d=d: pl.semaphore_signal(
                    token.at[(1 - d) // 2], inc=1, device_id={"lat": li + d, "lon": lo}, device_id_type=MESH))

    def wide(kind, d, j, src, dst):
        return pltpu.make_async_remote_copy(
            src_ref=src, dst_ref=dst, send_sem=wide_send.at[d + 1], recv_sem=wide_recv.at[kind],
            device_id={"lat": li + d, "lon": lon_at(j)}, device_id_type=MESH,
        )

    def rows_of(sem, ref, rows):
        whole = ref.at[pl.ds(0, rows)]
        return pltpu.make_async_remote_copy(
            src_ref=whole, dst_ref=whole, send_sem=sem, recv_sem=sem,
            device_id={"lat": li, "lon": lon_at(1)}, device_id_type=MESH)

    def with_sides(run):
        both = exists(-1) & exists(1)
        pl.when(both)(lambda: run(2))
        pl.when(jnp.logical_not(both))(lambda: run(1))

    def recv_rows(kind, own, side):
        with_sides(lambda sides: rows_of(wide_recv.at[kind], proxy, own + sides * side).wait_recv())

    def recv_wide(kind, rows):
        recv_rows(kind, (n_lon - 1) * rows, n_lon * rows)

    def slot_of(d, j, out):
        return (1 - d) * n_lon + (lo if out else lon_at(-j))

    def start_wide(make):
        for d in (-1, 1, 0):
            def run(d=d):
                for j in (2, 3, 1, 0) if n_lon == 4 else range(n_lon):
                    if (d, j) != (0, 0):
                        make(d, j).start()
            guarded(d, run)

    def code_make(d, j):
        return wide(0, d, j, code_out.at[d + 1], codes.at[slot_of(d, j, True)])

    def ask_make(d, j, out=True):
        return pltpu.make_async_remote_copy(
            src_ref=ask_out, dst_ref=ask_in.at[slot_of(d, j, out)],
            send_sem=ask_send, recv_sem=ask_recv.at[d + 1, j],
            device_id={"lat": li + d, "lon": lon_at(j)}, device_id_type=MESH)

    def place(d):
        return (HALO, clat) if d == 0 else ((0, HALO) if d == 1 else (HALO + clat, HALO))

    def main_make(d, j):
        first, size = place(d)
        src = main_out.at[j] if d == 0 else main_edge.at[(d + 1) // 2, j]
        return wide(1, d, j, src, main_in.at[:, lo, :, pl.ds(first, size), :])

    def strip_make(d, j):
        if d == 0:
            return wide(2, d, j, strip_out.at[j], strip_in.at[lo])
        return wide(3, d, j, strip_edge.at[(d + 1) // 2, j], strip_edge_in.at[(1 - d) // 2, lo])

    def term_make(rnd):
        def make(d, j):
            return wide(4 + rnd, d, j, terms.at[rnd, n_lon + lo], terms.at[rnd, slot_of(d, j, True)])
        return make

    def lat_make(f, d):
        return wide(7, d, 0, lat_out.at[f, (d + 1) // 2], lat_in.at[f, (1 - d) // 2])

    def lon_make(role, d):
        if d == 0:
            src, dst = lon_out.at[role], lon_in.at[role]
        else:
            src, dst = lon_edge_out.at[role, (d + 1) // 2], lon_edge_in.at[role, (1 - d) // 2]
        return wide(7, d, -1 if role == 0 else 1, src, dst)

    start_wide(ask_make)
    start_wide(code_make)
    news(0)
    codes[n_lon + lo] = code_out[1]

    flow_copy.wait()

    def flow_rows(f, lev, first, size):
        return flow[f, lev, first:first + size, :]

    def flow_levels(f, tile, lat):
        return flow_flat[pl.ds((f * levels + tile * 8) * clat + lat, 8, stride=clat), :]

    live_rows = sub < live
    w_rows = jnp.where(live_rows, weight[0], 0.0)
    wy_rows = w_rows * innov[0]
    stacked = jnp.concatenate([w_rows, wy_rows, jnp.zeros((clon - 2 * cap, clon), F32)], axis=0)
    columns = jnp.transpose(stacked)
    for b in range(cap):
        weight_wide[b] = jnp.broadcast_to(columns[:, b:b + 1], (clon, clon))
    wy_col = [columns[:, cap + b:cap + b + 1] for b in range(cap)]

    def spread(rnd, u_cols):
        out = [jnp.sum(obs_v[b] * u_cols[b], axis=0, keepdims=True) for b in range(cap)]
        terms[rnd, n_lon + lo] = jnp.concatenate(out, axis=0)
        start_wide(term_make(rnd))

    obs_copy.wait()
    spread(0, wy_col)

    flat_copy.wait()
    for f in range(2):
        for t in range(tiles):
            for k in range(STEPS):
                lat_out[f, 0, k, t] = flow_levels(f, t, k)
                lat_out[f, 1, k, t] = flow_levels(f, t, clat - STEPS + k)
    lane_lat = lane // width
    bunch = STEPS * width
    lane_bunch = lane // bunch
    for role in range(2):
        edges = [jnp.zeros((8, clon), F32)] * 2
        for f in range(2):
            for t in range(tiles):
                tile = jnp.zeros((8, clon), F32)
                for n in range(clat):
                    at = (n * width + role * width) % clon
                    tile = jnp.where(lane_lat == n, pltpu.roll(flow_levels(f, t, n), at, 1), tile)
                lon_out[role, f, t] = tile
                i = f * tiles + t
                for k, at in enumerate((i * bunch, (clon + i * bunch - (clat - STEPS) * width) % clon)):
                    edges[k] = jnp.where(lane_bunch == i, pltpu.roll(tile, at, 1), edges[k])
        for k in range(2):
            lon_edge_out[role, k] = edges[k]

    def send_dense(f):
        for d in (-1, 1):
            def send(d=d):
                lat_make(f, d).start()
                lon_make(f, d).start()
            guarded(d, send)
        lon_make(f, 0).start()

    send_dense(1)

    group = lane // HALO

    def answer(d, j):
        if d == 0:
            first, size = 0, clat
        elif d == 1:
            first, size = clat - HALO, HALO
        else:
            first, size = 0, HALO
        slot = (d + 1) * n_lon + lon_at(j)

        def asked(o, s):
            if (d, j) == (0, 0):
                return ask_out[0, o * SLOT + s]
            return ask_in[slot, 0, o * SLOT + s]

        tile = jnp.zeros((HALO, clon), F32)
        for s in range(SLOT):
            lev = asked(lo, s)
            right, left = asked(lon_at(-1), s), asked(lon_at(1), s)
            for f in range(2):
                rows = flow_rows(f, lev, first, size)
                if (d, j) == (0, 0):
                    main_in[f, lo, s, HALO:HALO + clat, :] = rows
                elif d == 0:
                    main_out[j, f, s] = rows
                else:
                    main_edge[(d + 1) // 2, j, f, s] = rows
                for k in range(size // HALO):
                    for g, lev_now, extra in ((s * 2 + f, right, 0), ((SLOT + s) * 2 + f, left, HALO)):
                        at = (k * middle + g * HALO + extra) % clon
                        moved = pltpu.roll(flow_rows(f, lev_now, first + k * HALO, HALO), at, 1)
                        tile = jnp.where(group == k * (middle // HALO) + g, moved, tile)
        if (d, j) == (0, 0):
            strip_in[lo] = tile
            return
        if d == 0:
            strip_out[j] = tile
        else:
            folded = pltpu.roll(pltpu.roll(tile, HALO // 2, 0), middle, 1)
            strip_edge[(d + 1) // 2, j] = jnp.where(lane < middle, tile, folded)[:HALO // 2]
        main_make(d, j).start()
        strip_make(d, j).start()

    def respond(d, j):
        def run():
            ask_make(-d, (n_lon - j) % n_lon, False).wait_recv()
            answer(d, j)
        guarded(d, run)

    answer(0, 0)
    near = [j for j in range(1, n_lon) if 2 * j != n_lon]
    far = [j for j in range(1, n_lon) if 2 * j == n_lon]
    for d, js in ((0, near), (1, [0]), (-1, [0]), (1, near), (-1, near), (1, far), (-1, far), (0, far)):
        for j in js:
            respond(d, j)

    news(1)
    pad = terms.shape[1] - n_src
    if pad:
        for rnd in range(3):
            terms[rnd, n_src:] = jnp.zeros((pad, cap, clon), F32)
    for d in (-1, 1):
        @pl.when(jnp.logical_not(exists(d)))
        def _(d=d):
            first = (d + 1) * n_lon
            codes[first:first + n_lon] = jnp.full((n_lon, 1, clon), -4.0 * span, F32)
            for rnd in range(3):
                terms[rnd, first:first + n_lon] = jnp.zeros((n_lon, cap, clon), F32)
            lat0 = 0 if d == -1 else HALO + clat
            main_in[:, :, :, lat0:lat0 + HALO, :] = jnp.zeros((2, n_lon, SLOT, HALO, clon), F32)
            strip_edge_in[(d + 1) // 2] = jnp.zeros((n_lon, HALO // 2, clon), F32)
            lat_in[:, (d + 1) // 2] = jnp.zeros((2, STEPS, tiles, 8, clon), F32)
            lon_edge_in[:, (d + 1) // 2] = jnp.zeros((2, 8, clon), F32)

    recv_wide(0, 1)
    code_parts = []
    for first in range(0, n_blocks, clon):
        line = jnp.full((1, clon), -4.0 * span, F32)
        for k in range(clon // cap):
            slot = first // cap + k
            if slot < n_src:
                line = jnp.where(lane // cap == k, pltpu.roll(codes[slot], k * cap, 1), line)
        code_parts.append(line)
    code_row = code_parts[0] if len(code_parts) == 1 else jnp.concatenate(code_parts, axis=1)

    def wide_tile(tile):
        return jnp.concatenate([tile] * (n_blocks // clon), axis=1) if n_blocks > clon else tile[:, :n_blocks]

    def matches(place_code):
        return jnp.where(place_code.astype(F32) == code_row, 1.0, 0.0).astype(BF16)

    for part, shift in enumerate((0, n_lon - 1, 1)):
        tile = wide_tile(code_of(lax.rem(owner_tile + shift, n_lon), lat_tile))
        for d in range(0, PAD_WIN, 2):
            rows = matches(jnp.concatenate([tile + (d - HALO), tile + (d + 1 - HALO)], axis=0))
            if part == 0:
                hot_main[d * cap:(d + 2) * cap, :] = rows
            else:
                hot_side[d * cap:(d + 2) * cap, (part - 1) * n_blocks:part * n_blocks] = rows

    def build_dense():
        lev_codes = lax.broadcasted_iota(jnp.int32, (levels, n_blocks), 0) * (n_lon * span)
        for part, shift in enumerate((0, n_lon - 1, 1)):
            for d in range(ring):
                rows = matches(lev_codes + (lon_at(shift) * span + (d - STEPS + clat)))
                if part == 0:
                    dense_main[d * levels:(d + 1) * levels, :] = rows
                else:
                    dense_side[d * levels:(d + 1) * levels, (part - 1) * n_blocks:part * n_blocks] = rows

    last_lane = lane == clon - 1
    first_lane = lane == 0

    def lon_up(m, s):
        mr, sr = pltpu.roll(m, clon - 1, 1), pltpu.roll(s, clon - 1, 1)
        return jnp.where(last_lane, sr, mr), jnp.where(last_lane, mr, sr)

    def lon_down(m, s):
        mr, sr = pltpu.roll(m, 1, 1), pltpu.roll(s, 1, 1)
        return jnp.where(first_lane, sr, mr), jnp.where(first_lane, mr, sr)

    def term_parts(rnd):
        flat = terms[rnd].reshape(n_blocks, clon)
        halves = [jnp.where(lane >= middle, flat, 0.0), jnp.where(lane < middle, flat, 0.0)]
        return split2(flat), split2(jnp.concatenate(halves, axis=0))

    def load_window(rnd):
        main_parts, side_parts = term_parts(rnd)
        field[0] = dot2(hot_main[...], main_parts).reshape(PAD_WIN, cap, clon)
        field[1] = dot2(hot_side[...], side_parts).reshape(PAD_WIN, cap, clon)

    def adjoint(rate, main, side, first, last):
        a, b, e, f, keep = range(5)
        for _ in range(STEPS):
            a_main = {d: rate(a, 0, d) * main[d] for d in range(first + 2, last + 1)}
            b_main = {d: rate(b, 0, d) * main[d] for d in range(first, last - 1)}
            a_side = {d: rate(a, 1, d) * side[d] for d in range(first + 3, last)}
            b_side = {d: rate(b, 1, d) * side[d] for d in range(first + 1, last - 2)}
            new_main, new_side = {}, {}
            for d in range(first + 1, last):
                up = lon_up(rate(e, 0, d) * main[d], rate(e, 1, d) * side[d])
                down = lon_down(rate(f, 0, d) * main[d], rate(f, 1, d) * side[d])
                new_main[d] = rate(keep, 0, d) * main[d] + a_main[d + 1] + b_main[d - 1] + up[0] + down[0]
                if first + 2 <= d < last - 1:
                    new_side[d] = rate(keep, 1, d) * side[d] + a_side[d + 1] + b_side[d - 1] + up[1] + down[1]
            main, side = new_main, new_side
            first, last = first + 1, last - 1
        return main, side

    recv_wide(4, cap)
    load_window(0)
    news(2)

    def unpack(sources, offset, first):
        for o in range(n_lon):
            from_right, from_left = sources[(o + 1) % n_lon], sources[(o - 1) % n_lon]
            for s in range(SLOT):
                for f in range(2):
                    at = offset + (s * 2 + f) * HALO
                    right = pltpu.roll(from_right, (clon - at) % clon, 1)
                    at = offset + ((SLOT + s) * 2 + f + 1) * HALO
                    left = pltpu.roll(from_left, (2 * clon - at) % clon, 1)
                    side_in[f, o, s, first:first + HALO, :] = jnp.where(lane < middle, right, left)

    rows_of(wide_recv.at[2], proxy, (n_lon - 1) * HALO).wait_recv()
    own_strips = [strip_in[o] for o in range(n_lon)]
    for k in range(clat // HALO):
        unpack(own_strips, k * middle, (k + 1) * HALO)
    news(3)
    recv_rows(3, 0, n_lon * HALO // 2)
    for k in range(2):
        edges = []
        for o in range(n_lon):
            edge = strip_edge_in[k, o]
            edges.append(jnp.concatenate([edge, pltpu.roll(edge, middle, 1)], axis=0))
        unpack(edges, 0, k * (HALO + clat))
    recv_rows(1, (n_lon - 1) * 2 * SLOT * clat, n_lon * 2 * SLOT * HALO)
    send_dense(0)

    def gather(ref, f, d):
        tile = None
        for b in range(cap):
            line = ref[f, owners[b], slots[b], pl.ds(lats[b] + d, 1), :]
            tile = jnp.broadcast_to(line, (cap, clon)) if tile is None else jnp.where(sub == b, line, tile)
        return tile

    for d in range(WIN):
        for side, ref in enumerate((main_in, side_in)):
            if d in (0, WIN - 1):
                if side == 0:
                    c0 = gather(ref, 0, d)
                    win_rates[1 if d == 0 else 0, d, side] = jnp.maximum(-c0 if d == 0 else c0, 0.0)
                continue
            for k, value in enumerate(split_rates(gather(ref, 0, d), gather(ref, 1, d))):
                win_rates[k, d, side] = value

    def window_model():
        a, b, e, f, keep = range(5)
        main = {d: field[0, d] for d in range(WIN)}
        side = {d: field[1, d] for d in range(1, WIN - 1)}
        main, side = adjoint(lambda k, n, d: win_rates[k, d, n], main, side, 0, WIN - 1)
        for d in list(main):
            lat_now = lat_tile + (li * clat + d - HALO)
            inside = (lat_now >= 0) & (lat_now < n_lat * clat)
            main[d] = jnp.where(inside, main[d], 0.0)
            if d in side:
                side[d] = jnp.where(inside, side[d], 0.0)
        for step in range(STEPS):
            reach = STEPS - 1 - step
            new_main, new_side = {}, {}
            for d in range(HALO - reach, HALO + reach + 1):
                down, up = lon_down(main[d], side[d]), lon_up(main[d], side[d])
                new_main[d] = (win_rates[keep, d, 0] * main[d] + win_rates[a, d, 0] * main[d - 1] + win_rates[b, d, 0] * main[d + 1]
                               + win_rates[e, d, 0] * down[0] + win_rates[f, d, 0] * up[0])
                if abs(d - HALO) < reach:
                    new_side[d] = (win_rates[keep, d, 1] * side[d] + win_rates[a, d, 1] * side[d - 1]
                                   + win_rates[b, d, 1] * side[d + 1] + win_rates[e, d, 1] * down[1] + win_rates[f, d, 1] * up[1])
            main, side = new_main, new_side
        seen = main[HALO]
        return [jnp.sum(obs_v[b] * seen[b:b + 1, :], axis=1, keepdims=True) for b in range(cap)]

    dense_own, dense_side_rows = 4 * tiles * 8, 2 * STEPS * tiles * 8 + 2 * 8

    def recv_dense():
        recv_rows(7, dense_own, dense_side_rows)
        for t in range(tiles):
            for d in range(ring):
                lat = d - STEPS
                if lat < 0:
                    main, edge, at = [lat_in[f, 0, d, t] for f in range(2)], 0, d
                elif lat >= clat:
                    main, edge, at = [lat_in[f, 1, lat - clat, t] for f in range(2)], 1, lat - clat
                else:
                    main, edge, at = [flow_levels(f, t, lat) for f in range(2)], None, lat
                side = []
                for f in range(2):
                    if edge is None:
                        first, pair = at * width, [lon_in[role, f, t] for role in range(2)]
                    else:
                        first, pair = (f * tiles + t) * bunch + at * width, [lon_edge_in[role, edge] for role in range(2)]
                    side.append(jnp.where(lane < middle, pltpu.roll(pair[0], (clon - first) % clon, 1),
                                          pltpu.roll(pair[1], (2 * clon - width - first) % clon, 1)))
                for n, pair in enumerate((main, side)):
                    for k, value in enumerate(split_rates(*pair)):
                        dense_rates[k, n, t, d] = value

    def dense(rnd):
        main_parts, side_parts = term_parts(rnd)
        dense_field[0] = dot2(dense_main[...], main_parts).reshape(ring, tiles, 8, clon)
        dense_field[1] = dot2(dense_side[...], side_parts).reshape(ring, tiles, 8, clon)

        @pl.loop(0, tiles, unroll=tiles)
        def _(t):
            main = {d: dense_field[0, d, t] for d in range(ring)}
            side = {d: dense_field[1, d, t] for d in range(1, ring - 1)}
            main, _ = adjoint(lambda k, n, d: dense_rates[k, n, t, d], main, side, 0, ring - 1)
            for lat in range(clat):
                parts[rnd, t, lat] = main[lat + STEPS]

    def red_make(n, ref, own, lat, lon):
        return pltpu.make_async_remote_copy(
            src_ref=ref.at[own], dst_ref=ref.at[own], send_sem=red_sems.at[n], recv_sem=red_sems.at[n + 1],
            device_id={"lat": lat, "lon": lon}, device_id_type=MESH)

    def red_all(n, ref, size):
        whole = ref.at[pl.ds(0, size)]
        return pltpu.make_async_remote_copy(
            src_ref=whole, dst_ref=whole, send_sem=red_sems.at[n], recv_sem=red_sems.at[n + 1],
            device_id={"lat": li, "lon": lon_at(1)}, device_id_type=MESH)

    def reduce_start(line):
        if direct:
            me = li * n_lon + lo
            red_far[me] = line
            for j in sorted(range(1, n_all), key=lambda j: abs(2 * j - n_all)):
                other = lax.rem(me + j, n_all)
                red_make(2, red_far, me, lax.div(other, n_lon), lax.rem(other, n_lon)).start()
        else:
            red_lon[lo] = line
            for j in range(1, n_lon):
                red_make(0, red_lon, lo, li, lon_at(j)).start()

    def reduce_turn():
        if not direct:
            red_all(0, red_lon, n_lon - 1).wait_recv()
            red_far[li] = jnp.sum(red_lon[...], axis=0)

            @pl.loop(1, n_lat)
            def _(j):
                red_make(2, red_far, li, lax.rem(li + j, n_lat), lo).start()

    far_size = n_all if direct else n_lat

    def packed(cols):
        tile = jnp.zeros((clon, clon), F32)
        for b in range(cap):
            tile = jnp.where(lane == b, cols[b], tile)
        return tile

    def line_of(value, n):
        return pltpu.roll(jnp.sum(value, axis=0, keepdims=True), n * cap, 1)

    p1 = window_model()
    spread(1, [weight_wide[b] * p1[b] for b in range(cap)])
    news(4)
    build_dense()
    p_all = packed(p1)
    u_all = columns * p_all
    news(5)
    line = line_of(pltpu.roll(columns, clon - cap, 1) * p_all, 0) + line_of(u_all * p_all, 1)
    recv_wide(5, cap)
    load_window(1)
    g1 = window_model()
    g_all = packed(g1)
    line = line + line_of(u_all * g_all, 2) + line_of(columns * g_all * g_all, 3)
    for k in range(6, max(rounds, 6) + 1):
        news(k)
    reduce_start(line)
    spread(2, [weight_wide[b] * g1[b] for b in range(cap)])
    recv_dense()
    dense(0)
    reduce_turn()
    dense(1)
    recv_wide(6, cap)
    dense(2)
    red_all(2, red_far, far_size - 1).wait_recv()

    line = jnp.sum(red_far[...], axis=0)
    sums = [jnp.sum(jnp.where(lane // cap == n, line, 0.0), axis=1, keepdims=True) for n in range(4)]
    bb, s1, tt, s3 = sums
    scale = bb + s1
    alpha1, left1 = bb / scale, s1 / scale
    rr = left1 * (left1 * bb - alpha1 * s1) - alpha1 * (left1 * s1 - alpha1 * tt)
    sr1 = left1 * s1 - alpha1 * tt
    srr = left1 * sr1 - alpha1 * (left1 * tt - alpha1 * s3)
    beta = rr / bb
    curve = rr + beta * beta * bb + (srr + 2.0 * beta * sr1 + beta * beta * s1)
    alpha2 = rr / curve
    mix = left1 + beta
    inc_b, inc_t = alpha1 + alpha2 * mix, -alpha2 * alpha1
    res_b, res_t, res_2 = left1 - alpha2 * mix, -alpha1 - alpha2 * (mix - alpha1), alpha2 * alpha1
    for t in range(tiles):
        for lat in range(clat):
            b0, t1, t2 = (parts[rnd, t, lat] for rnd in range(3))
            rows = pl.ds(t * 8 * clat + lat, 8, stride=clat)
            inc_out[rows, :] = inc_b * b0 + inc_t * t1
            res_out[rows, :] = res_b * b0 + res_t * t1 + res_2 * t2

    for d in (-1, 1, 0):
        def sent(d=d):
            edge = HALO if d else clat
            strip = HALO // 2 if d else HALO
            rows = (n_lon if d else n_lon - 1) * (1 + 2 * SLOT * edge + strip + 3 * cap)
            rows_of(wide_send.at[d + 1], proxy, rows + (dense_side_rows if d else dense_own)).wait_send()
        guarded(d, sent)
    with_sides(lambda sides: rows_of(ask_send, ask_in, n_lon - 1 + sides * n_lon).wait_send())
    if not direct:
        red_all(0, red_lon, n_lon - 1).wait_send()
    red_all(2, red_far, far_size - 1).wait_send()


def store_kernel(inc, res, inc_out, res_out, sems):
    pairs = ((inc, inc_out), (res, res_out))
    copies = [pltpu.make_async_copy(src, dst, sems.at[n]) for n, (src, dst) in enumerate(pairs)]
    for copy in copies:
        copy.start()
    for copy in copies:
        copy.wait()


def shards(n_lat, n_lon, courant, obs_matrix, obs_weight, innovation, block_owner, block_row, block_count):
    _, levels, clat, clon = courant.shape
    cap = block_row.shape[1]
    tiles = levels // 8
    ring = clat + 2 * STEPS
    rows = clat + 2 * HALO
    unit = clon // cap
    src_pad = -(-3 * n_lon // unit) * unit
    n_blocks = src_pad * cap
    anywhere = pl.BlockSpec(memory_space=pl.ANY)
    dma = pltpu.SemaphoreType.DMA

    def f32(*shape):
        return pltpu.VMEM(shape, F32)

    def bf16(*shape):
        return pltpu.VMEM(shape, BF16)

    def i32(*shape):
        return pltpu.SMEM(shape, jnp.int32)

    flat = (levels * clat, clon)
    fields = pl.pallas_call(
        functools.partial(kernel, n_lat, n_lon),
        out_shape=(f32(*flat), f32(*flat)),
        in_specs=[anywhere] * 8,
        out_specs=(pl.BlockSpec(memory_space=pltpu.VMEM),) * 2,
        scratch_shapes=[
            f32(2, levels, clat, clon),
            f32(2 * levels * clat, clon),
            f32(cap, clon, clon),
            f32(3, src_pad, cap, clon),
            f32(3 * n_lon, 1, clon),
            f32(3, 1, clon),
            bf16(PAD_WIN * cap, n_blocks),
            bf16(PAD_WIN * cap, 2 * n_blocks),
            bf16(ring * levels, n_blocks),
            bf16(ring * levels, 2 * n_blocks),
            f32(2, PAD_WIN, cap, clon),
            f32(2, ring, tiles, 8, clon),
            f32(n_lon, 2, SLOT, clat, clon),
            f32(2, n_lon, 2, SLOT, HALO, clon),
            f32(n_lon, HALO, clon),
            f32(2, n_lon, HALO // 2, clon),
            f32(2, n_lon, SLOT, rows, clon),
            f32(n_lon, HALO, clon),
            f32(2, n_lon, HALO // 2, clon),
            f32(2, n_lon, SLOT, rows, clon),
            f32(5, WIN, 2, cap, clon),
            f32(2, 2, STEPS, tiles, 8, clon),
            f32(2, 2, STEPS, tiles, 8, clon),
            f32(2, 2, tiles, 8, clon),
            f32(2, 2, tiles, 8, clon),
            f32(2, 2, 8, clon),
            f32(2, 2, 8, clon),
            f32(5, 2, tiles, ring, 8, clon),
            f32(cap, clon, clon),
            f32(3, tiles, clat, 8, clon),
            f32(n_lon, 1, clon),
            f32(n_lat * n_lon if n_lat * n_lon <= DIRECT else n_lat, 1, clon),
            f32(n_lon * 256, clon),
            i32(1, n_lon * SLOT),
            i32(3 * n_lon, 1, n_lon * SLOT),
            dma, dma, dma,
            dma((3,)), dma((8,)), dma, dma((3, n_lon)),
            dma((4,)),
            pltpu.SemaphoreType.REGULAR((2,)),
            f32(1, cap, clon), f32(1, cap, clon),
            i32(1, cap), i32(1, cap), i32(1, 1),
            dma((5,)),
        ],
        compiler_params=pltpu.CompilerParams(collective_id=0, has_side_effects=True),
    )(courant, courant.reshape(2 * levels * clat, clon), obs_matrix, obs_weight, innovation, block_owner[:, :, 0], block_row, block_count)
    out = jax.ShapeDtypeStruct(flat, F32)
    stored = pl.pallas_call(
        store_kernel,
        out_shape=(out, out),
        in_specs=[anywhere] * 2,
        out_specs=(anywhere,) * 2,
        scratch_shapes=[dma((2,))],
    )(*[pltpu.with_memory_space_constraint(field, pltpu.VMEM) for field in fields])
    return tuple(field.reshape(levels, clat, clon) for field in stored)


def solution(mesh):
    placed = (
        P(None, None, "lat", "lon"),
        P("lat", "lon", None, None),
        P("lat", "lon", None),
        P("lat", "lon", None),
        P("lat", "lon", None),
        P("lat", "lon"),
        P("lat", "lon"),
    )
    return jax.shard_map(
        functools.partial(shards, mesh.shape["lat"], mesh.shape["lon"]),
        mesh=mesh,
        in_specs=placed,
        out_specs=(P(None, "lat", "lon"), P(None, "lat", "lon")),
        check_vma=False,
    )
```
